32 devices in a mesh: gz: 8 (over z, y), gy: 4 (over x, core).
Axes of the slice: x: 2, y: 2, z: 4, core: 2. Of those that a mesh axis runs over, the one named last changes fastest.
Arguments:
- charges: float32 [64, 64, 1024], P('gz', 'gy'), may hold values from -6 to 6
- kernel: float32 [64, 64, 64], P('gz', 'gy'), may hold values from -0.01171875 to 0.01171875
Outputs:
- fine_potential: float32 [128, 128, 2048], P('gz', 'gy')
The draws below stay inside these ranges and needn't reach their ends.
All inputs are finite; a program needn't handle non-finite values.
Results may differ from the reference program's by a relative error of at most 0.000098.
Values sent between devices are 32-bit elements; how exact they have to be, the bound alone decides.
A program may use at most 128 MiB of HBM per device.

```python
import jax
import jax.numpy as jnp

GRID = 64
REPL = 16
FINE = 128


def block_scale(own_key, shape, cuts, smallest, largest):
    gain = 1.0
    for position, parts in cuts:
        steps = jax.random.uniform(jax.random.fold_in(jax.random.fold_in(own_key, 6), position), (parts,), jnp.float32, smallest / len(cuts), largest / len(cuts))
        gain = gain * jnp.repeat(jnp.exp(steps), shape[position] // parts).reshape((-1,) + (1,) * (len(shape) - 1 - position))
    return gain


def bell_draw(key, shape, width, bound, split=(), held_as=jnp.bfloat16):
    values = jax.random.normal(key, shape, jnp.float32) * width
    if len(split) > 0:
        values = block_scale(key, shape, split, -0.22, 0.18) * values
    return jnp.clip(values, min=-bound, max=bound).astype(held_as)


def setup_inputs(seed: int = 0) -> dict:
    streams_of = jax.random.split(jax.random.key(seed), 3)
    charges = bell_draw(streams_of[0], (GRID, GRID, GRID * REPL), 1.0, 6.0, ((0, 8), (1, 4)), jnp.float32)
    kernel = bell_draw(streams_of[1], (GRID, GRID, GRID), (GRID * GRID * GRID) ** -0.5, 0.01171875, ((0, 8), (1, 4)), jnp.float32)
    return {"charges": charges, "kernel": kernel}


def refine(coarse, axis):
    before = jnp.roll(coarse, 1, axis)
    after = jnp.roll(coarse, -1, axis)
    after_two = jnp.roll(coarse, -2, axis)
    middle = (9.0 * (coarse + after) - (before + after_two)) / 16.0
    stacked = jnp.stack([coarse, middle], axis=axis + 1)
    shape = list(coarse.shape)
    shape[axis] = 2 * shape[axis]
    return stacked.reshape(shape)


def reference(charges, kernel):
    grids = charges.reshape(GRID, GRID, GRID, REPL)
    charge_spec = jnp.fft.fftn(grids, axes=(0, 1, 2))
    kernel_spec = jnp.fft.fftn(kernel, axes=(0, 1, 2))
    potential = jnp.fft.ifftn(charge_spec * kernel_spec[:, :, :, None], axes=(0, 1, 2)).real.astype(jnp.float32)
    result = refine(potential, 0)
    result = refine(result, 1)
    result = refine(result, 2)
    return result.reshape(FINE, FINE, FINE * REPL)
```

```python
import functools

import jax
import jax.numpy as jnp
import numpy as np
from jax import lax
from jax.experimental import pallas as pl
from jax.experimental.pallas import tpu as pltpu
from jax.sharding import PartitionSpec as P

AXES = ("gz", "gy")


def angle(first, second, count):
    return 2.0 * np.pi / count * ((first * second) % count)


def x_table(count, replicas, devices):
    half = replicas // 2
    columns = count * half // devices
    device, part, column, x, side, pair = np.ix_(
        *(np.arange(s) for s in (devices, 2, columns, count, 2, half))
    )
    flat = device * columns + column
    theta = angle(flat // half, x, count)
    value = np.where(part == side, np.cos(theta), np.where(part == 0, np.sin(theta), -np.sin(theta)))
    value = value * (flat % half == pair)
    return value.reshape(devices * 2 * columns, count, replicas)


def x_kernel_table(count, replicas, devices):
    half = replicas // 2
    columns = count * half // devices
    lines = max(1, columns // half)
    device, part, line, x = np.ix_(*(np.arange(s) for s in (devices, 2, lines, count)))
    theta = angle(device * columns // half + line, x, count)
    value = np.where(part == 0, np.cos(theta), -np.sin(theta))
    return value.reshape(devices * 2 * lines, count)


def y_table(count, planes, rows):
    part, block, plane, row, new_plane, new_part, freq = np.ix_(
        *(np.arange(s) for s in (2, count // rows, planes, rows, planes, 2, count))
    )
    theta = angle(block * rows + row, freq, count)
    value = np.where(
        part == new_part, np.cos(theta), np.where(new_part == 0, np.sin(theta), -np.sin(theta))
    )
    value = value * (plane == new_plane)
    return value.reshape(2 * count * planes, planes * 2 * count)


def z_table(count, planes, columns, lines, group, wave):
    blocks = count // planes
    low, high, column, z_low, z_high, line = np.ix_(
        *(np.arange(s) for s in (planes, blocks, columns, planes, blocks, lines))
    )
    theta = angle(high * planes + low, z_high * planes + z_low, count)
    value = wave(theta) * (column // group == line)
    return value.reshape(count * columns, count * lines)


def refined(values, axis):
    before = np.roll(values, 1, axis)
    after = np.roll(values, -1, axis)
    after_two = np.roll(values, -2, axis)
    middle = (9.0 * (values + after) - (before + after_two)) / 16.0
    stacked = np.stack([values, middle], axis=axis + 1)
    shape = list(values.shape)
    shape[axis] = 2 * shape[axis]
    return stacked.reshape(shape)


def const(values):
    return jnp.asarray(np.asarray(values, np.float32))


def dot(left, right, dims=((1,), (0,))):
    return lax.dot_general(
        left, right, (dims, ((), ())), precision=lax.Precision.HIGH,
        preferred_element_type=jnp.float32,
    )


def extended(block, axis, dim):
    size = lax.axis_size(axis)
    forward = [(i, (i + 1) % size) for i in range(size)]
    backward = [(target, source) for source, target in forward]
    low = lax.ppermute(lax.slice_in_dim(block, block.shape[dim] - 1, None, axis=dim), axis, forward)
    high = lax.ppermute(lax.slice_in_dim(block, 0, 2, axis=dim), axis, backward)
    return jnp.concatenate([low, block, high], axis=dim)


def refine_rim(haloed, axis, count):
    centre = lax.slice_in_dim(haloed, 1, 1 + count, axis=axis)
    before = lax.slice_in_dim(haloed, 0, count, axis=axis)
    after = lax.slice_in_dim(haloed, 2, 2 + count, axis=axis)
    after_two = lax.slice_in_dim(haloed, 3, 3 + count, axis=axis)
    middle = (9.0 * (centre + after) - (before + after_two)) / 16.0
    stacked = jnp.stack([centre, middle], axis=axis + 1)
    shape = list(centre.shape)
    shape[axis] = 2 * count
    return stacked.reshape(shape)


def plain(charges, kernel):
    planes, rows, count = kernel.shape
    replicas = charges.shape[2] // count
    half = replicas // 2
    blocks_z, blocks_y = lax.axis_size("gz"), lax.axis_size("gy")
    devices = blocks_z * blocks_y
    place = planes * rows
    columns = count * half // devices
    lines = max(1, columns // half)
    table_x = x_table(count, replicas, devices)
    table_y = const(y_table(count, planes, rows))
    cos_z = const(z_table(count, planes, columns, columns, 1, np.cos))
    sin_z = const(z_table(count, planes, columns, columns, 1, np.sin))
    cos_k = const(z_table(count, planes, columns, lines, half, np.cos) / count**3)
    sin_k = const(z_table(count, planes, columns, lines, half, np.sin) / count**3)

    sent = dot(const(table_x.reshape(-1, count * replicas)), charges.reshape(place, -1), ((1,), (1,)))
    sent_k = dot(const(x_kernel_table(count, replicas, devices)), kernel.reshape(place, count), ((1,), (1,)))
    both = jnp.concatenate(
        [sent.reshape(devices, 2 * columns, place), sent_k.reshape(devices, 2 * lines, place)], axis=1
    )
    both = lax.all_to_all(both, AXES, split_axis=0, concat_axis=0, tiled=True)

    def by_y(block, width):
        block = block.reshape(blocks_z, blocks_y, 2, width, place).transpose(0, 3, 2, 1, 4)
        block = dot(block.reshape(blocks_z * width, 2 * blocks_y * place), table_y)
        block = block.reshape(blocks_z * width, planes, 2 * count).transpose(1, 0, 2)
        return block.reshape(count * width, 2 * count)

    def swap(values):
        return jnp.concatenate([values[:, count:], values[:, :count]], axis=1)

    sign = jnp.where(lax.broadcasted_iota(jnp.int32, (1, 2 * count), 1) < count, 1.0, -1.0)
    data = by_y(both[:, : 2 * columns], columns)
    green = by_y(both[:, 2 * columns :], lines)
    data = dot(cos_z, data) + sign * swap(dot(sin_z, data))
    green = dot(cos_k, green) + sign * swap(dot(sin_k, green))
    real, imag = green[:, :count], green[:, count:]
    data = data * jnp.concatenate([real, real], axis=1) + swap(data) * jnp.concatenate([-imag, imag], axis=1)
    data = dot(cos_z, data) - sign * swap(dot(sin_z, data))
    data = data.reshape(planes, blocks_z * columns, 2 * count).transpose(1, 0, 2)
    data = dot(data.reshape(blocks_z * columns, planes * 2 * count), table_y, ((1,), (1,)))
    data = data.reshape(blocks_z, columns, 2, blocks_y, place).transpose(0, 3, 2, 1, 4)
    data = lax.all_to_all(
        data.reshape(devices, 2 * columns, place), AXES, split_axis=0, concat_axis=0, tiled=True
    )
    fine_x = const(refined(table_x, 1).reshape(-1, 2 * count * replicas))
    result = dot(data.reshape(devices * 2 * columns, place), fine_x, ((0,), (0,)))
    result = result.reshape(planes, rows, 2 * count * replicas)
    result = extended(extended(result, "gz", 0), "gy", 1)
    result = refine_rim(result, 0, planes)
    return refine_rim(result, 1, rows)


LANES = 128
MESH = pl.DeviceIdType.MESH


def table(values):
    high = np.asarray(values, np.float32).astype(jnp.bfloat16)
    low = (np.asarray(values, np.float64) - high.astype(np.float64)).astype(jnp.bfloat16)
    return [jnp.asarray(high), jnp.asarray(low)]


def split(values):
    high = values.astype(jnp.bfloat16)
    return high, (values - high.astype(jnp.float32)).astype(jnp.bfloat16)


def mul(left, right, dims=((1,), (0,))):
    return lax.dot_general(left, right, (dims, ((), ())), preferred_element_type=jnp.float32)


def mul3(left, right, dims=((1,), (0,))):
    (a, b), (c, d) = left, right
    return mul(a, d, dims) + mul(b, c, dims) + mul(a, c, dims)


GROUPS = 4
CHUNKS = 2


def line_of(device, chunk, count):
    flip = np.where(device == 0, count // 2, (count - device) % count)
    return np.where(chunk == 0, device, flip)


def pair_table(count, replicas, devices):
    half = replicas // 2
    chunk, device, part, row, x, side, pair = np.ix_(
        *(np.arange(s) for s in (CHUNKS, devices, 2, half, count, 2, half))
    )
    theta = angle(line_of(device, chunk, count), x, count)
    value = np.where(part == side, np.cos(theta), np.where(part == 0, np.sin(theta), -np.sin(theta)))
    value = value * (row == pair)
    return value.reshape(CHUNKS, devices * 2 * half, count, replicas)


def line_table(count, devices):
    device, row, x = np.ix_(*(np.arange(s) for s in (devices, 8, count)))
    theta = angle(device, x, count)
    other = np.where(device == 0, np.cos(angle(count // 2, x, count)), -np.sin(theta))
    value = np.where(row == 0, np.cos(theta), np.where(row == 1, other, 0.0))
    return value.reshape(devices * 8, count)


def stack3(values):
    high = np.asarray(values, np.float32).astype(jnp.bfloat16)
    low = (np.asarray(values, np.float64) - high.astype(np.float64)).astype(jnp.bfloat16)
    return jnp.asarray(np.concatenate([high, high, low], axis=1))


def z_tables(count, blocks):
    planes = count // blocks
    freq = np.arange(count)[:, None]
    place = np.arange(count)[None, :]
    theta = angle(freq, (place % blocks) * planes + place // blocks, count)
    forward = stack3(np.concatenate([np.cos(theta), np.sin(theta)], axis=0))
    inverse = stack3(np.concatenate([np.cos(theta.T), np.sin(theta.T)], axis=0))
    return forward, inverse


def remote(source, target, sems, number, place):
    copy = pltpu.make_async_remote_copy(
        src_ref=source, dst_ref=target, send_sem=sems.at[0, number], recv_sem=sems.at[1, number],
        device_id=place, device_id_type=MESH,
    )
    copy.start()
    return copy


def exchange(blocks_z, blocks_y, rows, source, target, sems):
    size = blocks_z * blocks_y // GROUPS
    me = lax.axis_index("gz") * blocks_y + lax.axis_index("gy")
    group, inner = me // size, lax.rem(me, size)
    high, low = group // 2, lax.rem(group, 2)
    pitch_from, pitch_to = source.shape[0] // (size * GROUPS), target.shape[0] // (size * GROUPS)

    def span(ref, device, pitch):
        return ref.at[pl.ds(pl.multiple_of(device * pitch, 8), rows)]

    copies = []
    for flip_high, flip_low in ((1, 0), (1, 1), (0, 1), (0, 0)):
        other_group = lax.rem(high + flip_high, 2) * 2 + lax.rem(low + flip_low, 2)
        for step in range(size):
            if (flip_high, flip_low, step) == (0, 0, 0):
                continue
            other = other_group * size + lax.rem(inner + step, size)
            copies.append(remote(
                span(source, other, pitch_from), span(target, me, pitch_to), sems, len(copies),
                (other // blocks_y, lax.rem(other, blocks_y)),
            ))
    mine_from = pl.ds(pl.multiple_of(me * pitch_from, 8), min(pitch_from, pitch_to))
    mine_to = pl.ds(pl.multiple_of(me * pitch_to, 8), min(pitch_from, pitch_to))
    target[mine_to, :] = source[mine_from, :]
    return copies


def wait_recv(copies):
    for copy in copies:
        copy.wait_recv()


def swap_parts(values):
    half = LANES // 2
    pieces = [
        pltpu.roll(values[:, p : p + LANES], half, 1) for p in range(0, values.shape[1], LANES)
    ]
    return jnp.concatenate(pieces, axis=1)


def stacked(values):
    high, low = split(values)
    return jnp.concatenate([low, high, high], axis=0)


def repeat(values, times):
    return jnp.concatenate([values] * times, axis=1)


def y_lines(ref, start, stride, blocks):
    return ref[pl.ds(start, blocks, stride=stride), :]


def middle_stage(sizes, held, table_y, forward, inverse, green, back):
    count, blocks_z, blocks_y, half = sizes
    planes = count // blocks_z
    pitch = held.shape[0] // (blocks_z * blocks_y)
    lane = lax.broadcasted_iota(jnp.int32, (1, LANES), 1)
    sign = jnp.where(lane < count, 1.0, -1.0)

    def gather(row):
        pieces = [y_lines(held, y * pitch + row, blocks_y * pitch, blocks_z) for y in range(blocks_y)]
        return jnp.concatenate(pieces, axis=1)

    lines = [
        jnp.concatenate([gather(column), gather(half + column)], axis=1) for column in range(half)
    ]
    if green is None:
        me = lax.axis_index("gz") * blocks_y + lax.axis_index("gy")
        keep = jnp.where(me == 0, 0.0, 1.0).astype(jnp.float32)
        first, second = gather(2 * half), gather(2 * half + 1)
        lines.append(jnp.concatenate([first, keep * second], axis=1))
        lines.append(
            jnp.concatenate([keep * first + (1.0 - keep) * second, -keep * second], axis=1)
        )
    width = len(lines)
    data = mul3(split(jnp.concatenate(lines, axis=0)), table_y)
    data = jnp.concatenate(
        [
            jnp.concatenate(
                [
                    data[c * blocks_z : (c + 1) * blocks_z, p * LANES : (p + 1) * LANES]
                    for p in range(planes)
                ],
                axis=0,
            )
            for c in range(width)
        ],
        axis=1,
    )
    both = mul(forward, stacked(data))
    data = both[:count] + repeat(sign, width) * swap_parts(both[count:])
    spectra = None
    if green is None:
        scaled = data[:, half * LANES :] * (1.0 / count**3)
        green, spectra = scaled[:, :LANES], scaled
        data = data[:, : half * LANES]
    other = swap_parts(green)
    real = jnp.where(lane < count, green, other)
    imag = jnp.where(lane < count, -other, green)
    data = data * repeat(real, half) + swap_parts(data) * repeat(imag, half)
    both = mul(inverse, stacked(data))
    data = both[:count] - repeat(sign, half) * swap_parts(both[count:])
    data = jnp.concatenate(
        [
            jnp.concatenate(
                [
                    data[p * blocks_z : (p + 1) * blocks_z, c * LANES : (c + 1) * LANES]
                    for p in range(planes)
                ],
                axis=1,
            )
            for c in range(half)
        ],
        axis=0,
    )
    data = mul3(split(data), table_y, ((1,), (1,)))
    out_pitch = 2 * half
    for column in range(half):
        for part in range(2):
            for y in range(blocks_y):
                at = (part * blocks_y + y) * LANES
                back[pl.ds(y * out_pitch + part * half + column, blocks_z, stride=blocks_y * out_pitch), :] = (
                    data[column * blocks_z : (column + 1) * blocks_z, at : at + LANES]
                )
    return spectra


def send_rims(blocks_z, blocks_y, planes, rows, own, stage, rims, sems):
    to_up, to_down, to_corner = stage
    low_z, high_z, low_y, high_y, corner = rims
    gz, gy = lax.axis_index("gz"), lax.axis_index("gy")
    next_z, last_z = lax.rem(gz + 1, blocks_z), lax.rem(gz + blocks_z - 1, blocks_z)
    next_y, last_y = lax.rem(gy + 1, blocks_y), lax.rem(gy + blocks_y - 1, blocks_y)
    end = (planes - 1) * rows
    copies = [
        remote(own.at[pl.ds(0, 2 * rows)], high_z, sems, 0, (last_z, gy)),
        remote(own.at[pl.ds(end, rows)], low_z, sems, 1, (next_z, gy)),
    ]
    def side(row):
        return jnp.concatenate([own[p * rows + row : p * rows + row + 1, :] for p in range(planes)], axis=0)

    to_up[...] = side(rows - 1)
    to_down[...] = jnp.concatenate([side(0), side(1)], axis=0)
    picks = (
        (end + rows - 1,), (end, end + 1), (rows - 1, 2 * rows - 1), (0, 1, rows, rows + 1),
    )
    for number, pick in enumerate(picks):
        pieces = [own[r : r + 1, :] for r in pick]
        pieces.append(jnp.zeros((8 - len(pick), own.shape[1]), jnp.float32))
        to_corner[number] = jnp.concatenate(pieces, axis=0)
    copies.append(remote(to_down, high_y, sems, 2, (gz, last_y)))
    copies.append(remote(to_up, low_y, sems, 3, (gz, next_y)))
    places = ((next_z, next_y), (next_z, last_y), (last_z, next_y), (last_z, last_y))
    for number, (pick, place) in enumerate(zip(picks, places)):
        span = pl.ds(0, len(pick))
        copies.append(
            remote(to_corner.at[number, span], corner.at[number, span], sems, 4 + number, place)
        )
    return copies


def rim_lines(planes, rims):
    low_z, high_z, low_y, high_y, corner = rims
    empty = jnp.zeros((5, low_z.shape[1]), jnp.float32)
    tiles = [corner[0, 0:1, :], corner[1, 0:2, :], empty]
    for p in range(planes):
        tiles += [
            low_y[p : p + 1, :], high_y[p : p + 1, :], high_y[planes + p : planes + p + 1, :], empty,
        ]
    tiles += [corner[2, 0:1, :], corner[3, 0:2, :], empty]
    tiles += [corner[2, 1:2, :], corner[3, 2:4, :], empty]
    return jnp.concatenate([low_z[...], high_z[...], *tiles], axis=0)


def main_kernel(sizes, *refs):
    count, blocks_z, blocks_y, half, n_tables = sizes
    devices = blocks_z * blocks_y
    planes = count // blocks_z
    q_ref, k_ref = refs[:2]
    sources = refs[2 : 2 + n_tables]
    out = refs[2 + n_tables]
    tables = refs[3 + n_tables : 3 + 2 * n_tables]
    rest = list(refs[3 + 2 * n_tables :])
    table_sem, sent_sem, back_sem, rim_sem = rest[:4]
    sent, held, back, home, own = (rest[4 + 2 * i : 6 + 2 * i] for i in range(5))
    stages, rims = (rest[14:17], rest[17:20]), (rest[20:25], rest[25:30])
    table_x, table_k, table_y, table_z, table_f = (
        tables[0:2], tables[2:4], tables[4:6], tables[6:8], tables[8:12]
    )
    loads = [pltpu.make_async_copy(s, t, table_sem.at[i]) for i, (s, t) in enumerate(zip(sources, tables))]
    for load in loads:
        load.start()
    me = lax.axis_index("gz") * blocks_y + lax.axis_index("gy")
    barrier = pltpu.get_barrier_semaphore()
    for step in range(1, devices):
        other = lax.rem(me + step, devices)
        pl.semaphore_signal(
            barrier, inc=1, device_id=(other // blocks_y, lax.rem(other, blocks_y)), device_id_type=MESH
        )
    rows = q_ref.shape[0] // planes
    size = 2 * half
    charges = jnp.concatenate(split(q_ref[...]), axis=0)
    pitch = sent[0].shape[0] // devices

    def x_lines(chunk):
        per = LANES // size
        for group in range(devices // per):
            both = mul(table_x[chunk][group * 2 * LANES : (group + 1) * 2 * LANES, :], charges, ((1,), (1,)))
            made = both[:LANES, :LANES] + both[:LANES, LANES:] + both[LANES:, :LANES]
            step = sent[chunk].shape[0] // devices
            for inner in range(per):
                at = (group * per + inner) * step
                sent[chunk][at : at + size, :] = made[inner * size : (inner + 1) * size, :]

    loads[2].wait()
    loads[3].wait()
    lines = mul3((table_k[0][...], table_k[1][...]), split(k_ref[...]), ((1,), (1,)))
    for device in range(devices):
        sent[0][device * pitch + size : device * pitch + size + 8, :] = lines[device * 8 : (device + 1) * 8, :]
    loads[0].wait()
    x_lines(0)
    pl.semaphore_wait(barrier, devices - 1)
    there = [exchange(blocks_z, blocks_y, size + 2, sent[0], held[0], sent_sem.at[0])]
    loads[1].wait()
    x_lines(1)
    there.append(exchange(blocks_z, blocks_y, size, sent[1], held[1], sent_sem.at[1]))
    for load in loads[4:8]:
        load.wait()
    y_pair = (table_y[0][...], table_y[1][...])
    shape = (count, blocks_z, blocks_y, half)
    wait_recv(there[0])
    green = middle_stage(shape, held[0], y_pair, table_z[0][...], table_z[1][...], None, back[0])
    returns = [exchange(blocks_z, blocks_y, size, back[0], home[0], back_sem.at[0])]
    wait_recv(there[1])
    middle_stage(shape, held[1], y_pair, table_z[0][...], table_z[1][...], green[:, LANES:], back[1])
    returns.append(exchange(blocks_z, blocks_y, size, back[1], home[1], back_sem.at[1]))
    for load in loads[8:]:
        load.wait()
    borders = []
    for chunk in range(CHUNKS):
        fine = (table_f[2 * chunk][...], table_f[2 * chunk + 1][...])
        wait_recv(returns[chunk])
        turned = jnp.transpose(home[chunk][...])
        own[chunk][...] = turned
        borders.append(
            send_rims(blocks_z, blocks_y, planes, rows, own[chunk], stages[chunk], rims[chunk], rim_sem.at[chunk])
        )
        made = mul3(split(turned), fine).reshape(planes, rows, -1)
        if chunk:
            made = out[1 : planes + 1, :rows, :] + made
        out[1 : planes + 1, :rows, :] = made
        wait_recv(borders[chunk])
        made = mul3(split(rim_lines(planes, rims[chunk])), fine)
        deep = 3 * rows
        ends, sides = made[:deep].reshape(3, rows, -1), made[deep:].reshape(planes + 3, 8, -1)
        if chunk:
            sides = out[:, rows:, :] + sides
            ends = jnp.concatenate([out[0:1, :rows, :], out[planes + 1 :, :rows, :]], axis=0) + ends
        out[:, rows:, :] = sides
        out[0:1, :rows, :] = ends[0:1]
        out[planes + 1 :, :rows, :] = ends[1:]
    for copies in there + returns + borders:
        for copy in copies:
            copy.wait_send()


def refine_kernel(x_ref, r_ref, o_ref):
    step = pl.program_id(0)
    near = x_ref[pl.ds(step, 4)].reshape(4 * x_ref.shape[1], x_ref.shape[2])
    high, low = split(near)
    fine = mul(r_ref[...], jnp.concatenate([low, high], axis=0))
    o_ref[...] = fine.reshape(o_ref.shape)


def rim_table(count):
    made = np.zeros((2 * count, count + 3))
    for i in range(count):
        made[2 * i, i + 1] = 1.0
        made[2 * i + 1, i : i + 4] = np.array([-1.0, 9.0, 9.0, -1.0]) / 16.0
    return made


def refine(haloed, planes, rows, width):
    along_y = rim_table(rows)
    empty = np.zeros((2 * rows, 5))
    along_y = np.concatenate([along_y[:, 1 : rows + 1], along_y[:, :1], along_y[:, rows + 1 :], empty], axis=1)
    both = np.kron(rim_table(1), along_y)
    both = jnp.asarray(np.concatenate([both, both], axis=1), jnp.bfloat16)
    return pl.pallas_call(
        refine_kernel,
        grid=(planes,),
        out_shape=jax.ShapeDtypeStruct((2 * planes, 2 * rows, width), jnp.float32),
        in_specs=[
            pl.BlockSpec(haloed.shape, lambda i: (0, 0, 0)),
            pl.BlockSpec(both.shape, lambda i: (0, 0)),
        ],
        out_specs=pl.BlockSpec((2, 2 * rows, width), lambda i: (i, 0, 0)),
        compiler_params=pltpu.CompilerParams(vmem_limit_bytes=16 * 1024 * 1024),
    )(haloed, both)


def per_device(charges, kernel):
    planes, rows, count = kernel.shape
    width = charges.shape[2]
    replicas = width // count
    half = replicas // 2
    blocks_z, blocks_y = lax.axis_size("gz"), lax.axis_size("gy")
    devices = blocks_z * blocks_y
    place = planes * rows
    fits = place == LANES and 2 * count == LANES and half == 8 and blocks_z == 8
    if not fits or count != CHUNKS * devices or replicas % 2 or rows % 8 or planes != 8 or devices % 8:
        return plain(charges, kernel)
    size = 2 * half
    per = LANES // size
    lines_x = pair_table(count, replicas, devices)
    table_x, table_f = [], []
    for chunk in range(CHUNKS):
        high, low = table(lines_x[chunk].reshape(devices // per, LANES, width))
        table_x.append(jnp.concatenate([high, low], axis=1).reshape(-1, width))
        table_f += table(refined(lines_x[chunk], 1).reshape(-1, 2 * width))
    table_y = table(y_table(count, planes, rows))
    tables = [*table_x, *table(line_table(count, devices)), *table_y, *z_tables(count, blocks_z), *table_f]
    deep = devices * size
    vmem = pl.BlockSpec(memory_space=pltpu.VMEM)
    block = lambda *shape: pltpu.VMEM(shape, jnp.float32)
    dma = pltpu.SemaphoreType.DMA
    stage = [block(planes, deep), block(2 * planes, deep), block(4, 8, deep)]
    rim = [
        block(rows, deep), block(2 * rows, deep), block(planes, deep), block(2 * planes, deep),
        block(4, 8, deep),
    ]
    haloed = pl.pallas_call(
        functools.partial(main_kernel, (count, blocks_z, blocks_y, half, len(tables))),
        out_shape=jax.ShapeDtypeStruct((planes + 3, rows + 8, 2 * width), jnp.float32),
        in_specs=[vmem, vmem] + [pl.BlockSpec(memory_space=pl.ANY)] * len(tables),
        out_specs=vmem,
        scratch_shapes=[
            *(pltpu.VMEM(t.shape, t.dtype) for t in tables),
            dma((len(tables),)), dma((CHUNKS, 2, devices)), dma((CHUNKS, 2, devices)), dma((CHUNKS, 2, 8)),
            block(devices * (size + 8), LANES), block(deep, LANES),
            block(devices * (size + 8), LANES), block(deep, LANES),
            block(deep, LANES), block(deep, LANES),
            block(deep, LANES), block(deep, LANES),
            block(place, deep), block(place, deep),
            *stage, *stage, *rim, *rim,
        ],
        compiler_params=pltpu.CompilerParams(
            collective_id=0, has_side_effects=True, vmem_limit_bytes=44 * 1024 * 1024
        ),
    )(charges.reshape(place, width), kernel.reshape(place, count), *tables)
    return refine(haloed, planes, rows, 2 * width)


def solution(mesh):
    placed = (P("gz", "gy", None), P("gz", "gy", None))
    return jax.shard_map(
        per_device, mesh=mesh, in_specs=placed, out_specs=P("gz", "gy", None), check_vma=False
    )
```

```python
import functools

import jax
import jax.numpy as jnp
import numpy as np
from jax import lax
from jax.experimental import pallas as pl
from jax.experimental.pallas import tpu as pltpu
from jax.sharding import PartitionSpec as P

AXES = ("gz", "gy")


def angle(first, second, count):
    return 2.0 * np.pi / count * ((first * second) % count)


def x_table(count, replicas, devices):
    half = replicas // 2
    columns = count * half // devices
    device, part, column, x, side, pair = np.ix_(
        *(np.arange(s) for s in (devices, 2, columns, count, 2, half))
    )
    flat = device * columns + column
    theta = angle(flat // half, x, count)
    value = np.where(part == side, np.cos(theta), np.where(part == 0, np.sin(theta), -np.sin(theta)))
    value = value * (flat % half == pair)
    return value.reshape(devices * 2 * columns, count, replicas)


def x_kernel_table(count, replicas, devices):
    half = replicas // 2
    columns = count * half // devices
    lines = max(1, columns // half)
    device, part, line, x = np.ix_(*(np.arange(s) for s in (devices, 2, lines, count)))
    theta = angle(device * columns // half + line, x, count)
    value = np.where(part == 0, np.cos(theta), -np.sin(theta))
    return value.reshape(devices * 2 * lines, count)


def y_table(count, planes, rows):
    part, block, plane, row, new_plane, new_part, freq = np.ix_(
        *(np.arange(s) for s in (2, count // rows, planes, rows, planes, 2, count))
    )
    theta = angle(block * rows + row, freq, count)
    value = np.where(
        part == new_part, np.cos(theta), np.where(new_part == 0, np.sin(theta), -np.sin(theta))
    )
    value = value * (plane == new_plane)
    return value.reshape(2 * count * planes, planes * 2 * count)


def z_table(count, planes, columns, lines, group, wave):
    blocks = count // planes
    low, high, column, z_low, z_high, line = np.ix_(
        *(np.arange(s) for s in (planes, blocks, columns, planes, blocks, lines))
    )
    theta = angle(high * planes + low, z_high * planes + z_low, count)
    value = wave(theta) * (column // group == line)
    return value.reshape(count * columns, count * lines)


def refined(values, axis):
    before = np.roll(values, 1, axis)
    after = np.roll(values, -1, axis)
    after_two = np.roll(values, -2, axis)
    middle = (9.0 * (values + after) - (before + after_two)) / 16.0
    stacked = np.stack([values, middle], axis=axis + 1)
    shape = list(values.shape)
    shape[axis] = 2 * shape[axis]
    return stacked.reshape(shape)


def const(values):
    return jnp.asarray(np.asarray(values, np.float32))


def dot(left, right, dims=((1,), (0,))):
    return lax.dot_general(
        left, right, (dims, ((), ())), precision=lax.Precision.HIGH,
        preferred_element_type=jnp.float32,
    )


def extended(block, axis, dim):
    size = lax.axis_size(axis)
    forward = [(i, (i + 1) % size) for i in range(size)]
    backward = [(target, source) for source, target in forward]
    low = lax.ppermute(lax.slice_in_dim(block, block.shape[dim] - 1, None, axis=dim), axis, forward)
    high = lax.ppermute(lax.slice_in_dim(block, 0, 2, axis=dim), axis, backward)
    return jnp.concatenate([low, block, high], axis=dim)


def refine_rim(haloed, axis, count):
    centre = lax.slice_in_dim(haloed, 1, 1 + count, axis=axis)
    before = lax.slice_in_dim(haloed, 0, count, axis=axis)
    after = lax.slice_in_dim(haloed, 2, 2 + count, axis=axis)
    after_two = lax.slice_in_dim(haloed, 3, 3 + count, axis=axis)
    middle = (9.0 * (centre + after) - (before + after_two)) / 16.0
    stacked = jnp.stack([centre, middle], axis=axis + 1)
    shape = list(centre.shape)
    shape[axis] = 2 * count
    return stacked.reshape(shape)


def plain(charges, kernel):
    planes, rows, count = kernel.shape
    replicas = charges.shape[2] // count
    half = replicas // 2
    blocks_z, blocks_y = lax.axis_size("gz"), lax.axis_size("gy")
    devices = blocks_z * blocks_y
    place = planes * rows
    columns = count * half // devices
    lines = max(1, columns // half)
    table_x = x_table(count, replicas, devices)
    table_y = const(y_table(count, planes, rows))
    cos_z = const(z_table(count, planes, columns, columns, 1, np.cos))
    sin_z = const(z_table(count, planes, columns, columns, 1, np.sin))
    cos_k = const(z_table(count, planes, columns, lines, half, np.cos) / count**3)
    sin_k = const(z_table(count, planes, columns, lines, half, np.sin) / count**3)

    sent = dot(const(table_x.reshape(-1, count * replicas)), charges.reshape(place, -1), ((1,), (1,)))
    sent_k = dot(const(x_kernel_table(count, replicas, devices)), kernel.reshape(place, count), ((1,), (1,)))
    both = jnp.concatenate(
        [sent.reshape(devices, 2 * columns, place), sent_k.reshape(devices, 2 * lines, place)], axis=1
    )
    both = lax.all_to_all(both, AXES, split_axis=0, concat_axis=0, tiled=True)

    def by_y(block, width):
        block = block.reshape(blocks_z, blocks_y, 2, width, place).transpose(0, 3, 2, 1, 4)
        block = dot(block.reshape(blocks_z * width, 2 * blocks_y * place), table_y)
        block = block.reshape(blocks_z * width, planes, 2 * count).transpose(1, 0, 2)
        return block.reshape(count * width, 2 * count)

    def swap(values):
        return jnp.concatenate([values[:, count:], values[:, :count]], axis=1)

    sign = jnp.where(lax.broadcasted_iota(jnp.int32, (1, 2 * count), 1) < count, 1.0, -1.0)
    data = by_y(both[:, : 2 * columns], columns)
    green = by_y(both[:, 2 * columns :], lines)
    data = dot(cos_z, data) + sign * swap(dot(sin_z, data))
    green = dot(cos_k, green) + sign * swap(dot(sin_k, green))
    real, imag = green[:, :count], green[:, count:]
    data = data * jnp.concatenate([real, real], axis=1) + swap(data) * jnp.concatenate([-imag, imag], axis=1)
    data = dot(cos_z, data) - sign * swap(dot(sin_z, data))
    data = data.reshape(planes, blocks_z * columns, 2 * count).transpose(1, 0, 2)
    data = dot(data.reshape(blocks_z * columns, planes * 2 * count), table_y, ((1,), (1,)))
    data = data.reshape(blocks_z, columns, 2, blocks_y, place).transpose(0, 3, 2, 1, 4)
    data = lax.all_to_all(
        data.reshape(devices, 2 * columns, place), AXES, split_axis=0, concat_axis=0, tiled=True
    )
    fine_x = const(refined(table_x, 1).reshape(-1, 2 * count * replicas))
    result = dot(data.reshape(devices * 2 * columns, place), fine_x, ((0,), (0,)))
    result = result.reshape(planes, rows, 2 * count * replicas)
    result = extended(extended(result, "gz", 0), "gy", 1)
    result = refine_rim(result, 0, planes)
    return refine_rim(result, 1, rows)


LANES = 128
MESH = pl.DeviceIdType.MESH


def table(values):
    high = np.asarray(values, np.float32).astype(jnp.bfloat16)
    low = (np.asarray(values, np.float64) - high.astype(np.float64)).astype(jnp.bfloat16)
    return [jnp.asarray(high), jnp.asarray(low)]


def split(values):
    high = values.astype(jnp.bfloat16)
    return high, (values - high.astype(jnp.float32)).astype(jnp.bfloat16)


def mul(left, right, dims=((1,), (0,))):
    return lax.dot_general(left, right, (dims, ((), ())), preferred_element_type=jnp.float32)


def mul3(left, right, dims=((1,), (0,))):
    (a, b), (c, d) = left, right
    return mul(a, d, dims) + mul(b, c, dims) + mul(a, c, dims)


GROUPS = 4
CHUNKS = 2


def line_of(device, chunk, count):
    flip = np.where(device == 0, count // 2, (count - device) % count)
    return np.where(chunk == 0, device, flip)


def pair_table(count, replicas, devices):
    half = replicas // 2
    chunk, device, part, row, x, side, pair = np.ix_(
        *(np.arange(s) for s in (CHUNKS, devices, 2, half, count, 2, half))
    )
    theta = angle(line_of(device, chunk, count), x, count)
    value = np.where(part == side, np.cos(theta), np.where(part == 0, np.sin(theta), -np.sin(theta)))
    value = value * (row == pair)
    return value.reshape(CHUNKS, devices * 2 * half, count, replicas)


def line_table(count, devices):
    device, row, x = np.ix_(*(np.arange(s) for s in (devices, 8, count)))
    theta = angle(device, x, count)
    other = np.where(device == 0, np.cos(angle(count // 2, x, count)), -np.sin(theta))
    value = np.where(row == 0, np.cos(theta), np.where(row == 1, other, 0.0))
    return value.reshape(devices * 8, count)


def stack3(values):
    high = np.asarray(values, np.float32).astype(jnp.bfloat16)
    low = (np.asarray(values, np.float64) - high.astype(np.float64)).astype(jnp.bfloat16)
    return jnp.asarray(np.concatenate([high, high, low], axis=1))


def z_tables(count, blocks):
    planes = count // blocks
    freq = np.arange(count)[:, None]
    place = np.arange(count)[None, :]
    theta = angle(freq, (place % blocks) * planes + place // blocks, count)
    forward = stack3(np.concatenate([np.cos(theta), np.sin(theta)], axis=0))
    inverse = stack3(np.concatenate([np.cos(theta.T), np.sin(theta.T)], axis=0))
    return forward, inverse


def remote(source, target, sems, number, place):
    copy = pltpu.make_async_remote_copy(
        src_ref=source, dst_ref=target, send_sem=sems.at[0, number], recv_sem=sems.at[1, number],
        device_id=place, device_id_type=MESH,
    )
    copy.start()
    return copy


def exchange(blocks_z, blocks_y, rows, source, target, sems):
    size = blocks_z * blocks_y // GROUPS
    me = lax.axis_index("gz") * blocks_y + lax.axis_index("gy")
    group, inner = me // size, lax.rem(me, size)
    high, low = group // 2, lax.rem(group, 2)
    pitch_from, pitch_to = source.shape[0] // (size * GROUPS), target.shape[0] // (size * GROUPS)

    def span(ref, device, pitch):
        return ref.at[pl.ds(pl.multiple_of(device * pitch, 8), rows)]

    copies = []
    for flip_high, flip_low in ((1, 0), (1, 1), (0, 1), (0, 0)):
        other_group = lax.rem(high + flip_high, 2) * 2 + lax.rem(low + flip_low, 2)
        for step in range(size):
            if (flip_high, flip_low, step) == (0, 0, 0):
                continue
            other = other_group * size + lax.rem(inner + step, size)
            copies.append(remote(
                span(source, other, pitch_from), span(target, me, pitch_to), sems, len(copies),
                (other // blocks_y, lax.rem(other, blocks_y)),
            ))
    mine_from = pl.ds(pl.multiple_of(me * pitch_from, 8), min(pitch_from, pitch_to))
    mine_to = pl.ds(pl.multiple_of(me * pitch_to, 8), min(pitch_from, pitch_to))
    target[mine_to, :] = source[mine_from, :]
    return copies


def wait_recv(copies):
    for copy in copies:
        copy.wait_recv()


def swap_parts(values):
    half = LANES // 2
    pieces = [
        pltpu.roll(values[:, p : p + LANES], half, 1) for p in range(0, values.shape[1], LANES)
    ]
    return jnp.concatenate(pieces, axis=1)


def stacked(values):
    high, low = split(values)
    return jnp.concatenate([low, high, high], axis=0)


def repeat(values, times):
    return jnp.concatenate([values] * times, axis=1)


def y_lines(ref, start, stride, blocks):
    return ref[pl.ds(start, blocks, stride=stride), :]


def middle_stage(sizes, held, table_y, forward, inverse, green, back):
    count, blocks_z, blocks_y, half = sizes
    planes = count // blocks_z
    pitch = held.shape[0] // (blocks_z * blocks_y)
    lane = lax.broadcasted_iota(jnp.int32, (1, LANES), 1)
    sign = jnp.where(lane < count, 1.0, -1.0)

    def gather(row):
        pieces = [y_lines(held, y * pitch + row, blocks_y * pitch, blocks_z) for y in range(blocks_y)]
        return jnp.concatenate(pieces, axis=1)

    lines = [
        jnp.concatenate([gather(column), gather(half + column)], axis=1) for column in range(half)
    ]
    if green is None:
        me = lax.axis_index("gz") * blocks_y + lax.axis_index("gy")
        keep = jnp.where(me == 0, 0.0, 1.0).astype(jnp.float32)
        first, second = gather(2 * half), gather(2 * half + 1)
        lines.append(jnp.concatenate([first, keep * second], axis=1))
        lines.append(
            jnp.concatenate([keep * first + (1.0 - keep) * second, -keep * second], axis=1)
        )
    width = len(lines)
    data = mul3(split(jnp.concatenate(lines, axis=0)), table_y)
    data = jnp.concatenate(
        [
            jnp.concatenate(
                [
                    data[c * blocks_z : (c + 1) * blocks_z, p * LANES : (p + 1) * LANES]
                    for p in range(planes)
                ],
                axis=0,
            )
            for c in range(width)
        ],
        axis=1,
    )
    both = mul(forward, stacked(data))
    data = both[:count] + repeat(sign, width) * swap_parts(both[count:])
    spectra = None
    if green is None:
        scaled = data[:, half * LANES :] * (1.0 / count**3)
        green, spectra = scaled[:, :LANES], scaled
        data = data[:, : half * LANES]
    other = swap_parts(green)
    real = jnp.where(lane < count, green, other)
    imag = jnp.where(lane < count, -other, green)
    data = data * repeat(real, half) + swap_parts(data) * repeat(imag, half)
    both = mul(inverse, stacked(data))
    data = both[:count] - repeat(sign, half) * swap_parts(both[count:])
    data = jnp.concatenate(
        [
            jnp.concatenate(
                [
                    data[p * blocks_z : (p + 1) * blocks_z, c * LANES : (c + 1) * LANES]
                    for p in range(planes)
                ],
                axis=1,
            )
            for c in range(half)
        ],
        axis=0,
    )
    data = mul3(split(data), table_y, ((1,), (1,)))
    out_pitch = 2 * half
    for column in range(half):
        for part in range(2):
            for y in range(blocks_y):
                at = (part * blocks_y + y) * LANES
                back[pl.ds(y * out_pitch + part * half + column, blocks_z, stride=blocks_y * out_pitch), :] = (
                    data[column * blocks_z : (column + 1) * blocks_z, at : at + LANES]
                )
    return spectra


def send_rims(blocks_z, blocks_y, planes, rows, own, stage, rims, sems):
    to_up, to_down, to_corner = stage
    low_z, high_z, low_y, high_y, corner = rims
    gz, gy = lax.axis_index("gz"), lax.axis_index("gy")
    next_z, last_z = lax.rem(gz + 1, blocks_z), lax.rem(gz + blocks_z - 1, blocks_z)
    next_y, last_y = lax.rem(gy + 1, blocks_y), lax.rem(gy + blocks_y - 1, blocks_y)
    end = (planes - 1) * rows
    copies = [
        remote(own.at[pl.ds(0, 2 * rows)], high_z, sems, 0, (last_z, gy)),
        remote(own.at[pl.ds(end, rows)], low_z, sems, 1, (next_z, gy)),
    ]
    def side(row):
        return jnp.concatenate([own[p * rows + row : p * rows + row + 1, :] for p in range(planes)], axis=0)

    to_up[...] = side(rows - 1)
    to_down[...] = jnp.concatenate([side(0), side(1)], axis=0)
    picks = (
        (end + rows - 1,), (end, end + 1), (rows - 1, 2 * rows - 1), (0, 1, rows, rows + 1),
    )
    for number, pick in enumerate(picks):
        pieces = [own[r : r + 1, :] for r in pick]
        pieces.append(jnp.zeros((8 - len(pick), own.shape[1]), jnp.float32))
        to_corner[number] = jnp.concatenate(pieces, axis=0)
    copies.append(remote(to_down, high_y, sems, 2, (gz, last_y)))
    copies.append(remote(to_up, low_y, sems, 3, (gz, next_y)))
    places = ((next_z, next_y), (next_z, last_y), (last_z, next_y), (last_z, last_y))
    for number, (pick, place) in enumerate(zip(picks, places)):
        span = pl.ds(0, len(pick))
        copies.append(
            remote(to_corner.at[number, span], corner.at[number, span], sems, 4 + number, place)
        )
    return copies


def rim_lines(planes, rims):
    low_z, high_z, low_y, high_y, corner = rims
    empty = jnp.zeros((5, low_z.shape[1]), jnp.float32)
    tiles = [corner[0, 0:1, :], corner[1, 0:2, :], empty]
    for p in range(planes):
        tiles += [
            low_y[p : p + 1, :], high_y[p : p + 1, :], high_y[planes + p : planes + p + 1, :], empty,
        ]
    tiles += [corner[2, 0:1, :], corner[3, 0:2, :], empty]
    tiles += [corner[2, 1:2, :], corner[3, 2:4, :], empty]
    return jnp.concatenate([low_z[...], high_z[...], *tiles], axis=0)


def main_kernel(sizes, *refs):
    count, blocks_z, blocks_y, half, n_tables = sizes
    devices = blocks_z * blocks_y
    planes = count // blocks_z
    q_ref, k_ref = refs[:2]
    sources = refs[2 : 2 + n_tables]
    out = refs[2 + n_tables]
    tables = refs[3 + n_tables : 3 + 2 * n_tables]
    rest = list(refs[3 + 2 * n_tables :])
    table_sem, sent_sem, back_sem, rim_sem = rest[:4]
    sent, held, back, home, own = (rest[4 + 2 * i : 6 + 2 * i] for i in range(5))
    stages, rims = (rest[14:17], rest[17:20]), (rest[20:25], rest[25:30])
    table_x, table_k, table_y, table_z, table_f = (
        tables[0:2], tables[2:4], tables[4:6], tables[6:8], tables[8:12]
    )
    loads = [pltpu.make_async_copy(s, t, table_sem.at[i]) for i, (s, t) in enumerate(zip(sources, tables))]
    for load in loads:
        load.start()
    me = lax.axis_index("gz") * blocks_y + lax.axis_index("gy")
    barrier = pltpu.get_barrier_semaphore()
    for step in range(1, devices):
        other = lax.rem(me + step, devices)
        pl.semaphore_signal(
            barrier, inc=1, device_id=(other // blocks_y, lax.rem(other, blocks_y)), device_id_type=MESH
        )
    rows = q_ref.shape[0] // planes
    size = 2 * half
    charges = jnp.concatenate(split(q_ref[...]), axis=0)
    pitch = sent[0].shape[0] // devices

    def x_lines(chunk):
        per = LANES // size
        for group in range(devices // per):
            both = mul(table_x[chunk][group * 2 * LANES : (group + 1) * 2 * LANES, :], charges, ((1,), (1,)))
            made = both[:LANES, :LANES] + both[:LANES, LANES:] + both[LANES:, :LANES]
            step = sent[chunk].shape[0] // devices
            for inner in range(per):
                at = (group * per + inner) * step
                sent[chunk][at : at + size, :] = made[inner * size : (inner + 1) * size, :]

    scope = jax.named_scope
    with scope("kernel_lines"):
        loads[2].wait()
        loads[3].wait()
        lines = mul3((table_k[0][...], table_k[1][...]), split(k_ref[...]), ((1,), (1,)))
        for device in range(devices):
            at = device * pitch + size
            sent[0][at : at + 8, :] = lines[device * 8 : (device + 1) * 8, :]
    with scope("x_load"):
        loads[0].wait()
    with scope("x_lines0"):
        x_lines(0)
    with scope("barrier"):
        pl.semaphore_wait(barrier, devices - 1)
    with scope("send0"):
        there = [exchange(blocks_z, blocks_y, size + 2, sent[0], held[0], sent_sem.at[0])]
    with scope("x_lines1"):
        loads[1].wait()
        x_lines(1)
    with scope("send1"):
        there.append(exchange(blocks_z, blocks_y, size, sent[1], held[1], sent_sem.at[1]))
    with scope("wait_there0"):
        for load in loads[4:8]:
            load.wait()
        wait_recv(there[0])
    y_pair = (table_y[0][...], table_y[1][...])
    z_pair = (table_z[0][...], table_z[1][...])
    shape = (count, blocks_z, blocks_y, half)
    with scope("middle0"):
        green = middle_stage(shape, held[0], y_pair, *z_pair, None, back[0])
    with scope("return0"):
        returns = [exchange(blocks_z, blocks_y, size, back[0], home[0], back_sem.at[0])]
    with scope("wait_there1"):
        wait_recv(there[1])
    with scope("middle1"):
        middle_stage(shape, held[1], y_pair, *z_pair, green[:, LANES:], back[1])
    with scope("return1"):
        returns.append(exchange(blocks_z, blocks_y, size, back[1], home[1], back_sem.at[1]))
    for load in loads[8:]:
        load.wait()
    borders = []
    for chunk in range(CHUNKS):
        fine = (table_f[2 * chunk][...], table_f[2 * chunk + 1][...])
        with scope(f"wait_back{chunk}"):
            wait_recv(returns[chunk])
        with scope(f"turn{chunk}"):
            turned = jnp.transpose(home[chunk][...])
            own[chunk][...] = turned
        with scope(f"send_rim{chunk}"):
            borders.append(send_rims(
                blocks_z, blocks_y, planes, rows, own[chunk], stages[chunk], rims[chunk], rim_sem.at[chunk]
            ))
        with scope(f"own{chunk}"):
            made = mul3(split(turned), fine).reshape(planes, rows, -1)
            if chunk:
                made = out[1 : planes + 1, :rows, :] + made
            out[1 : planes + 1, :rows, :] = made
        with scope(f"wait_rim{chunk}"):
            wait_recv(borders[chunk])
        with scope(f"rim{chunk}"):
            made = mul3(split(rim_lines(planes, rims[chunk])), fine)
            deep = 3 * rows
            ends, sides = made[:deep].reshape(3, rows, -1), made[deep:].reshape(planes + 3, 8, -1)
            if chunk:
                sides = out[:, rows:, :] + sides
                held_ends = [out[0:1, :rows, :], out[planes + 1 :, :rows, :]]
                ends = jnp.concatenate(held_ends, axis=0) + ends
            out[:, rows:, :] = sides
            out[0:1, :rows, :] = ends[0:1]
            out[planes + 1 :, :rows, :] = ends[1:]
    with scope("wait_sends"):
        for copies in there + returns + borders:
            for copy in copies:
                copy.wait_send()


def refine_kernel(x_ref, r_ref, o_ref):
    step = pl.program_id(0)
    near = x_ref[pl.ds(step, 4)].reshape(4 * x_ref.shape[1], x_ref.shape[2])
    high, low = split(near)
    fine = mul(r_ref[...], jnp.concatenate([low, high], axis=0))
    o_ref[...] = fine.reshape(o_ref.shape)


def rim_table(count):
    made = np.zeros((2 * count, count + 3))
    for i in range(count):
        made[2 * i, i + 1] = 1.0
        made[2 * i + 1, i : i + 4] = np.array([-1.0, 9.0, 9.0, -1.0]) / 16.0
    return made


def refine(haloed, planes, rows, width):
    along_y = rim_table(rows)
    empty = np.zeros((2 * rows, 5))
    along_y = np.concatenate([along_y[:, 1 : rows + 1], along_y[:, :1], along_y[:, rows + 1 :], empty], axis=1)
    both = np.kron(rim_table(1), along_y)
    both = jnp.asarray(np.concatenate([both, both], axis=1), jnp.bfloat16)
    return pl.pallas_call(
        refine_kernel,
        grid=(planes,),
        out_shape=jax.ShapeDtypeStruct((2 * planes, 2 * rows, width), jnp.float32),
        in_specs=[
            pl.BlockSpec(haloed.shape, lambda i: (0, 0, 0)),
            pl.BlockSpec(both.shape, lambda i: (0, 0)),
        ],
        out_specs=pl.BlockSpec((2, 2 * rows, width), lambda i: (i, 0, 0)),
    )(haloed, both)


def per_device(charges, kernel):
    planes, rows, count = kernel.shape
    width = charges.shape[2]
    replicas = width // count
    half = replicas // 2
    blocks_z, blocks_y = lax.axis_size("gz"), lax.axis_size("gy")
    devices = blocks_z * blocks_y
    place = planes * rows
    fits = place == LANES and 2 * count == LANES and half == 8 and blocks_z == 8
    if not fits or count != CHUNKS * devices or replicas % 2 or rows % 8 or planes != 8 or devices % 8:
        return plain(charges, kernel)
    size = 2 * half
    per = LANES // size
    lines_x = pair_table(count, replicas, devices)
    table_x, table_f = [], []
    for chunk in range(CHUNKS):
        high, low = table(lines_x[chunk].reshape(devices // per, LANES, width))
        table_x.append(jnp.concatenate([high, low], axis=1).reshape(-1, width))
        table_f += table(refined(lines_x[chunk], 1).reshape(-1, 2 * width))
    table_y = table(y_table(count, planes, rows))
    tables = [*table_x, *table(line_table(count, devices)), *table_y, *z_tables(count, blocks_z), *table_f]
    deep = devices * size
    vmem = pl.BlockSpec(memory_space=pltpu.VMEM)
    block = lambda *shape: pltpu.VMEM(shape, jnp.float32)
    dma = pltpu.SemaphoreType.DMA
    stage = [block(planes, deep), block(2 * planes, deep), block(4, 8, deep)]
    rim = [
        block(rows, deep), block(2 * rows, deep), block(planes, deep), block(2 * planes, deep),
        block(4, 8, deep),
    ]
    haloed = pl.pallas_call(
        functools.partial(main_kernel, (count, blocks_z, blocks_y, half, len(tables))),
        out_shape=jax.ShapeDtypeStruct((planes + 3, rows + 8, 2 * width), jnp.float32),
        in_specs=[vmem, vmem] + [pl.BlockSpec(memory_space=pl.ANY)] * len(tables),
        out_specs=vmem,
        scratch_shapes=[
            *(pltpu.VMEM(t.shape, t.dtype) for t in tables),
            dma((len(tables),)), dma((CHUNKS, 2, devices)), dma((CHUNKS, 2, devices)), dma((CHUNKS, 2, 8)),
            block(devices * (size + 8), LANES), block(deep, LANES),
            block(devices * (size + 8), LANES), block(deep, LANES),
            block(deep, LANES), block(deep, LANES),
            block(deep, LANES), block(deep, LANES),
            block(place, deep), block(place, deep),
            *stage, *stage, *rim, *rim,
        ],
        compiler_params=pltpu.CompilerParams(
            collective_id=0, has_side_effects=True, vmem_limit_bytes=60 * 1024 * 1024
        ),
    )(charges.reshape(place, width), kernel.reshape(place, count), *tables)
    return refine(haloed, planes, rows, 2 * width)


def solution(mesh):
    placed = (P("gz", "gy", None), P("gz", "gy", None))
    return jax.shard_map(
        per_device, mesh=mesh, in_specs=placed, out_specs=P("gz", "gy", None), check_vma=False
    )
```

```python
import functools

import jax
import jax.numpy as jnp
import numpy as np
from jax import lax
from jax.experimental import pallas as pl
from jax.experimental.pallas import tpu as pltpu
from jax.sharding import PartitionSpec as P

AXES = ("gz", "gy")


def angle(first, second, count):
    return 2.0 * np.pi / count * ((first * second) % count)


def x_table(count, replicas, devices):
    half = replicas // 2
    columns = count * half // devices
    device, part, column, x, side, pair = np.ix_(
        *(np.arange(s) for s in (devices, 2, columns, count, 2, half))
    )
    flat = device * columns + column
    theta = angle(flat // half, x, count)
    value = np.where(part == side, np.cos(theta), np.where(part == 0, np.sin(theta), -np.sin(theta)))
    value = value * (flat % half == pair)
    return value.reshape(devices * 2 * columns, count, replicas)


def x_kernel_table(count, replicas, devices):
    half = replicas // 2
    columns = count * half // devices
    lines = max(1, columns // half)
    device, part, line, x = np.ix_(*(np.arange(s) for s in (devices, 2, lines, count)))
    theta = angle(device * columns // half + line, x, count)
    value = np.where(part == 0, np.cos(theta), -np.sin(theta))
    return value.reshape(devices * 2 * lines, count)


def y_table(count, planes, rows):
    part, block, plane, row, new_plane, new_part, freq = np.ix_(
        *(np.arange(s) for s in (2, count // rows, planes, rows, planes, 2, count))
    )
    theta = angle(block * rows + row, freq, count)
    value = np.where(
        part == new_part, np.cos(theta), np.where(new_part == 0, np.sin(theta), -np.sin(theta))
    )
    value = value * (plane == new_plane)
    return value.reshape(2 * count * planes, planes * 2 * count)


def z_table(count, planes, columns, lines, group, wave):
    blocks = count // planes
    low, high, column, z_low, z_high, line = np.ix_(
        *(np.arange(s) for s in (planes, blocks, columns, planes, blocks, lines))
    )
    theta = angle(high * planes + low, z_high * planes + z_low, count)
    value = wave(theta) * (column // group == line)
    return value.reshape(count * columns, count * lines)


def refined(values, axis):
    before = np.roll(values, 1, axis)
    after = np.roll(values, -1, axis)
    after_two = np.roll(values, -2, axis)
    middle = (9.0 * (values + after) - (before + after_two)) / 16.0
    stacked = np.stack([values, middle], axis=axis + 1)
    shape = list(values.shape)
    shape[axis] = 2 * shape[axis]
    return stacked.reshape(shape)


def const(values):
    return jnp.asarray(np.asarray(values, np.float32))


def dot(left, right, dims=((1,), (0,))):
    return lax.dot_general(
        left, right, (dims, ((), ())), precision=lax.Precision.HIGH,
        preferred_element_type=jnp.float32,
    )


def extended(block, axis, dim):
    size = lax.axis_size(axis)
    forward = [(i, (i + 1) % size) for i in range(size)]
    backward = [(target, source) for source, target in forward]
    low = lax.ppermute(lax.slice_in_dim(block, block.shape[dim] - 1, None, axis=dim), axis, forward)
    high = lax.ppermute(lax.slice_in_dim(block, 0, 2, axis=dim), axis, backward)
    return jnp.concatenate([low, block, high], axis=dim)


def refine_rim(haloed, axis, count):
    centre = lax.slice_in_dim(haloed, 1, 1 + count, axis=axis)
    before = lax.slice_in_dim(haloed, 0, count, axis=axis)
    after = lax.slice_in_dim(haloed, 2, 2 + count, axis=axis)
    after_two = lax.slice_in_dim(haloed, 3, 3 + count, axis=axis)
    middle = (9.0 * (centre + after) - (before + after_two)) / 16.0
    stacked = jnp.stack([centre, middle], axis=axis + 1)
    shape = list(centre.shape)
    shape[axis] = 2 * count
    return stacked.reshape(shape)


def plain(charges, kernel):
    planes, rows, count = kernel.shape
    replicas = charges.shape[2] // count
    half = replicas // 2
    blocks_z, blocks_y = lax.axis_size("gz"), lax.axis_size("gy")
    devices = blocks_z * blocks_y
    place = planes * rows
    columns = count * half // devices
    lines = max(1, columns // half)
    table_x = x_table(count, replicas, devices)
    table_y = const(y_table(count, planes, rows))
    cos_z = const(z_table(count, planes, columns, columns, 1, np.cos))
    sin_z = const(z_table(count, planes, columns, columns, 1, np.sin))
    cos_k = const(z_table(count, planes, columns, lines, half, np.cos) / count**3)
    sin_k = const(z_table(count, planes, columns, lines, half, np.sin) / count**3)

    sent = dot(const(table_x.reshape(-1, count * replicas)), charges.reshape(place, -1), ((1,), (1,)))
    sent_k = dot(const(x_kernel_table(count, replicas, devices)), kernel.reshape(place, count), ((1,), (1,)))
    both = jnp.concatenate(
        [sent.reshape(devices, 2 * columns, place), sent_k.reshape(devices, 2 * lines, place)], axis=1
    )
    both = lax.all_to_all(both, AXES, split_axis=0, concat_axis=0, tiled=True)

    def by_y(block, width):
        block = block.reshape(blocks_z, blocks_y, 2, width, place).transpose(0, 3, 2, 1, 4)
        block = dot(block.reshape(blocks_z * width, 2 * blocks_y * place), table_y)
        block = block.reshape(blocks_z * width, planes, 2 * count).transpose(1, 0, 2)
        return block.reshape(count * width, 2 * count)

    def swap(values):
        return jnp.concatenate([values[:, count:], values[:, :count]], axis=1)

    sign = jnp.where(lax.broadcasted_iota(jnp.int32, (1, 2 * count), 1) < count, 1.0, -1.0)
    data = by_y(both[:, : 2 * columns], columns)
    green = by_y(both[:, 2 * columns :], lines)
    data = dot(cos_z, data) + sign * swap(dot(sin_z, data))
    green = dot(cos_k, green) + sign * swap(dot(sin_k, green))
    real, imag = green[:, :count], green[:, count:]
    data = data * jnp.concatenate([real, real], axis=1) + swap(data) * jnp.concatenate([-imag, imag], axis=1)
    data = dot(cos_z, data) - sign * swap(dot(sin_z, data))
    data = data.reshape(planes, blocks_z * columns, 2 * count).transpose(1, 0, 2)
    data = dot(data.reshape(blocks_z * columns, planes * 2 * count), table_y, ((1,), (1,)))
    data = data.reshape(blocks_z, columns, 2, blocks_y, place).transpose(0, 3, 2, 1, 4)
    data = lax.all_to_all(
        data.reshape(devices, 2 * columns, place), AXES, split_axis=0, concat_axis=0, tiled=True
    )
    fine_x = const(refined(table_x, 1).reshape(-1, 2 * count * replicas))
    result = dot(data.reshape(devices * 2 * columns, place), fine_x, ((0,), (0,)))
    result = result.reshape(planes, rows, 2 * count * replicas)
    result = extended(extended(result, "gz", 0), "gy", 1)
    result = refine_rim(result, 0, planes)
    return refine_rim(result, 1, rows)


LANES = 128
MESH = pl.DeviceIdType.MESH


def table(values):
    high = np.asarray(values, np.float32).astype(jnp.bfloat16)
    low = (np.asarray(values, np.float64) - high.astype(np.float64)).astype(jnp.bfloat16)
    return [jnp.asarray(high), jnp.asarray(low)]


def split(values):
    high = values.astype(jnp.bfloat16)
    return high, (values - high.astype(jnp.float32)).astype(jnp.bfloat16)


def mul(left, right, dims=((1,), (0,))):
    return lax.dot_general(left, right, (dims, ((), ())), preferred_element_type=jnp.float32)


def mul3(left, right, dims=((1,), (0,))):
    (a, b), (c, d) = left, right
    return mul(a, d, dims) + mul(b, c, dims) + mul(a, c, dims)


GROUPS = 4
CHUNKS = 2


def mul3_rows(left, right):
    (a, b), (c, d) = left, right
    rows = a.shape[0]
    both = mul(jnp.concatenate([b, a], axis=0), c)
    return mul(a, d) + both[:rows] + both[rows:]


def line_of(device, chunk, count):
    flip = np.where(device == 0, count // 2, (count - device) % count)
    return np.where(chunk == 0, device, flip)


def pair_table(count, replicas, devices):
    half = replicas // 2
    chunk, device, part, row, x, side, pair = np.ix_(
        *(np.arange(s) for s in (CHUNKS, devices, 2, half, count, 2, half))
    )
    theta = angle(line_of(device, chunk, count), x, count)
    value = np.where(part == side, np.cos(theta), np.where(part == 0, np.sin(theta), -np.sin(theta)))
    value = value * (row == pair)
    return value.reshape(CHUNKS, devices * 2 * half, count, replicas)


def line_table(count, devices):
    device, row, x = np.ix_(*(np.arange(s) for s in (devices, 8, count)))
    theta = angle(device, x, count)
    other = np.where(device == 0, np.cos(angle(count // 2, x, count)), -np.sin(theta))
    value = np.where(row == 0, np.cos(theta), np.where(row == 1, other, 0.0))
    return value.reshape(devices * 8, count)


def stack3(values):
    high = np.asarray(values, np.float32).astype(jnp.bfloat16)
    low = (np.asarray(values, np.float64) - high.astype(np.float64)).astype(jnp.bfloat16)
    return jnp.asarray(np.concatenate([high, high, low], axis=1))


def z_tables(count, blocks):
    planes = count // blocks
    freq = np.arange(count)[:, None]
    place = np.arange(count)[None, :]
    theta = angle(freq, (place % blocks) * planes + place // blocks, count)
    forward = stack3(np.concatenate([np.cos(theta), np.sin(theta)], axis=0))
    inverse = stack3(np.concatenate([np.cos(theta.T), np.sin(theta.T)], axis=0))
    return forward, inverse


def remote(source, target, sems, place):
    return pltpu.make_async_remote_copy(
        src_ref=source, dst_ref=target, send_sem=sems.at[0], recv_sem=sems.at[1],
        device_id=place, device_id_type=MESH,
    )


def exchange(blocks_z, blocks_y, rows, source, target, sems):
    size = blocks_z * blocks_y // GROUPS
    devices = size * GROUPS
    me = lax.axis_index("gz") * blocks_y + lax.axis_index("gy")
    group, inner = me // size, lax.rem(me, size)
    high, low = group // 2, lax.rem(group, 2)
    turn = lax.rem(high + low, 2)
    pitch_from, pitch_to = source.shape[0] // devices, target.shape[0] // devices

    for flip_high, flip_low in ((1, 0), (1, 1), (0, 1), (0, 0)):
        far = lax.rem(high + flip_high + turn, 2) * 2 + lax.rem(low + flip_low + turn, 2)
        for step in range(size):
            other = far * size + lax.rem(inner + step, size)
            there = remote(
                source.at[pl.ds(pl.multiple_of(other * pitch_from, 8), rows)],
                target.at[pl.ds(pl.multiple_of(me * pitch_to, 8), rows)],
                sems, (other // blocks_y, lax.rem(other, blocks_y)),
            )
            if step == 0 and flip_high == flip_low:
                pl.when(other != me)(there.start)
            else:
                there.start()
    span = min(pitch_from, pitch_to)
    mine_from = pl.ds(pl.multiple_of(me * pitch_from, 8), span)
    target[pl.ds(pl.multiple_of(me * pitch_to, 8), span), :] = source[mine_from, :]
    other = lax.rem(me + 1, devices)
    count = pl.ds(0, (devices - 1) * rows)
    return remote(
        source.at[count], target.at[count], sems, (other // blocks_y, lax.rem(other, blocks_y))
    )


def swap_parts(values):
    half = LANES // 2
    pieces = [
        pltpu.roll(values[:, p : p + LANES], half, 1) for p in range(0, values.shape[1], LANES)
    ]
    return jnp.concatenate(pieces, axis=1)


def stacked(values):
    high, low = split(values)
    return jnp.concatenate([low, high, high], axis=0)


def repeat(values, times):
    return jnp.concatenate([values] * times, axis=1)


def y_lines(ref, start, stride, blocks):
    return ref[pl.ds(start, blocks, stride=stride), :]


def middle_stage(sizes, held, table_y, table_b, forward, inverse, green, back):
    count, blocks_z, blocks_y, half = sizes
    planes = count // blocks_z
    pitch = held.shape[0] // (blocks_z * blocks_y)
    lane = lax.broadcasted_iota(jnp.int32, (1, LANES), 1)
    sign = jnp.where(lane < count, 1.0, -1.0)

    def gather(row):
        pieces = [y_lines(held, y * pitch + row, blocks_y * pitch, blocks_z) for y in range(blocks_y)]
        return jnp.concatenate(pieces, axis=1)

    lines = [
        jnp.concatenate([gather(column), gather(half + column)], axis=1) for column in range(half)
    ]
    if green is None:
        me = lax.axis_index("gz") * blocks_y + lax.axis_index("gy")
        keep = jnp.where(me == 0, 0.0, 1.0).astype(jnp.float32)
        first, second = gather(2 * half), gather(2 * half + 1)
        lines.append(jnp.concatenate([first, keep * second], axis=1))
        lines.append(
            jnp.concatenate([keep * first + (1.0 - keep) * second, -keep * second], axis=1)
        )
    width = len(lines)
    data = mul3_rows(split(jnp.concatenate(lines, axis=0)), table_y)
    data = jnp.concatenate(
        [
            jnp.concatenate(
                [
                    data[c * blocks_z : (c + 1) * blocks_z, p * LANES : (p + 1) * LANES]
                    for p in range(planes)
                ],
                axis=0,
            )
            for c in range(width)
        ],
        axis=1,
    )
    both = mul(forward, stacked(data))
    data = both[:count] + repeat(sign, width) * swap_parts(both[count:])
    spectra = None
    if green is None:
        scaled = data[:, half * LANES :] * (1.0 / count**3)
        green, spectra = scaled[:, :LANES], scaled
        data = data[:, : half * LANES]
    other = swap_parts(green)
    real = jnp.where(lane < count, green, other)
    imag = jnp.where(lane < count, -other, green)
    data = data * repeat(real, half) + swap_parts(data) * repeat(imag, half)
    both = mul(inverse, stacked(data))
    data = both[:count] - repeat(sign, half) * swap_parts(both[count:])
    data = jnp.concatenate(
        [
            jnp.concatenate(
                [
                    data[p * blocks_z : (p + 1) * blocks_z, c * LANES : (c + 1) * LANES]
                    for p in range(planes)
                ],
                axis=1,
            )
            for c in range(half)
        ],
        axis=0,
    )
    data = mul3_rows(split(data), table_b)
    out_pitch = 2 * half
    for column in range(half):
        for part in range(2):
            for y in range(blocks_y):
                at = (part * blocks_y + y) * LANES
                back[pl.ds(y * out_pitch + part * half + column, blocks_z, stride=blocks_y * out_pitch), :] = (
                    data[column * blocks_z : (column + 1) * blocks_z, at : at + LANES]
                )
    return spectra


def send_rims(blocks_z, blocks_y, planes, rows, own, sizes, stage, rims, sems):
    to_up, to_down, to_corner = stage
    low_z, high_z, low_y, high_y, corner = rims
    gz, gy = lax.axis_index("gz"), lax.axis_index("gy")
    next_z, last_z = lax.rem(gz + 1, blocks_z), lax.rem(gz + blocks_z - 1, blocks_z)
    next_y, last_y = lax.rem(gy + 1, blocks_y), lax.rem(gy + blocks_y - 1, blocks_y)
    end = (planes - 1) * rows
    def side(row):
        return jnp.concatenate([own[p * rows + row : p * rows + row + 1, :] for p in range(planes)], axis=0)

    to_up[...] = side(rows - 1)
    to_down[...] = jnp.concatenate([side(0), side(1)], axis=0)
    picks = (
        (end + rows - 1,), (end, end + 1), (rows - 1, 2 * rows - 1), (0, 1, rows, rows + 1),
    )
    for number, pick in enumerate(picks):
        pieces = [own[r : r + 1, :] for r in pick]
        pieces.append(jnp.zeros((8 - len(pick), own.shape[1]), jnp.float32))
        to_corner[number] = jnp.concatenate(pieces, axis=0)
    places = ((next_z, next_y), (next_z, last_y), (last_z, next_y), (last_z, last_y))
    copies = []
    for number, (pick, place) in enumerate(zip(picks, places)):
        span = pl.ds(0, len(pick))
        copies.append(
            remote(to_corner.at[number, span], corner.at[number, span], sems, place)
        )
    for copy in copies:
        copy.start()
    down = remote(own.at[pl.ds(0, 2 * rows)], high_z, sems, (last_z, gy))
    up = remote(own.at[pl.ds(end, rows)], low_z, sems, (next_z, gy))
    pl.when(gz == 0)(down.start)
    up.start()
    pl.when(gz != 0)(down.start)
    sides = [
        remote(to_up, low_y, sems, (gz, next_y)), remote(to_down, high_y, sems, (gz, last_y)),
    ]
    for copy in sides:
        copy.start()
    count = pl.ds(0, 3 * (planes + rows + 3) * own.shape[1] // LANES)
    return remote(sizes[0].at[count], sizes[1].at[count], sems, (next_z, gy))


def rim_lines(planes, rims):
    low_z, high_z, low_y, high_y, corner = rims
    empty = jnp.zeros((5, low_z.shape[1]), jnp.float32)
    tiles = [corner[0, 0:1, :], corner[1, 0:2, :], empty]
    for p in range(planes):
        tiles += [
            low_y[p : p + 1, :], high_y[p : p + 1, :], high_y[planes + p : planes + p + 1, :], empty,
        ]
    tiles += [corner[2, 0:1, :], corner[3, 0:2, :], empty]
    tiles += [corner[2, 1:2, :], corner[3, 2:4, :], empty]
    tiles += [jnp.zeros((8, low_z.shape[1]), jnp.float32)]
    return jnp.concatenate([low_z[...], high_z[...], *tiles], axis=0)


def main_kernel(sizes, *refs):
    count, blocks_z, blocks_y, half, n_tables = sizes
    devices = blocks_z * blocks_y
    planes = count // blocks_z
    sources = refs[: 2 + n_tables]
    out = refs[2 + n_tables]
    loaded = refs[3 + n_tables : 5 + 2 * n_tables]
    (q_ref, k_ref), tables = loaded[:2], loaded[2:]
    rest = list(refs[5 + 2 * n_tables :])
    load_sem, sent_sem, back_sem, rim_sem, out_sem, total, packed = rest[:7]
    sent, held, back, home, own = (rest[7 + 2 * i : 9 + 2 * i] for i in range(5))
    stages, rims = (rest[17:20], rest[20:23]), (rest[23:28], rest[28:33])
    table_k, table_x, table_y, table_b, table_z, table_f = (
        tables[0:2], tables[2:4], tables[4:6], tables[6:8], tables[8:10], tables[10:14]
    )
    me = lax.axis_index("gz") * blocks_y + lax.axis_index("gy")
    barrier = pltpu.get_barrier_semaphore()
    for step in range(1, devices):
        other = lax.rem(me + step, devices)
        pl.semaphore_signal(
            barrier, inc=1, device_id=(other // blocks_y, lax.rem(other, blocks_y)), device_id_type=MESH
        )
    loads = [
        pltpu.make_async_copy(s, t, load_sem.at[i]) for i, (s, t) in enumerate(zip(sources, loaded))
    ]
    for load in loads[:5]:
        load.start()
    rows = q_ref.shape[0] // planes
    size = 2 * half
    pitch = sent[0].shape[0] // devices

    def x_lines(chunk, charges):
        per = LANES // size
        for group in range(devices // per):
            both = mul(table_x[chunk][group * 2 * LANES : (group + 1) * 2 * LANES, :], charges, ((1,), (1,)))
            made = both[:LANES, :LANES] + both[:LANES, LANES:] + both[LANES:, :LANES]
            step = sent[chunk].shape[0] // devices
            for inner in range(per):
                at = (group * per + inner) * step
                sent[chunk][at : at + size, :] = made[inner * size : (inner + 1) * size, :]

    scope = jax.named_scope
    with scope("kernel_lines"):
        for load in loads[1:4]:
            load.wait()
        lines = mul3((table_k[0][...], table_k[1][...]), split(k_ref[...]), ((1,), (1,)))
        for device in range(devices):
            at = device * pitch + size
            sent[0][at : at + 8, :] = lines[device * 8 : (device + 1) * 8, :]
    with scope("x_load"):
        loads[0].wait()
        loads[4].wait()
        for load in loads[5:]:
            load.start()
    with scope("x_lines0"):
        charges = jnp.concatenate(split(q_ref[...]), axis=0)
        x_lines(0, charges)
    with scope("barrier"):
        pl.semaphore_wait(barrier, devices - 1)
    with scope("send0"):
        there = [exchange(blocks_z, blocks_y, size + 2, sent[0], held[0], sent_sem.at[0])]
    with scope("x_lines1"):
        loads[5].wait()
        x_lines(1, charges)
    with scope("send1"):
        there.append(exchange(blocks_z, blocks_y, size, sent[1], held[1], sent_sem.at[1]))
    with scope("wait_there0"):
        for load in loads[6:12]:
            load.wait()
        there[0].wait_recv()
    y_pairs = ((table_y[0][...], table_y[1][...]), (table_b[0][...], table_b[1][...]))
    z_pair = (table_z[0][...], table_z[1][...])
    shape = (count, blocks_z, blocks_y, half)
    with scope("middle0"):
        green = middle_stage(shape, held[0], *y_pairs, *z_pair, None, back[0])
    with scope("return0"):
        returns = [exchange(blocks_z, blocks_y, size, back[0], home[0], back_sem.at[0])]
    with scope("wait_there1"):
        there[1].wait_recv()
    with scope("middle1"):
        middle_stage(shape, held[1], *y_pairs, *z_pair, green[:, LANES:], back[1])
    with scope("return1"):
        returns.append(exchange(blocks_z, blocks_y, size, back[1], home[1], back_sem.at[1]))
    for load in loads[12:]:
        load.wait()
    borders = []
    fine = [(table_f[2 * c][...], table_f[2 * c + 1][...]) for c in range(CHUNKS)]
    for chunk in range(CHUNKS):
        with scope(f"wait_back{chunk}"):
            returns[chunk].wait_recv()
        with scope(f"turn{chunk}"):
            turned = jnp.transpose(home[chunk][...])
            own[chunk][...] = turned
        with scope(f"send_rim{chunk}"):
            borders.append(send_rims(
                blocks_z, blocks_y, planes, rows, own[chunk], home, stages[chunk], rims[chunk], rim_sem.at[chunk]
            ))
        with scope(f"own{chunk}"):
            made = mul3_rows(split(turned), fine[chunk]).reshape(planes, rows, -1)
            if chunk:
                made = total[1 : planes + 1, :rows, :] + made
            total[1 : planes + 1, :rows, :] = made
    flat = 3 * rows

    def pack_own(first, last):
        values = total[first:last, :rows, :]
        high, low = split(values)
        packed[first:last, :rows, :] = high
        packed[first:last, rows : 2 * rows, :] = low

    pack_own(1, planes + 1)
    inside, around = (pl.ds(1, planes), pl.ds(0, 2 * rows)), (pl.ds(0, planes + 3), pl.ds(2 * rows, 16))
    first, last = (pl.ds(0, 1), pl.ds(0, 2 * rows)), (pl.ds(planes + 1, 2), pl.ds(0, 2 * rows))
    stores = [
        pltpu.make_async_copy(packed.at[span], out.at[span], out_sem.at[i])
        for i, span in enumerate((inside, around, first, last))
    ]
    stores[0].start()
    for chunk in range(CHUNKS):
        with scope(f"wait_rim{chunk}"):
            borders[chunk].wait_recv()
        with scope(f"rim{chunk}"):
            made = mul3_rows(split(rim_lines(planes, rims[chunk])), fine[chunk])
            sides = 8 * (planes + 3)
            ends = made[:flat].reshape(3, rows, -1)
            sides = made[flat : flat + sides].reshape(planes + 3, 8, -1)
            if not chunk:
                total[:, rows:, :] = sides
                total[0:1, :rows, :] = ends[0:1]
                total[planes + 1 :, :rows, :] = ends[1:]
                continue
            sides = total[:, rows:, :] + sides
            high = sides.astype(jnp.bfloat16).astype(jnp.float32)
            packed[:, 2 * rows :, :] = jnp.concatenate([high, sides - high], axis=1).astype(jnp.bfloat16)
            stores[1].start()
            for i, place in enumerate((0, planes + 1, planes + 2)):
                high, low = split(total[place, :rows, :] + ends[i])
                packed[place, :rows, :] = high
                packed[place, rows : 2 * rows, :] = low
    for store in stores[2:]:
        store.start()
    with scope("wait_sends"):
        for copy in there + returns + borders:
            copy.wait_send()
        for store in stores:
            store.wait()


def refine_kernel(x_ref, r_ref, o_ref, held, made, sem, out_sem):
    planes = x_ref.shape[0] - 3
    loads = [
        pltpu.make_async_copy(x_ref.at[p], held.at[p], sem.at[p]) for p in range(planes + 3)
    ]
    for load in loads:
        load.start()
    for load in loads[:3]:
        load.wait()
    stores = []
    for p in range(planes):
        loads[p + 3].wait()
        near = held[p : p + 4].reshape(4 * held.shape[1], held.shape[2])
        made[2 * p : 2 * p + 2] = mul(r_ref[...], near).reshape(2, -1, made.shape[2])
        span = pl.ds(2 * p, 2)
        stores.append(pltpu.make_async_copy(made.at[span], o_ref.at[span], out_sem.at[p]))
        stores[-1].start()
    for store in stores:
        store.wait()


def rim_table(count):
    made = np.zeros((2 * count, count + 3))
    for i in range(count):
        made[2 * i, i + 1] = 1.0
        made[2 * i + 1, i : i + 4] = np.array([-1.0, 9.0, 9.0, -1.0]) / 16.0
    return made


def refine(haloed, planes, rows, width):
    along_y = rim_table(rows)
    middle = along_y[:, 1 : rows + 1]
    sides = np.concatenate([along_y[:, :1], along_y[:, rows + 1 :], np.zeros((2 * rows, 5))], axis=1)
    along_y = np.concatenate([middle, middle, sides, sides], axis=1)
    both = jnp.asarray(np.kron(rim_table(1), along_y), jnp.bfloat16)
    shape = (2 * planes, 2 * rows, width)
    return pl.pallas_call(
        refine_kernel,
        out_shape=jax.ShapeDtypeStruct(shape, jnp.float32),
        in_specs=[
            pl.BlockSpec(memory_space=pl.ANY),
            pl.BlockSpec(memory_space=pltpu.VMEM),
        ],
        out_specs=pl.BlockSpec(memory_space=pl.ANY),
        scratch_shapes=[
            pltpu.VMEM(haloed.shape, haloed.dtype), pltpu.VMEM(shape, jnp.float32),
            pltpu.SemaphoreType.DMA((planes + 3,)), pltpu.SemaphoreType.DMA((planes,)),
        ],
    )(haloed, both)


def per_device(charges, kernel):
    planes, rows, count = kernel.shape
    width = charges.shape[2]
    replicas = width // count
    half = replicas // 2
    blocks_z, blocks_y = lax.axis_size("gz"), lax.axis_size("gy")
    devices = blocks_z * blocks_y
    place = planes * rows
    fits = place == LANES and 2 * count == LANES and half == 8 and blocks_z == 8
    if not fits or count != CHUNKS * devices or replicas % 2 or rows != 16 or planes != 8 or devices % 8:
        return plain(charges, kernel)
    size = 2 * half
    per = LANES // size
    lines_x = pair_table(count, replicas, devices)
    table_x, table_f = [], []
    for chunk in range(CHUNKS):
        high, low = table(lines_x[chunk].reshape(devices // per, LANES, width))
        table_x.append(jnp.concatenate([high, low], axis=1).reshape(-1, width))
        table_f += table(refined(lines_x[chunk], 1).reshape(-1, 2 * width))
    lines_y = y_table(count, planes, rows)
    tables = [
        *table(line_table(count, devices)), *table_x, *table(lines_y), *table(lines_y.T),
        *z_tables(count, blocks_z), *table_f,
    ]
    arrays = [charges.reshape(place, width), kernel.reshape(place, count), *tables]
    deep = devices * size
    block = lambda *shape: pltpu.VMEM(shape, jnp.float32)
    dma = pltpu.SemaphoreType.DMA
    stage = [block(planes, deep), block(2 * planes, deep), block(4, 8, deep)]
    rim = [
        block(rows, deep), block(2 * rows, deep), block(planes, deep), block(2 * planes, deep),
        block(4, 8, deep),
    ]
    haloed = pl.pallas_call(
        functools.partial(main_kernel, (count, blocks_z, blocks_y, half, len(tables))),
        out_shape=jax.ShapeDtypeStruct((planes + 3, 3 * rows, 2 * width), jnp.bfloat16),
        in_specs=[pl.BlockSpec(memory_space=pl.ANY)] * len(arrays),
        out_specs=pl.BlockSpec(memory_space=pl.ANY),
        scratch_shapes=[
            *(pltpu.VMEM(a.shape, a.dtype) for a in arrays),
            dma((len(arrays),)), dma((CHUNKS, 2)), dma((CHUNKS, 2)), dma((CHUNKS, 2)),
            dma((4,)), block(planes + 3, rows + 8, 2 * width),
            pltpu.VMEM((planes + 3, 3 * rows, 2 * width), jnp.bfloat16),
            block(devices * (size + 8), LANES), block(deep, LANES),
            block(devices * (size + 8), LANES), block(deep, LANES),
            block(deep, LANES), block(deep, LANES),
            block(deep, LANES), block(deep, LANES),
            block(place, deep), block(place, deep),
            *stage, *stage, *rim, *rim,
        ],
        compiler_params=pltpu.CompilerParams(
            collective_id=0, has_side_effects=True, vmem_limit_bytes=60 * 1024 * 1024
        ),
    )(*arrays)
    return refine(haloed, planes, rows, 2 * width)


def solution(mesh):
    placed = (P("gz", "gy", None), P("gz", "gy", None))
    return jax.shard_map(
        per_device, mesh=mesh, in_specs=placed, out_specs=P("gz", "gy", None), check_vma=False
    )
```

```python
import functools

import jax
import jax.numpy as jnp
import numpy as np
from jax import lax
from jax.experimental import pallas as pl
from jax.experimental.pallas import tpu as pltpu
from jax.sharding import PartitionSpec as P

AXES = ("gz", "gy")


def angle(first, second, count):
    return 2.0 * np.pi / count * ((first * second) % count)


def x_table(count, replicas, devices):
    half = replicas // 2
    columns = count * half // devices
    device, part, column, x, side, pair = np.ix_(
        *(np.arange(s) for s in (devices, 2, columns, count, 2, half))
    )
    flat = device * columns + column
    theta = angle(flat // half, x, count)
    value = np.where(part == side, np.cos(theta), np.where(part == 0, np.sin(theta), -np.sin(theta)))
    value = value * (flat % half == pair)
    return value.reshape(devices * 2 * columns, count, replicas)


def x_kernel_table(count, replicas, devices):
    half = replicas // 2
    columns = count * half // devices
    lines = max(1, columns // half)
    device, part, line, x = np.ix_(*(np.arange(s) for s in (devices, 2, lines, count)))
    theta = angle(device * columns // half + line, x, count)
    value = np.where(part == 0, np.cos(theta), -np.sin(theta))
    return value.reshape(devices * 2 * lines, count)


def y_table(count, planes, rows):
    part, block, plane, row, new_plane, new_part, freq = np.ix_(
        *(np.arange(s) for s in (2, count // rows, planes, rows, planes, 2, count))
    )
    theta = angle(block * rows + row, freq, count)
    value = np.where(
        part == new_part, np.cos(theta), np.where(new_part == 0, np.sin(theta), -np.sin(theta))
    )
    value = value * (plane == new_plane)
    return value.reshape(2 * count * planes, planes * 2 * count)


def z_table(count, planes, columns, lines, group, wave):
    blocks = count // planes
    low, high, column, z_low, z_high, line = np.ix_(
        *(np.arange(s) for s in (planes, blocks, columns, planes, blocks, lines))
    )
    theta = angle(high * planes + low, z_high * planes + z_low, count)
    value = wave(theta) * (column // group == line)
    return value.reshape(count * columns, count * lines)


def refined(values, axis):
    before = np.roll(values, 1, axis)
    after = np.roll(values, -1, axis)
    after_two = np.roll(values, -2, axis)
    middle = (9.0 * (values + after) - (before + after_two)) / 16.0
    stacked = np.stack([values, middle], axis=axis + 1)
    shape = list(values.shape)
    shape[axis] = 2 * shape[axis]
    return stacked.reshape(shape)


def const(values):
    return jnp.asarray(np.asarray(values, np.float32))


def dot(left, right, dims=((1,), (0,))):
    return lax.dot_general(
        left, right, (dims, ((), ())), precision=lax.Precision.HIGH,
        preferred_element_type=jnp.float32,
    )


def extended(block, axis, dim):
    size = lax.axis_size(axis)
    forward = [(i, (i + 1) % size) for i in range(size)]
    backward = [(target, source) for source, target in forward]
    low = lax.ppermute(lax.slice_in_dim(block, block.shape[dim] - 1, None, axis=dim), axis, forward)
    high = lax.ppermute(lax.slice_in_dim(block, 0, 2, axis=dim), axis, backward)
    return jnp.concatenate([low, block, high], axis=dim)


def refine_rim(haloed, axis, count):
    centre = lax.slice_in_dim(haloed, 1, 1 + count, axis=axis)
    before = lax.slice_in_dim(haloed, 0, count, axis=axis)
    after = lax.slice_in_dim(haloed, 2, 2 + count, axis=axis)
    after_two = lax.slice_in_dim(haloed, 3, 3 + count, axis=axis)
    middle = (9.0 * (centre + after) - (before + after_two)) / 16.0
    stacked = jnp.stack([centre, middle], axis=axis + 1)
    shape = list(centre.shape)
    shape[axis] = 2 * count
    return stacked.reshape(shape)


def plain(charges, kernel):
    planes, rows, count = kernel.shape
    replicas = charges.shape[2] // count
    half = replicas // 2
    blocks_z, blocks_y = lax.axis_size("gz"), lax.axis_size("gy")
    devices = blocks_z * blocks_y
    place = planes * rows
    columns = count * half // devices
    lines = max(1, columns // half)
    table_x = x_table(count, replicas, devices)
    table_y = const(y_table(count, planes, rows))
    cos_z = const(z_table(count, planes, columns, columns, 1, np.cos))
    sin_z = const(z_table(count, planes, columns, columns, 1, np.sin))
    cos_k = const(z_table(count, planes, columns, lines, half, np.cos) / count**3)
    sin_k = const(z_table(count, planes, columns, lines, half, np.sin) / count**3)

    sent = dot(const(table_x.reshape(-1, count * replicas)), charges.reshape(place, -1), ((1,), (1,)))
    sent_k = dot(const(x_kernel_table(count, replicas, devices)), kernel.reshape(place, count), ((1,), (1,)))
    both = jnp.concatenate(
        [sent.reshape(devices, 2 * columns, place), sent_k.reshape(devices, 2 * lines, place)], axis=1
    )
    both = lax.all_to_all(both, AXES, split_axis=0, concat_axis=0, tiled=True)

    def by_y(block, width):
        block = block.reshape(blocks_z, blocks_y, 2, width, place).transpose(0, 3, 2, 1, 4)
        block = dot(block.reshape(blocks_z * width, 2 * blocks_y * place), table_y)
        block = block.reshape(blocks_z * width, planes, 2 * count).transpose(1, 0, 2)
        return block.reshape(count * width, 2 * count)

    def swap(values):
        return jnp.concatenate([values[:, count:], values[:, :count]], axis=1)

    sign = jnp.where(lax.broadcasted_iota(jnp.int32, (1, 2 * count), 1) < count, 1.0, -1.0)
    data = by_y(both[:, : 2 * columns], columns)
    green = by_y(both[:, 2 * columns :], lines)
    data = dot(cos_z, data) + sign * swap(dot(sin_z, data))
    green = dot(cos_k, green) + sign * swap(dot(sin_k, green))
    real, imag = green[:, :count], green[:, count:]
    data = data * jnp.concatenate([real, real], axis=1) + swap(data) * jnp.concatenate([-imag, imag], axis=1)
    data = dot(cos_z, data) - sign * swap(dot(sin_z, data))
    data = data.reshape(planes, blocks_z * columns, 2 * count).transpose(1, 0, 2)
    data = dot(data.reshape(blocks_z * columns, planes * 2 * count), table_y, ((1,), (1,)))
    data = data.reshape(blocks_z, columns, 2, blocks_y, place).transpose(0, 3, 2, 1, 4)
    data = lax.all_to_all(
        data.reshape(devices, 2 * columns, place), AXES, split_axis=0, concat_axis=0, tiled=True
    )
    fine_x = const(refined(table_x, 1).reshape(-1, 2 * count * replicas))
    result = dot(data.reshape(devices * 2 * columns, place), fine_x, ((0,), (0,)))
    result = result.reshape(planes, rows, 2 * count * replicas)
    result = extended(extended(result, "gz", 0), "gy", 1)
    result = refine_rim(result, 0, planes)
    return refine_rim(result, 1, rows)


LANES = 128
MESH = pl.DeviceIdType.MESH


def table(values):
    high = np.asarray(values, np.float32).astype(jnp.bfloat16)
    low = (np.asarray(values, np.float64) - high.astype(np.float64)).astype(jnp.bfloat16)
    return [jnp.asarray(high), jnp.asarray(low)]


def split(values):
    high = values.astype(jnp.bfloat16)
    return high, (values - high.astype(jnp.float32)).astype(jnp.bfloat16)


def mul(left, right, dims=((1,), (0,))):
    return lax.dot_general(left, right, (dims, ((), ())), preferred_element_type=jnp.float32)


def mul3(left, right, dims=((1,), (0,))):
    (a, b), (c, d) = left, right
    return mul(a, d, dims) + mul(b, c, dims) + mul(a, c, dims)


GROUPS = 4
CHUNKS = 2


def mul3_rows(left, right):
    (a, b), (c, d) = left, right
    rows = a.shape[0]
    both = mul(jnp.concatenate([b, a], axis=0), c)
    return mul(a, d) + both[:rows] + both[rows:]


def line_of(device, chunk, count):
    flip = np.where(device == 0, count // 2, (count - device) % count)
    return np.where(chunk == 0, device, flip)


def pair_table(count, replicas, devices):
    half = replicas // 2
    chunk, device, part, row, x, side, pair = np.ix_(
        *(np.arange(s) for s in (CHUNKS, devices, 2, half, count, 2, half))
    )
    theta = angle(line_of(device, chunk, count), x, count)
    value = np.where(part == side, np.cos(theta), np.where(part == 0, np.sin(theta), -np.sin(theta)))
    value = value * (row == pair)
    return value.reshape(CHUNKS, devices * 2 * half, count, replicas)


def line_table(count, devices):
    device, row, x = np.ix_(*(np.arange(s) for s in (devices, 8, count)))
    theta = angle(device, x, count)
    other = np.where(device == 0, np.cos(angle(count // 2, x, count)), -np.sin(theta))
    value = np.where(row == 0, np.cos(theta), np.where(row == 1, other, 0.0))
    return value.reshape(devices * 8, count)


def stack3(values):
    high = np.asarray(values, np.float32).astype(jnp.bfloat16)
    low = (np.asarray(values, np.float64) - high.astype(np.float64)).astype(jnp.bfloat16)
    return jnp.asarray(np.concatenate([high, high, low], axis=1))


def z_tables(count, blocks):
    planes = count // blocks
    freq = np.arange(count)[:, None]
    place = np.arange(count)[None, :]
    theta = angle(freq, (place % blocks) * planes + place // blocks, count)
    forward = stack3(np.concatenate([np.cos(theta), np.sin(theta)], axis=0))
    inverse = stack3(np.concatenate([np.cos(theta.T), np.sin(theta.T)], axis=0))
    return forward, inverse


def remote(source, target, sems, place):
    return pltpu.make_async_remote_copy(
        src_ref=source, dst_ref=target, send_sem=sems.at[0], recv_sem=sems.at[1],
        device_id=place, device_id_type=MESH,
    )


def exchange(blocks_z, blocks_y, rows, source, target, sems):
    size = blocks_z * blocks_y // GROUPS
    devices = size * GROUPS
    me = lax.axis_index("gz") * blocks_y + lax.axis_index("gy")
    group, inner = me // size, lax.rem(me, size)
    high, low = group // 2, lax.rem(group, 2)
    turn = lax.rem(high + low, 2)
    pitch_from, pitch_to = source.shape[0] // devices, target.shape[0] // devices

    for flip_high, flip_low in ((1, 0), (1, 1), (0, 1), (0, 0)):
        far = lax.rem(high + flip_high + turn, 2) * 2 + lax.rem(low + flip_low + turn, 2)
        for step in range(size):
            other = far * size + lax.rem(inner + step, size)
            there = remote(
                source.at[pl.ds(pl.multiple_of(other * pitch_from, 8), rows)],
                target.at[pl.ds(pl.multiple_of(me * pitch_to, 8), rows)],
                sems, (other // blocks_y, lax.rem(other, blocks_y)),
            )
            if step == 0 and flip_high == flip_low:
                pl.when(other != me)(there.start)
            else:
                there.start()
    span = min(pitch_from, pitch_to)
    mine_from = pl.ds(pl.multiple_of(me * pitch_from, 8), span)
    target[pl.ds(pl.multiple_of(me * pitch_to, 8), span), :] = source[mine_from, :]
    other = lax.rem(me + 1, devices)
    count = pl.ds(0, (devices - 1) * rows)
    return remote(
        source.at[count], target.at[count], sems, (other // blocks_y, lax.rem(other, blocks_y))
    )


def swap_parts(values):
    half = LANES // 2
    pieces = [
        pltpu.roll(values[:, p : p + LANES], half, 1) for p in range(0, values.shape[1], LANES)
    ]
    return jnp.concatenate(pieces, axis=1)


def stacked(values):
    high, low = split(values)
    return jnp.concatenate([low, high, high], axis=0)


def repeat(values, times):
    return jnp.concatenate([values] * times, axis=1)


def y_lines(ref, start, stride, blocks):
    return ref[pl.ds(start, blocks, stride=stride), :]


def middle_stage(sizes, held, table_y, table_b, forward, inverse, green, back):
    count, blocks_z, blocks_y, half = sizes
    planes = count // blocks_z
    pitch = held.shape[0] // (blocks_z * blocks_y)
    lane = lax.broadcasted_iota(jnp.int32, (1, LANES), 1)
    sign = jnp.where(lane < count, 1.0, -1.0)

    def gather(row):
        pieces = [y_lines(held, y * pitch + row, blocks_y * pitch, blocks_z) for y in range(blocks_y)]
        return jnp.concatenate(pieces, axis=1)

    lines = [
        jnp.concatenate([gather(column), gather(half + column)], axis=1) for column in range(half)
    ]
    if green is None:
        me = lax.axis_index("gz") * blocks_y + lax.axis_index("gy")
        keep = jnp.where(me == 0, 0.0, 1.0).astype(jnp.float32)
        first, second = gather(2 * half), gather(2 * half + 1)
        lines.append(jnp.concatenate([first, keep * second], axis=1))
        lines.append(
            jnp.concatenate([keep * first + (1.0 - keep) * second, -keep * second], axis=1)
        )
    width = len(lines)
    data = mul3_rows(split(jnp.concatenate(lines, axis=0)), table_y)
    data = jnp.concatenate(
        [
            jnp.concatenate(
                [
                    data[c * blocks_z : (c + 1) * blocks_z, p * LANES : (p + 1) * LANES]
                    for p in range(planes)
                ],
                axis=0,
            )
            for c in range(width)
        ],
        axis=1,
    )
    both = mul(forward, stacked(data))
    data = both[:count] + repeat(sign, width) * swap_parts(both[count:])
    spectra = None
    if green is None:
        scaled = data[:, half * LANES :] * (1.0 / count**3)
        green, spectra = scaled[:, :LANES], scaled
        data = data[:, : half * LANES]
    other = swap_parts(green)
    real = jnp.where(lane < count, green, other)
    imag = jnp.where(lane < count, -other, green)
    data = data * repeat(real, half) + swap_parts(data) * repeat(imag, half)
    both = mul(inverse, stacked(data))
    data = both[:count] - repeat(sign, half) * swap_parts(both[count:])
    data = jnp.concatenate(
        [
            jnp.concatenate(
                [
                    data[p * blocks_z : (p + 1) * blocks_z, c * LANES : (c + 1) * LANES]
                    for p in range(planes)
                ],
                axis=1,
            )
            for c in range(half)
        ],
        axis=0,
    )
    data = mul3_rows(split(data), table_b)
    out_pitch = 2 * half
    for column in range(half):
        for part in range(2):
            for y in range(blocks_y):
                at = (part * blocks_y + y) * LANES
                back[pl.ds(y * out_pitch + part * half + column, blocks_z, stride=blocks_y * out_pitch), :] = (
                    data[column * blocks_z : (column + 1) * blocks_z, at : at + LANES]
                )
    return spectra


def send_rims(blocks_z, blocks_y, planes, rows, own, sizes, stage, rims, sems):
    to_up, to_down, to_corner = stage
    low_z, high_z, low_y, high_y, corner = rims
    gz, gy = lax.axis_index("gz"), lax.axis_index("gy")
    next_z, last_z = lax.rem(gz + 1, blocks_z), lax.rem(gz + blocks_z - 1, blocks_z)
    next_y, last_y = lax.rem(gy + 1, blocks_y), lax.rem(gy + blocks_y - 1, blocks_y)
    end = (planes - 1) * rows
    def side(row):
        return jnp.concatenate([own[p * rows + row : p * rows + row + 1, :] for p in range(planes)], axis=0)

    to_up[...] = side(rows - 1)
    to_down[...] = jnp.concatenate([side(0), side(1)], axis=0)
    picks = (
        (end + rows - 1,), (end, end + 1), (rows - 1, 2 * rows - 1), (0, 1, rows, rows + 1),
    )
    for number, pick in enumerate(picks):
        pieces = [own[r : r + 1, :] for r in pick]
        pieces.append(jnp.zeros((8 - len(pick), own.shape[1]), jnp.float32))
        to_corner[number] = jnp.concatenate(pieces, axis=0)
    places = ((next_z, next_y), (next_z, last_y), (last_z, next_y), (last_z, last_y))
    copies = []
    for number, (pick, place) in enumerate(zip(picks, places)):
        span = pl.ds(0, len(pick))
        copies.append(
            remote(to_corner.at[number, span], corner.at[number, span], sems, place)
        )
    for copy in copies:
        copy.start()
    down = remote(own.at[pl.ds(0, 2 * rows)], high_z, sems, (last_z, gy))
    up = remote(own.at[pl.ds(end, rows)], low_z, sems, (next_z, gy))
    pl.when(gz == 0)(down.start)
    up.start()
    pl.when(gz != 0)(down.start)
    sides = [
        remote(to_up, low_y, sems, (gz, next_y)), remote(to_down, high_y, sems, (gz, last_y)),
    ]
    for copy in sides:
        copy.start()
    count = pl.ds(0, 3 * (planes + rows + 3) * own.shape[1] // LANES)
    return remote(sizes[0].at[count], sizes[1].at[count], sems, (next_z, gy))


def rim_lines(planes, rims):
    low_z, high_z, low_y, high_y, corner = rims
    empty = jnp.zeros((5, low_z.shape[1]), jnp.float32)
    tiles = [corner[0, 0:1, :], corner[1, 0:2, :], empty]
    for p in range(planes):
        tiles += [
            low_y[p : p + 1, :], high_y[p : p + 1, :], high_y[planes + p : planes + p + 1, :], empty,
        ]
    tiles += [corner[2, 0:1, :], corner[3, 0:2, :], empty]
    tiles += [corner[2, 1:2, :], corner[3, 2:4, :], empty]
    tiles += [jnp.zeros((8, low_z.shape[1]), jnp.float32)]
    return jnp.concatenate([low_z[...], high_z[...], *tiles], axis=0)


def main_kernel(sizes, *refs):
    count, blocks_z, blocks_y, half, n_tables = sizes
    devices = blocks_z * blocks_y
    planes = count // blocks_z
    sources = refs[: 2 + n_tables]
    packed = refs[2 + n_tables]
    loaded = refs[3 + n_tables : 5 + 2 * n_tables]
    (q_ref, k_ref), tables = loaded[:2], loaded[2:]
    rest = list(refs[5 + 2 * n_tables :])
    load_sem, sent_sem, back_sem, rim_sem, total = rest[:5]
    sent, held, back, home, own = (rest[5 + 2 * i : 7 + 2 * i] for i in range(5))
    stages, rims = (rest[15:18], rest[18:21]), (rest[21:26], rest[26:31])
    table_k, table_x, table_y, table_b, table_z, table_f = (
        tables[0:2], tables[2:4], tables[4:6], tables[6:8], tables[8:10], tables[10:14]
    )
    me = lax.axis_index("gz") * blocks_y + lax.axis_index("gy")
    barrier = pltpu.get_barrier_semaphore()
    for step in range(1, devices):
        other = lax.rem(me + step, devices)
        pl.semaphore_signal(
            barrier, inc=1, device_id=(other // blocks_y, lax.rem(other, blocks_y)), device_id_type=MESH
        )
    loads = [
        pltpu.make_async_copy(s, t, load_sem.at[i]) for i, (s, t) in enumerate(zip(sources, loaded))
    ]
    for load in loads[:5]:
        load.start()
    rows = q_ref.shape[0] // planes
    size = 2 * half
    pitch = sent[0].shape[0] // devices

    def x_lines(chunk, charges):
        per = LANES // size
        for group in range(devices // per):
            both = mul(table_x[chunk][group * 2 * LANES : (group + 1) * 2 * LANES, :], charges, ((1,), (1,)))
            made = both[:LANES, :LANES] + both[:LANES, LANES:] + both[LANES:, :LANES]
            step = sent[chunk].shape[0] // devices
            for inner in range(per):
                at = (group * per + inner) * step
                sent[chunk][at : at + size, :] = made[inner * size : (inner + 1) * size, :]

    scope = jax.named_scope
    with scope("kernel_lines"):
        for load in loads[1:4]:
            load.wait()
        lines = mul3((table_k[0][...], table_k[1][...]), split(k_ref[...]), ((1,), (1,)))
        for device in range(devices):
            at = device * pitch + size
            sent[0][at : at + 8, :] = lines[device * 8 : (device + 1) * 8, :]
    with scope("x_load"):
        loads[0].wait()
        loads[4].wait()
        for load in loads[5:]:
            load.start()
    with scope("x_lines0"):
        charges = jnp.concatenate(split(q_ref[...]), axis=0)
        x_lines(0, charges)
    with scope("barrier"):
        pl.semaphore_wait(barrier, devices - 1)
    with scope("send0"):
        there = [exchange(blocks_z, blocks_y, size + 2, sent[0], held[0], sent_sem.at[0])]
    with scope("x_lines1"):
        loads[5].wait()
        x_lines(1, charges)
    with scope("send1"):
        there.append(exchange(blocks_z, blocks_y, size, sent[1], held[1], sent_sem.at[1]))
    with scope("wait_there0"):
        for load in loads[6:12]:
            load.wait()
        there[0].wait_recv()
    y_pairs = ((table_y[0][...], table_y[1][...]), (table_b[0][...], table_b[1][...]))
    z_pair = (table_z[0][...], table_z[1][...])
    shape = (count, blocks_z, blocks_y, half)
    with scope("middle0"):
        green = middle_stage(shape, held[0], *y_pairs, *z_pair, None, back[0])
    with scope("return0"):
        returns = [exchange(blocks_z, blocks_y, size, back[0], home[0], back_sem.at[0])]
    with scope("wait_there1"):
        there[1].wait_recv()
    with scope("middle1"):
        middle_stage(shape, held[1], *y_pairs, *z_pair, green[:, LANES:], back[1])
    with scope("return1"):
        returns.append(exchange(blocks_z, blocks_y, size, back[1], home[1], back_sem.at[1]))
    for load in loads[12:]:
        load.wait()
    borders = []
    fine = [(table_f[2 * c][...], table_f[2 * c + 1][...]) for c in range(CHUNKS)]
    for chunk in range(CHUNKS):
        with scope(f"wait_back{chunk}"):
            returns[chunk].wait_recv()
        with scope(f"turn{chunk}"):
            turned = jnp.transpose(home[chunk][...])
            own[chunk][...] = turned
        with scope(f"send_rim{chunk}"):
            borders.append(send_rims(
                blocks_z, blocks_y, planes, rows, own[chunk], home, stages[chunk], rims[chunk], rim_sem.at[chunk]
            ))
        with scope(f"own{chunk}"):
            made = mul3_rows(split(turned), fine[chunk]).reshape(planes, rows, -1)
            if chunk:
                made = total[1 : planes + 1, :rows, :] + made
            total[1 : planes + 1, :rows, :] = made
    flat = 3 * rows

    def pack_own(first, last):
        values = total[first:last, :rows, :]
        high, low = split(values)
        packed[first:last, :rows, :] = high
        packed[first:last, rows : 2 * rows, :] = low

    pack_own(1, planes + 1)
    for chunk in range(CHUNKS):
        with scope(f"wait_rim{chunk}"):
            borders[chunk].wait_recv()
        with scope(f"rim{chunk}"):
            made = mul3_rows(split(rim_lines(planes, rims[chunk])), fine[chunk])
            sides = 8 * (planes + 3)
            ends = made[:flat].reshape(3, rows, -1)
            sides = made[flat : flat + sides].reshape(planes + 3, 8, -1)
            if not chunk:
                total[:, rows:, :] = sides
                total[0:1, :rows, :] = ends[0:1]
                total[planes + 1 :, :rows, :] = ends[1:]
                continue
            sides = total[:, rows:, :] + sides
            high = sides.astype(jnp.bfloat16).astype(jnp.float32)
            packed[:, 2 * rows :, :] = jnp.concatenate([high, sides - high], axis=1).astype(jnp.bfloat16)
            for i, place in enumerate((0, planes + 1, planes + 2)):
                high, low = split(total[place, :rows, :] + ends[i])
                packed[place, :rows, :] = high
                packed[place, rows : 2 * rows, :] = low
    with scope("wait_sends"):
        for copy in there + returns + borders:
            copy.wait_send()


STEP = 2


def refine_kernel(x_ref, r_ref, o_ref, made, out_sem):
    planes = x_ref.shape[0] - 3
    stores = []
    for p in range(0, planes, STEP):
        with jax.named_scope(f"refine{p}"):
            near = x_ref[p : p + STEP + 3].reshape((STEP + 3) * x_ref.shape[1], x_ref.shape[2])
            span = pl.ds(2 * p, 2 * STEP)
            made[span] = mul(r_ref[...], near).reshape(2 * STEP, -1, made.shape[2])
            stores.append(pltpu.make_async_copy(made.at[span], o_ref.at[span], out_sem.at[p // STEP]))
            stores[-1].start()
    with jax.named_scope("refine_store"):
        for store in stores:
            store.wait()


def rim_table(count):
    made = np.zeros((2 * count, count + 3))
    for i in range(count):
        made[2 * i, i + 1] = 1.0
        made[2 * i + 1, i : i + 4] = np.array([-1.0, 9.0, 9.0, -1.0]) / 16.0
    return made


def refine(haloed, planes, rows, width):
    along_y = rim_table(rows)
    middle = along_y[:, 1 : rows + 1]
    sides = np.concatenate([along_y[:, :1], along_y[:, rows + 1 :], np.zeros((2 * rows, 5))], axis=1)
    along_y = np.concatenate([middle, middle, sides, sides], axis=1)
    both = jnp.asarray(np.kron(rim_table(STEP), along_y), jnp.bfloat16)
    shape = (2 * planes, 2 * rows, width)
    return pl.pallas_call(
        refine_kernel,
        out_shape=jax.ShapeDtypeStruct(shape, jnp.float32),
        in_specs=[
            pl.BlockSpec(memory_space=pltpu.VMEM),
            pl.BlockSpec(memory_space=pltpu.VMEM),
        ],
        out_specs=pl.BlockSpec(memory_space=pl.ANY),
        scratch_shapes=[
            pltpu.VMEM(shape, jnp.float32), pltpu.SemaphoreType.DMA((planes // STEP,)),
        ],
        compiler_params=pltpu.CompilerParams(vmem_limit_bytes=16 * 1024 * 1024),
    )(haloed, both)


def per_device(charges, kernel):
    planes, rows, count = kernel.shape
    width = charges.shape[2]
    replicas = width // count
    half = replicas // 2
    blocks_z, blocks_y = lax.axis_size("gz"), lax.axis_size("gy")
    devices = blocks_z * blocks_y
    place = planes * rows
    fits = place == LANES and 2 * count == LANES and half == 8 and blocks_z == 8
    if not fits or count != CHUNKS * devices or replicas % 2 or rows != 16 or planes != 8 or devices % 8:
        return plain(charges, kernel)
    size = 2 * half
    per = LANES // size
    lines_x = pair_table(count, replicas, devices)
    table_x, table_f = [], []
    for chunk in range(CHUNKS):
        high, low = table(lines_x[chunk].reshape(devices // per, LANES, width))
        table_x.append(jnp.concatenate([high, low], axis=1).reshape(-1, width))
        table_f += table(refined(lines_x[chunk], 1).reshape(-1, 2 * width))
    lines_y = y_table(count, planes, rows)
    tables = [
        *table(line_table(count, devices)), *table_x, *table(lines_y), *table(lines_y.T),
        *z_tables(count, blocks_z), *table_f,
    ]
    arrays = [charges.reshape(place, width), kernel.reshape(place, count), *tables]
    deep = devices * size
    block = lambda *shape: pltpu.VMEM(shape, jnp.float32)
    dma = pltpu.SemaphoreType.DMA
    stage = [block(planes, deep), block(2 * planes, deep), block(4, 8, deep)]
    rim = [
        block(rows, deep), block(2 * rows, deep), block(planes, deep), block(2 * planes, deep),
        block(4, 8, deep),
    ]
    haloed = pl.pallas_call(
        functools.partial(main_kernel, (count, blocks_z, blocks_y, half, len(tables))),
        out_shape=pltpu.VMEM((planes + 3, 3 * rows, 2 * width), jnp.bfloat16),
        in_specs=[pl.BlockSpec(memory_space=pl.ANY)] * len(arrays),
        out_specs=pl.BlockSpec(memory_space=pltpu.VMEM),
        scratch_shapes=[
            *(pltpu.VMEM(a.shape, a.dtype) for a in arrays),
            dma((len(arrays),)), dma((CHUNKS, 2)), dma((CHUNKS, 2)), dma((CHUNKS, 2)),
            block(planes + 3, rows + 8, 2 * width),
            block(devices * (size + 8), LANES), block(deep, LANES),
            block(devices * (size + 8), LANES), block(deep, LANES),
            block(deep, LANES), block(deep, LANES),
            block(deep, LANES), block(deep, LANES),
            block(place, deep), block(place, deep),
            *stage, *stage, *rim, *rim,
        ],
        compiler_params=pltpu.CompilerParams(
            collective_id=0, has_side_effects=True, vmem_limit_bytes=60 * 1024 * 1024
        ),
    )(*arrays)
    return refine(haloed, planes, rows, 2 * width)


def solution(mesh):
    placed = (P("gz", "gy", None), P("gz", "gy", None))
    return jax.shard_map(
        per_device, mesh=mesh, in_specs=placed, out_specs=P("gz", "gy", None), check_vma=False
    )
```

```python
import functools

import jax
import jax.numpy as jnp
import numpy as np
from jax import lax
from jax.experimental import pallas as pl
from jax.experimental.pallas import tpu as pltpu
from jax.sharding import PartitionSpec as P

AXES = ("gz", "gy")


def angle(first, second, count):
    return 2.0 * np.pi / count * ((first * second) % count)


def x_table(count, replicas, devices):
    half = replicas // 2
    columns = count * half // devices
    device, part, column, x, side, pair = np.ix_(
        *(np.arange(s) for s in (devices, 2, columns, count, 2, half))
    )
    flat = device * columns + column
    theta = angle(flat // half, x, count)
    value = np.where(part == side, np.cos(theta), np.where(part == 0, np.sin(theta), -np.sin(theta)))
    value = value * (flat % half == pair)
    return value.reshape(devices * 2 * columns, count, replicas)


def x_kernel_table(count, replicas, devices):
    half = replicas // 2
    columns = count * half // devices
    lines = max(1, columns // half)
    device, part, line, x = np.ix_(*(np.arange(s) for s in (devices, 2, lines, count)))
    theta = angle(device * columns // half + line, x, count)
    value = np.where(part == 0, np.cos(theta), -np.sin(theta))
    return value.reshape(devices * 2 * lines, count)


def y_table(count, planes, rows):
    part, block, plane, row, new_plane, new_part, freq = np.ix_(
        *(np.arange(s) for s in (2, count // rows, planes, rows, planes, 2, count))
    )
    theta = angle(block * rows + row, freq, count)
    value = np.where(
        part == new_part, np.cos(theta), np.where(new_part == 0, np.sin(theta), -np.sin(theta))
    )
    value = value * (plane == new_plane)
    return value.reshape(2 * count * planes, planes * 2 * count)


def z_table(count, planes, columns, lines, group, wave):
    blocks = count // planes
    low, high, column, z_low, z_high, line = np.ix_(
        *(np.arange(s) for s in (planes, blocks, columns, planes, blocks, lines))
    )
    theta = angle(high * planes + low, z_high * planes + z_low, count)
    value = wave(theta) * (column // group == line)
    return value.reshape(count * columns, count * lines)


def refined(values, axis):
    before = np.roll(values, 1, axis)
    after = np.roll(values, -1, axis)
    after_two = np.roll(values, -2, axis)
    middle = (9.0 * (values + after) - (before + after_two)) / 16.0
    stacked = np.stack([values, middle], axis=axis + 1)
    shape = list(values.shape)
    shape[axis] = 2 * shape[axis]
    return stacked.reshape(shape)


def const(values):
    return jnp.asarray(np.asarray(values, np.float32))


def dot(left, right, dims=((1,), (0,))):
    return lax.dot_general(
        left, right, (dims, ((), ())), precision=lax.Precision.HIGH,
        preferred_element_type=jnp.float32,
    )


def extended(block, axis, dim):
    size = lax.axis_size(axis)
    forward = [(i, (i + 1) % size) for i in range(size)]
    backward = [(target, source) for source, target in forward]
    low = lax.ppermute(lax.slice_in_dim(block, block.shape[dim] - 1, None, axis=dim), axis, forward)
    high = lax.ppermute(lax.slice_in_dim(block, 0, 2, axis=dim), axis, backward)
    return jnp.concatenate([low, block, high], axis=dim)


def refine_rim(haloed, axis, count):
    centre = lax.slice_in_dim(haloed, 1, 1 + count, axis=axis)
    before = lax.slice_in_dim(haloed, 0, count, axis=axis)
    after = lax.slice_in_dim(haloed, 2, 2 + count, axis=axis)
    after_two = lax.slice_in_dim(haloed, 3, 3 + count, axis=axis)
    middle = (9.0 * (centre + after) - (before + after_two)) / 16.0
    stacked = jnp.stack([centre, middle], axis=axis + 1)
    shape = list(centre.shape)
    shape[axis] = 2 * count
    return stacked.reshape(shape)


def plain(charges, kernel):
    planes, rows, count = kernel.shape
    replicas = charges.shape[2] // count
    half = replicas // 2
    blocks_z, blocks_y = lax.axis_size("gz"), lax.axis_size("gy")
    devices = blocks_z * blocks_y
    place = planes * rows
    columns = count * half // devices
    lines = max(1, columns // half)
    table_x = x_table(count, replicas, devices)
    table_y = const(y_table(count, planes, rows))
    cos_z = const(z_table(count, planes, columns, columns, 1, np.cos))
    sin_z = const(z_table(count, planes, columns, columns, 1, np.sin))
    cos_k = const(z_table(count, planes, columns, lines, half, np.cos) / count**3)
    sin_k = const(z_table(count, planes, columns, lines, half, np.sin) / count**3)

    sent = dot(const(table_x.reshape(-1, count * replicas)), charges.reshape(place, -1), ((1,), (1,)))
    sent_k = dot(const(x_kernel_table(count, replicas, devices)), kernel.reshape(place, count), ((1,), (1,)))
    both = jnp.concatenate(
        [sent.reshape(devices, 2 * columns, place), sent_k.reshape(devices, 2 * lines, place)], axis=1
    )
    both = lax.all_to_all(both, AXES, split_axis=0, concat_axis=0, tiled=True)

    def by_y(block, width):
        block = block.reshape(blocks_z, blocks_y, 2, width, place).transpose(0, 3, 2, 1, 4)
        block = dot(block.reshape(blocks_z * width, 2 * blocks_y * place), table_y)
        block = block.reshape(blocks_z * width, planes, 2 * count).transpose(1, 0, 2)
        return block.reshape(count * width, 2 * count)

    def swap(values):
        return jnp.concatenate([values[:, count:], values[:, :count]], axis=1)

    sign = jnp.where(lax.broadcasted_iota(jnp.int32, (1, 2 * count), 1) < count, 1.0, -1.0)
    data = by_y(both[:, : 2 * columns], columns)
    green = by_y(both[:, 2 * columns :], lines)
    data = dot(cos_z, data) + sign * swap(dot(sin_z, data))
    green = dot(cos_k, green) + sign * swap(dot(sin_k, green))
    real, imag = green[:, :count], green[:, count:]
    data = data * jnp.concatenate([real, real], axis=1) + swap(data) * jnp.concatenate([-imag, imag], axis=1)
    data = dot(cos_z, data) - sign * swap(dot(sin_z, data))
    data = data.reshape(planes, blocks_z * columns, 2 * count).transpose(1, 0, 2)
    data = dot(data.reshape(blocks_z * columns, planes * 2 * count), table_y, ((1,), (1,)))
    data = data.reshape(blocks_z, columns, 2, blocks_y, place).transpose(0, 3, 2, 1, 4)
    data = lax.all_to_all(
        data.reshape(devices, 2 * columns, place), AXES, split_axis=0, concat_axis=0, tiled=True
    )
    fine_x = const(refined(table_x, 1).reshape(-1, 2 * count * replicas))
    result = dot(data.reshape(devices * 2 * columns, place), fine_x, ((0,), (0,)))
    result = result.reshape(planes, rows, 2 * count * replicas)
    result = extended(extended(result, "gz", 0), "gy", 1)
    result = refine_rim(result, 0, planes)
    return refine_rim(result, 1, rows)


LANES = 128
MESH = pl.DeviceIdType.MESH


def table(values):
    high = np.asarray(values, np.float32).astype(jnp.bfloat16)
    low = (np.asarray(values, np.float64) - high.astype(np.float64)).astype(jnp.bfloat16)
    return [jnp.asarray(high), jnp.asarray(low)]


def split(values):
    high = values.astype(jnp.bfloat16)
    return high, (values - high.astype(jnp.float32)).astype(jnp.bfloat16)


def mul(left, right, dims=((1,), (0,))):
    return lax.dot_general(left, right, (dims, ((), ())), preferred_element_type=jnp.float32)


def mul3(left, right, dims=((1,), (0,))):
    (a, b), (c, d) = left, right
    return mul(a, d, dims) + mul(b, c, dims) + mul(a, c, dims)


GROUPS = 4
CHUNKS = 2


def mul3_rows(left, right):
    (a, b), (c, d) = left, right
    rows = a.shape[0]
    both = mul(jnp.concatenate([b, a], axis=0), c)
    return mul(a, d) + both[:rows] + both[rows:]


def line_of(device, chunk, count):
    flip = np.where(device == 0, count // 2, (count - device) % count)
    return np.where(chunk == 0, device, flip)


def pair_table(count, replicas, devices):
    half = replicas // 2
    chunk, device, part, row, x, side, pair = np.ix_(
        *(np.arange(s) for s in (CHUNKS, devices, 2, half, count, 2, half))
    )
    theta = angle(line_of(device, chunk, count), x, count)
    value = np.where(part == side, np.cos(theta), np.where(part == 0, np.sin(theta), -np.sin(theta)))
    value = value * (row == pair)
    return value.reshape(CHUNKS, devices * 2 * half, count, replicas)


def line_table(count, devices):
    device, row, x = np.ix_(*(np.arange(s) for s in (devices, 8, count)))
    theta = angle(device, x, count)
    other = np.where(device == 0, np.cos(angle(count // 2, x, count)), -np.sin(theta))
    value = np.where(row == 0, np.cos(theta), np.where(row == 1, other, 0.0))
    return value.reshape(devices * 8, count)


def stack3(values):
    high = np.asarray(values, np.float32).astype(jnp.bfloat16)
    low = (np.asarray(values, np.float64) - high.astype(np.float64)).astype(jnp.bfloat16)
    return jnp.asarray(np.concatenate([high, high, low], axis=1))


def z_tables(count, blocks):
    planes = count // blocks
    freq = np.arange(count)[:, None]
    place = np.arange(count)[None, :]
    theta = angle(freq, (place % blocks) * planes + place // blocks, count)
    forward = stack3(np.concatenate([np.cos(theta), np.sin(theta)], axis=0))
    inverse = stack3(np.concatenate([np.cos(theta.T), np.sin(theta.T)], axis=0))
    return forward, inverse


def remote(source, target, sems, place):
    return pltpu.make_async_remote_copy(
        src_ref=source, dst_ref=target, send_sem=sems[0], recv_sem=sems[1],
        device_id=place, device_id_type=MESH,
    )


def exchange(blocks_z, blocks_y, rows, source, target, sems, halves=False):
    size = blocks_z * blocks_y // GROUPS
    devices = size * GROUPS
    me = lax.axis_index("gz") * blocks_y + lax.axis_index("gy")
    group, inner = me // size, lax.rem(me, size)
    high, low = group // 2, lax.rem(group, 2)
    turn = lax.rem(high + low, 2)
    pitch_from, pitch_to = source.shape[0] // devices, target.shape[0] // devices

    for flip_high, flip_low in ((1, 0), (1, 1), (0, 1), (0, 0)):
        far = lax.rem(high + flip_high + turn, 2) * 2 + lax.rem(low + flip_low + turn, 2)
        for step in range(size):
            other = far * size + lax.rem(inner + step, size)
            there = remote(
                source.at[pl.ds(pl.multiple_of(other * pitch_from, 8), rows)],
                target.at[pl.ds(pl.multiple_of(me * pitch_to, 8), rows)],
                (sems.at[0], sems.at[1 + lax.rem(flip_high + turn, 2) if halves else 1]),
                (other // blocks_y, lax.rem(other, blocks_y)),
            )
            if step == 0 and flip_high == flip_low:
                pl.when(other != me)(there.start)
            else:
                there.start()
    span = min(pitch_from, pitch_to)
    mine_from = pl.ds(pl.multiple_of(me * pitch_from, 8), span)
    target[pl.ds(pl.multiple_of(me * pitch_to, 8), span), :] = source[mine_from, :]
    other = lax.rem(me + 1, devices)

    def counter(number, senders):
        span = pl.ds(0, senders * rows)
        place = (other // blocks_y, lax.rem(other, blocks_y))
        return remote(source.at[span], target.at[span], (sems.at[0], sems.at[number]), place)

    everything = counter(1, devices - 1)
    if halves:
        return everything, counter(1, devices // 2 - 1), counter(2, devices // 2)
    return everything, everything


def swap_parts(values):
    half = LANES // 2
    pieces = [
        pltpu.roll(values[:, p : p + LANES], half, 1) for p in range(0, values.shape[1], LANES)
    ]
    return jnp.concatenate(pieces, axis=1)


def stacked(values):
    high, low = split(values)
    return jnp.concatenate([low, high, high], axis=0)


def repeat(values, times):
    return jnp.concatenate([values] * times, axis=1)


def y_lines(ref, start, stride, blocks):
    return ref[pl.ds(start, blocks, stride=stride), :]


def middle_stage(sizes, held, table_y, table_b, forward, inverse, green, back):
    count, blocks_z, blocks_y, half = sizes
    planes = count // blocks_z
    pitch = held.shape[0] // (blocks_z * blocks_y)
    lane = lax.broadcasted_iota(jnp.int32, (1, LANES), 1)
    sign = jnp.where(lane < count, 1.0, -1.0)

    def gather(row):
        pieces = [y_lines(held, y * pitch + row, blocks_y * pitch, blocks_z) for y in range(blocks_y)]
        return jnp.concatenate(pieces, axis=1)

    lines = [
        jnp.concatenate([gather(column), gather(half + column)], axis=1) for column in range(half)
    ]
    if green is None:
        me = lax.axis_index("gz") * blocks_y + lax.axis_index("gy")
        keep = jnp.where(me == 0, 0.0, 1.0).astype(jnp.float32)
        first, second = gather(2 * half), gather(2 * half + 1)
        lines.append(jnp.concatenate([first, keep * second], axis=1))
        lines.append(
            jnp.concatenate([keep * first + (1.0 - keep) * second, -keep * second], axis=1)
        )
    width = len(lines)
    data = mul3_rows(split(jnp.concatenate(lines, axis=0)), table_y)
    data = jnp.concatenate(
        [
            jnp.concatenate(
                [
                    data[c * blocks_z : (c + 1) * blocks_z, p * LANES : (p + 1) * LANES]
                    for p in range(planes)
                ],
                axis=0,
            )
            for c in range(width)
        ],
        axis=1,
    )
    both = mul(forward, stacked(data))
    data = both[:count] + repeat(sign, width) * swap_parts(both[count:])
    spectra = None
    if green is None:
        scaled = data[:, half * LANES :] * (1.0 / count**3)
        green, spectra = scaled[:, :LANES], scaled
        data = data[:, : half * LANES]
    other = swap_parts(green)
    real = jnp.where(lane < count, green, other)
    imag = jnp.where(lane < count, -other, green)
    data = data * repeat(real, half) + swap_parts(data) * repeat(imag, half)
    both = mul(inverse, stacked(data))
    data = both[:count] - repeat(sign, half) * swap_parts(both[count:])
    data = jnp.concatenate(
        [
            jnp.concatenate(
                [
                    data[p * blocks_z : (p + 1) * blocks_z, c * LANES : (c + 1) * LANES]
                    for p in range(planes)
                ],
                axis=1,
            )
            for c in range(half)
        ],
        axis=0,
    )
    data = mul3_rows(split(data), table_b)
    out_pitch = 2 * half
    for column in range(half):
        for part in range(2):
            for y in range(blocks_y):
                at = (part * blocks_y + y) * LANES
                back[pl.ds(y * out_pitch + part * half + column, blocks_z, stride=blocks_y * out_pitch), :] = (
                    data[column * blocks_z : (column + 1) * blocks_z, at : at + LANES]
                )
    return spectra


def send_rims(blocks_z, blocks_y, planes, rows, own, sizes, stage, rims, sems):
    to_up, to_down, to_corner = stage
    low_z, high_z, low_y, high_y, corner = rims
    gz, gy = lax.axis_index("gz"), lax.axis_index("gy")
    next_z, last_z = lax.rem(gz + 1, blocks_z), lax.rem(gz + blocks_z - 1, blocks_z)
    next_y, last_y = lax.rem(gy + 1, blocks_y), lax.rem(gy + blocks_y - 1, blocks_y)
    end = (planes - 1) * rows
    def side(row):
        return jnp.concatenate([own[p * rows + row : p * rows + row + 1, :] for p in range(planes)], axis=0)

    to_up[...] = side(rows - 1)
    to_down[...] = jnp.concatenate([side(0), side(1)], axis=0)
    picks = (
        (end + rows - 1,), (end, end + 1), (rows - 1, 2 * rows - 1), (0, 1, rows, rows + 1),
    )
    for number, pick in enumerate(picks):
        pieces = [own[r : r + 1, :] for r in pick]
        pieces.append(jnp.zeros((8 - len(pick), own.shape[1]), jnp.float32))
        to_corner[number] = jnp.concatenate(pieces, axis=0)
    places = ((next_z, next_y), (next_z, last_y), (last_z, next_y), (last_z, last_y))
    copies = []
    for number, (pick, place) in enumerate(zip(picks, places)):
        span = pl.ds(0, len(pick))
        copies.append(
            remote(to_corner.at[number, span], corner.at[number, span], sems, place)
        )
    for copy in copies:
        copy.start()
    down = remote(own.at[pl.ds(0, 2 * rows)], high_z, sems, (last_z, gy))
    up = remote(own.at[pl.ds(end, rows)], low_z, sems, (next_z, gy))
    pl.when(gz == 0)(down.start)
    up.start()
    pl.when(gz != 0)(down.start)
    sides = [
        remote(to_up, low_y, sems, (gz, next_y)), remote(to_down, high_y, sems, (gz, last_y)),
    ]
    for copy in sides:
        copy.start()
    count = pl.ds(0, 3 * (planes + rows + 3) * own.shape[1] // LANES)
    return remote(sizes[0].at[count], sizes[1].at[count], sems, (next_z, gy))


def rim_lines(rims):
    low_z, high_z, low_y, high_y, corner = rims
    planes = low_y.shape[0]
    empty = jnp.zeros((5, low_z.shape[1]), jnp.float32)
    tiles = [low_z[...], high_z[...]]
    tiles += [low_y[...], corner[0, 0:1, :], corner[2, 0:2, :], empty]
    tiles += [high_y[:planes, :], corner[1, 0:1, :], corner[3, 0:1, :], corner[3, 2:3, :], empty]
    tiles += [high_y[planes:, :], corner[1, 1:2, :], corner[3, 1:2, :], corner[3, 3:4, :], empty]
    return jnp.concatenate(tiles, axis=0)


def main_kernel(sizes, *refs):
    count, blocks_z, blocks_y, half, n_tables = sizes
    devices = blocks_z * blocks_y
    planes = count // blocks_z
    sources = refs[: 2 + n_tables]
    packed = refs[2 + n_tables]
    loaded = refs[3 + n_tables : 5 + 2 * n_tables]
    (q_ref, k_ref), tables = loaded[:2], loaded[2:]
    rest = list(refs[5 + 2 * n_tables :])
    load_sem, sent_sem, back_sem, rim_sem, total, edge = rest[:6]
    sent, held, back, home = (rest[6 + 2 * i : 8 + 2 * i] for i in range(4))
    own = rest[14:17]
    stages = [rest[17 + 3 * i : 20 + 3 * i] for i in range(3)]
    rims = [rest[26 + 5 * i : 31 + 5 * i] for i in range(2)]
    table_k, table_x, table_y, table_b, table_z, table_f = (
        tables[0:2], tables[2:4], tables[4:6], tables[6:8], tables[8:10], tables[10:14]
    )
    me = lax.axis_index("gz") * blocks_y + lax.axis_index("gy")
    barrier = pltpu.get_barrier_semaphore()
    for step in range(1, devices):
        other = lax.rem(me + step, devices)
        pl.semaphore_signal(
            barrier, inc=1, device_id=(other // blocks_y, lax.rem(other, blocks_y)), device_id_type=MESH
        )
    loads = [
        pltpu.make_async_copy(s, t, load_sem.at[i]) for i, (s, t) in enumerate(zip(sources, loaded))
    ]
    for load in loads[:5]:
        load.start()
    rows = q_ref.shape[0] // planes
    size = 2 * half
    pitch = sent[0].shape[0] // devices

    def x_lines(chunk, charges):
        per = LANES // size
        for group in range(devices // per):
            both = mul(table_x[chunk][group * 2 * LANES : (group + 1) * 2 * LANES, :], charges, ((1,), (1,)))
            made = both[:LANES, :LANES] + both[:LANES, LANES:] + both[LANES:, :LANES]
            step = sent[chunk].shape[0] // devices
            for inner in range(per):
                at = (group * per + inner) * step
                sent[chunk][at : at + size, :] = made[inner * size : (inner + 1) * size, :]

    scope = jax.named_scope
    with scope("kernel_lines"):
        for load in loads[1:4]:
            load.wait()
        lines = mul3((table_k[0][...], table_k[1][...]), split(k_ref[...]), ((1,), (1,)))
        for device in range(devices):
            at = device * pitch + size
            sent[0][at : at + 8, :] = lines[device * 8 : (device + 1) * 8, :]
    with scope("x_load"):
        loads[0].wait()
        loads[4].wait()
        for load in loads[5:]:
            load.start()
    with scope("x_lines0"):
        charges = jnp.concatenate(split(q_ref[...]), axis=0)
        x_lines(0, charges)
    with scope("barrier"):
        pl.semaphore_wait(barrier, devices - 1)
    with scope("send0"):
        there = [exchange(blocks_z, blocks_y, size + 2, sent[0], held[0], sent_sem.at[0])]
    with scope("x_lines1"):
        loads[5].wait()
        x_lines(1, charges)
    with scope("send1"):
        there.append(exchange(blocks_z, blocks_y, size, sent[1], held[1], sent_sem.at[1]))
    with scope("wait_there0"):
        for load in loads[6:12]:
            load.wait()
        there[0][1].wait_recv()
    y_pairs = ((table_y[0][...], table_y[1][...]), (table_b[0][...], table_b[1][...]))
    z_pair = (table_z[0][...], table_z[1][...])
    shape = (count, blocks_z, blocks_y, half)
    with scope("middle0"):
        green = middle_stage(shape, held[0], *y_pairs, *z_pair, None, back[0])
    with scope("return0"):
        returns = [exchange(blocks_z, blocks_y, size, back[0], home[0], back_sem.at[0])]
    with scope("wait_there1"):
        there[1][1].wait_recv()
    with scope("middle1"):
        middle_stage(shape, held[1], *y_pairs, *z_pair, green[:, LANES:], back[1])
    with scope("return1"):
        returns.append(exchange(blocks_z, blocks_y, size, back[1], home[1], back_sem.at[1], True))
    for load in loads[12:]:
        load.wait()
    deep = home[0].shape[0]
    near = pl.multiple_of(me // (devices // 2) * (deep // 2), LANES)
    far = pl.multiple_of(deep // 2 - near, LANES)
    pieces = (
        (0, pl.ds(0, deep), returns[0][1]), (1, pl.ds(near, deep // 2), returns[1][1]),
        (1, pl.ds(far, deep // 2), returns[1][2]),
    )
    borders = []

    def fine_of(number):
        chunk, span, _ = pieces[number]
        return table_f[2 * chunk][span, :], table_f[2 * chunk + 1][span, :]

    half_of = me // (devices // 2)
    slots = (rims[0], *([r.at[s] for r in rims[1]] for s in (half_of, 1 - half_of)))
    rim_sems = [
        (rim_sem.at[0, 0], rim_sem.at[1, 0]),
        (rim_sem.at[0, 1], rim_sem.at[1, 1 + half_of]),
        (rim_sem.at[0, 2], rim_sem.at[1, 2 - half_of]),
    ]
    for number, (chunk, span, coming) in enumerate(pieces):
        with scope(f"wait_back{number}"):
            coming.wait_recv()
        with scope(f"turn{number}"):
            turned = jnp.transpose(home[chunk][span, :])
            own[number][...] = turned
        with scope(f"send_rim{number}"):
            borders.append(send_rims(
                blocks_z, blocks_y, planes, rows, own[number], home, stages[number], slots[number],
                rim_sems[number],
            ))
        with scope(f"own{number}"):
            made = mul3_rows(split(turned), fine_of(number))
            total[...] = total[...] + made if number else made
    flat = 3 * rows

    def pack(place, values):
        high, low = split(values)
        packed[place, :] = high
        packed[pl.ds(place.start + place.size, place.size), :] = low

    for p in range(planes):
        pack(pl.ds(2 * (p + 1) * rows, rows), total[p * rows : (p + 1) * rows, :])
    for number in range(len(pieces)):
        with scope(f"wait_rim{number}"):
            borders[number].wait_recv()
        with scope(f"rim{number}"):
            made = mul3_rows(split(rim_lines(slots[number])), fine_of(number))
            if number:
                made = edge[...] + made
            if number < len(pieces) - 1:
                edge[...] = made
                continue
            for i, p in enumerate((0, planes + 1, planes + 2)):
                pack(pl.ds(2 * p * rows, rows), made[i * rows : (i + 1) * rows, :])
            pack(pl.ds(2 * (planes + 3) * rows, flat), made[flat:, :])
    with scope("wait_sends"):
        for copy in [there[0][0], there[1][0], returns[0][0], returns[1][0], *borders]:
            copy.wait_send()


STEP = 2


def refine_kernel(rows, x_ref, r_ref, o_ref, made, out_sem):
    planes = made.shape[0] // 2
    stores = []
    for p in range(0, planes, STEP):
        with jax.named_scope(f"refine{p}"):
            near = x_ref[2 * p * rows : 2 * (p + STEP + 3) * rows, :]
            near = jnp.concatenate([near, x_ref[2 * (planes + 3) * rows :, :]], axis=0)
            span = pl.ds(2 * p, 2 * STEP)
            made[span] = mul(r_ref[p // STEP], near).reshape(2 * STEP, -1, made.shape[2])
            stores.append(pltpu.make_async_copy(made.at[span], o_ref.at[span], out_sem.at[p // STEP]))
            stores[-1].start()
    with jax.named_scope("refine_store"):
        for store in stores:
            store.wait()


def rim_table(count):
    made = np.zeros((2 * count, count + 3))
    for i in range(count):
        made[2 * i, i + 1] = 1.0
        made[2 * i + 1, i : i + 4] = np.array([-1.0, 9.0, 9.0, -1.0]) / 16.0
    return made


def refine_tables(planes, rows):
    along_y = rim_table(rows)
    along_z = rim_table(planes)
    middle, sides = along_y[:, 1 : rows + 1], np.delete(along_y, np.arange(1, rows + 1), axis=1)
    order = [*range(1, planes + 1), 0, planes + 1, planes + 2]
    made = []
    for p in range(0, planes, STEP):
        lines = along_z[2 * p : 2 * (p + STEP)]
        own = np.kron(lines[:, p : p + STEP + 3], np.concatenate([middle, middle], axis=1))
        beside = np.einsum("ze,ys->zyse", lines[:, order], sides)
        beside = np.pad(beside, ((0, 0), (0, 0), (0, 0), (0, rows - len(order))))
        beside = beside.reshape(own.shape[0], 3 * rows)
        made.append(np.concatenate([own, beside, beside], axis=1))
    return np.stack(made)


def refine(haloed, planes, rows, width):
    tables = jnp.asarray(refine_tables(planes, rows), jnp.bfloat16)
    shape = (2 * planes, 2 * rows, width)
    return pl.pallas_call(
        functools.partial(refine_kernel, rows),
        out_shape=jax.ShapeDtypeStruct(shape, jnp.float32),
        in_specs=[
            pl.BlockSpec(memory_space=pltpu.VMEM),
            pl.BlockSpec(memory_space=pltpu.VMEM),
        ],
        out_specs=pl.BlockSpec(memory_space=pl.ANY),
        scratch_shapes=[
            pltpu.VMEM(shape, jnp.float32), pltpu.SemaphoreType.DMA((planes // STEP,)),
        ],
        compiler_params=pltpu.CompilerParams(vmem_limit_bytes=16 * 1024 * 1024),
    )(haloed, tables)


def per_device(charges, kernel):
    planes, rows, count = kernel.shape
    width = charges.shape[2]
    replicas = width // count
    half = replicas // 2
    blocks_z, blocks_y = lax.axis_size("gz"), lax.axis_size("gy")
    devices = blocks_z * blocks_y
    place = planes * rows
    fits = place == LANES and 2 * count == LANES and half == 8 and blocks_z == 8
    if not fits or count != CHUNKS * devices or replicas % 2 or rows != 16 or planes != 8 or devices % 8:
        return plain(charges, kernel)
    size = 2 * half
    per = LANES // size
    lines_x = pair_table(count, replicas, devices)
    table_x, table_f = [], []
    for chunk in range(CHUNKS):
        high, low = table(lines_x[chunk].reshape(devices // per, LANES, width))
        table_x.append(jnp.concatenate([high, low], axis=1).reshape(-1, width))
        table_f += table(refined(lines_x[chunk], 1).reshape(-1, 2 * width))
    lines_y = y_table(count, planes, rows)
    tables = [
        *table(line_table(count, devices)), *table_x, *table(lines_y), *table(lines_y.T),
        *z_tables(count, blocks_z), *table_f,
    ]
    arrays = [charges.reshape(place, width), kernel.reshape(place, count), *tables]
    deep = devices * size
    block = lambda *shape: pltpu.VMEM(shape, jnp.float32)
    dma = pltpu.SemaphoreType.DMA
    widths = (deep, deep // 2, deep // 2)
    stages = [block(*shape) for w in widths for shape in ((planes, w), (2 * planes, w), (4, 8, w))]
    rims = [
        block(*lead, *shape, w)
        for lead, w in (((), deep), ((2,), deep // 2))
        for shape in ((rows,), (2 * rows,), (planes,), (2 * planes,), (4, 8))
    ]
    haloed = pl.pallas_call(
        functools.partial(main_kernel, (count, blocks_z, blocks_y, half, len(tables))),
        out_shape=pltpu.VMEM((2 * (planes + 6) * rows, 2 * width), jnp.bfloat16),
        in_specs=[pl.BlockSpec(memory_space=pl.ANY)] * len(arrays),
        out_specs=pl.BlockSpec(memory_space=pltpu.VMEM),
        scratch_shapes=[
            *(pltpu.VMEM(a.shape, a.dtype) for a in arrays),
            dma((len(arrays),)), dma((CHUNKS, 2)), dma((CHUNKS, 3)), dma((2, 3)),
            block(place, 2 * width), block(6 * rows, 2 * width),
            block(devices * (size + 8), LANES), block(deep, LANES),
            block(devices * (size + 8), LANES), block(deep, LANES),
            block(deep, LANES), block(deep, LANES),
            block(deep, LANES), block(deep, LANES),
            *(block(place, w) for w in widths), *stages, *rims,
        ],
        compiler_params=pltpu.CompilerParams(
            collective_id=0, has_side_effects=True, vmem_limit_bytes=60 * 1024 * 1024
        ),
    )(*arrays)
    return refine(haloed, planes, rows, 2 * width)


def solution(mesh):
    placed = (P("gz", "gy", None), P("gz", "gy", None))
    return jax.shard_map(
        per_device, mesh=mesh, in_specs=placed, out_specs=P("gz", "gy", None), check_vma=False
    )
```

```python
import functools

import jax
import jax.numpy as jnp
import numpy as np
from jax import lax
from jax.experimental import pallas as pl
from jax.experimental.pallas import tpu as pltpu
from jax.sharding import PartitionSpec as P

AXES = ("gz", "gy")


def angle(first, second, count):
    return 2.0 * np.pi / count * ((first * second) % count)


def x_table(count, replicas, devices):
    half = replicas // 2
    columns = count * half // devices
    device, part, column, x, side, pair = np.ix_(
        *(np.arange(s) for s in (devices, 2, columns, count, 2, half))
    )
    flat = device * columns + column
    theta = angle(flat // half, x, count)
    value = np.where(part == side, np.cos(theta), np.where(part == 0, np.sin(theta), -np.sin(theta)))
    value = value * (flat % half == pair)
    return value.reshape(devices * 2 * columns, count, replicas)


def x_kernel_table(count, replicas, devices):
    half = replicas // 2
    columns = count * half // devices
    lines = max(1, columns // half)
    device, part, line, x = np.ix_(*(np.arange(s) for s in (devices, 2, lines, count)))
    theta = angle(device * columns // half + line, x, count)
    value = np.where(part == 0, np.cos(theta), -np.sin(theta))
    return value.reshape(devices * 2 * lines, count)


def y_table(count, planes, rows):
    part, block, plane, row, new_plane, new_part, freq = np.ix_(
        *(np.arange(s) for s in (2, count // rows, planes, rows, planes, 2, count))
    )
    theta = angle(block * rows + row, freq, count)
    value = np.where(
        part == new_part, np.cos(theta), np.where(new_part == 0, np.sin(theta), -np.sin(theta))
    )
    value = value * (plane == new_plane)
    return value.reshape(2 * count * planes, planes * 2 * count)


def z_table(count, planes, columns, lines, group, wave):
    blocks = count // planes
    low, high, column, z_low, z_high, line = np.ix_(
        *(np.arange(s) for s in (planes, blocks, columns, planes, blocks, lines))
    )
    theta = angle(high * planes + low, z_high * planes + z_low, count)
    value = wave(theta) * (column // group == line)
    return value.reshape(count * columns, count * lines)


def refined(values, axis):
    before = np.roll(values, 1, axis)
    after = np.roll(values, -1, axis)
    after_two = np.roll(values, -2, axis)
    middle = (9.0 * (values + after) - (before + after_two)) / 16.0
    stacked = np.stack([values, middle], axis=axis + 1)
    shape = list(values.shape)
    shape[axis] = 2 * shape[axis]
    return stacked.reshape(shape)


def const(values):
    return jnp.asarray(np.asarray(values, np.float32))


def dot(left, right, dims=((1,), (0,))):
    return lax.dot_general(
        left, right, (dims, ((), ())), precision=lax.Precision.HIGH,
        preferred_element_type=jnp.float32,
    )


def extended(block, axis, dim):
    size = lax.axis_size(axis)
    forward = [(i, (i + 1) % size) for i in range(size)]
    backward = [(target, source) for source, target in forward]
    low = lax.ppermute(lax.slice_in_dim(block, block.shape[dim] - 1, None, axis=dim), axis, forward)
    high = lax.ppermute(lax.slice_in_dim(block, 0, 2, axis=dim), axis, backward)
    return jnp.concatenate([low, block, high], axis=dim)


def refine_rim(haloed, axis, count):
    centre = lax.slice_in_dim(haloed, 1, 1 + count, axis=axis)
    before = lax.slice_in_dim(haloed, 0, count, axis=axis)
    after = lax.slice_in_dim(haloed, 2, 2 + count, axis=axis)
    after_two = lax.slice_in_dim(haloed, 3, 3 + count, axis=axis)
    middle = (9.0 * (centre + after) - (before + after_two)) / 16.0
    stacked = jnp.stack([centre, middle], axis=axis + 1)
    shape = list(centre.shape)
    shape[axis] = 2 * count
    return stacked.reshape(shape)


def plain(charges, kernel):
    planes, rows, count = kernel.shape
    replicas = charges.shape[2] // count
    half = replicas // 2
    blocks_z, blocks_y = lax.axis_size("gz"), lax.axis_size("gy")
    devices = blocks_z * blocks_y
    place = planes * rows
    columns = count * half // devices
    lines = max(1, columns // half)
    table_x = x_table(count, replicas, devices)
    table_y = const(y_table(count, planes, rows))
    cos_z = const(z_table(count, planes, columns, columns, 1, np.cos))
    sin_z = const(z_table(count, planes, columns, columns, 1, np.sin))
    cos_k = const(z_table(count, planes, columns, lines, half, np.cos) / count**3)
    sin_k = const(z_table(count, planes, columns, lines, half, np.sin) / count**3)

    sent = dot(const(table_x.reshape(-1, count * replicas)), charges.reshape(place, -1), ((1,), (1,)))
    sent_k = dot(const(x_kernel_table(count, replicas, devices)), kernel.reshape(place, count), ((1,), (1,)))
    both = jnp.concatenate(
        [sent.reshape(devices, 2 * columns, place), sent_k.reshape(devices, 2 * lines, place)], axis=1
    )
    both = lax.all_to_all(both, AXES, split_axis=0, concat_axis=0, tiled=True)

    def by_y(block, width):
        block = block.reshape(blocks_z, blocks_y, 2, width, place).transpose(0, 3, 2, 1, 4)
        block = dot(block.reshape(blocks_z * width, 2 * blocks_y * place), table_y)
        block = block.reshape(blocks_z * width, planes, 2 * count).transpose(1, 0, 2)
        return block.reshape(count * width, 2 * count)

    def swap(values):
        return jnp.concatenate([values[:, count:], values[:, :count]], axis=1)

    sign = jnp.where(lax.broadcasted_iota(jnp.int32, (1, 2 * count), 1) < count, 1.0, -1.0)
    data = by_y(both[:, : 2 * columns], columns)
    green = by_y(both[:, 2 * columns :], lines)
    data = dot(cos_z, data) + sign * swap(dot(sin_z, data))
    green = dot(cos_k, green) + sign * swap(dot(sin_k, green))
    real, imag = green[:, :count], green[:, count:]
    data = data * jnp.concatenate([real, real], axis=1) + swap(data) * jnp.concatenate([-imag, imag], axis=1)
    data = dot(cos_z, data) - sign * swap(dot(sin_z, data))
    data = data.reshape(planes, blocks_z * columns, 2 * count).transpose(1, 0, 2)
    data = dot(data.reshape(blocks_z * columns, planes * 2 * count), table_y, ((1,), (1,)))
    data = data.reshape(blocks_z, columns, 2, blocks_y, place).transpose(0, 3, 2, 1, 4)
    data = lax.all_to_all(
        data.reshape(devices, 2 * columns, place), AXES, split_axis=0, concat_axis=0, tiled=True
    )
    fine_x = const(refined(table_x, 1).reshape(-1, 2 * count * replicas))
    result = dot(data.reshape(devices * 2 * columns, place), fine_x, ((0,), (0,)))
    result = result.reshape(planes, rows, 2 * count * replicas)
    result = extended(extended(result, "gz", 0), "gy", 1)
    result = refine_rim(result, 0, planes)
    return refine_rim(result, 1, rows)


LANES = 128
MESH = pl.DeviceIdType.MESH


def table(values):
    high = np.asarray(values, np.float32).astype(jnp.bfloat16)
    low = (np.asarray(values, np.float64) - high.astype(np.float64)).astype(jnp.bfloat16)
    return [jnp.asarray(high), jnp.asarray(low)]


def split(values):
    high = values.astype(jnp.bfloat16)
    return high, (values - high.astype(jnp.float32)).astype(jnp.bfloat16)


def mul(left, right, dims=((1,), (0,))):
    return lax.dot_general(left, right, (dims, ((), ())), preferred_element_type=jnp.float32)


def mul3(left, right, dims=((1,), (0,))):
    (a, b), (c, d) = left, right
    return mul(a, d, dims) + mul(b, c, dims) + mul(a, c, dims)


GROUPS = 4
CHUNKS = 2


def mul3_rows(left, right):
    (a, b), (c, d) = left, right
    rows = a.shape[0]
    both = mul(jnp.concatenate([b, a], axis=0), c)
    return mul(a, d) + both[:rows] + both[rows:]


def line_of(device, chunk, count):
    flip = np.where(device == 0, count // 2, (count - device) % count)
    return np.where(chunk == 0, device, flip)


def pair_table(count, replicas, devices):
    half = replicas // 2
    chunk, device, part, row, x, side, pair = np.ix_(
        *(np.arange(s) for s in (CHUNKS, devices, 2, half, count, 2, half))
    )
    theta = angle(line_of(device, chunk, count), x, count)
    value = np.where(part == side, np.cos(theta), np.where(part == 0, np.sin(theta), -np.sin(theta)))
    value = value * (row == pair)
    return value.reshape(CHUNKS, devices * 2 * half, count, replicas)


def line_table(count, devices):
    device, row, x = np.ix_(*(np.arange(s) for s in (devices, 8, count)))
    theta = angle(device, x, count)
    other = np.where(device == 0, np.cos(angle(count // 2, x, count)), -np.sin(theta))
    value = np.where(row == 0, np.cos(theta), np.where(row == 1, other, 0.0))
    return value.reshape(devices * 8, count)


def stack3(values):
    high = np.asarray(values, np.float32).astype(jnp.bfloat16)
    low = (np.asarray(values, np.float64) - high.astype(np.float64)).astype(jnp.bfloat16)
    return jnp.asarray(np.concatenate([high, high, low], axis=1))


def z_tables(count, blocks):
    planes = count // blocks
    freq = np.arange(count)[:, None]
    place = np.arange(count)[None, :]
    theta = angle(freq, (place % blocks) * planes + place // blocks, count)
    forward = stack3(np.concatenate([np.cos(theta), np.sin(theta)], axis=0))
    inverse = stack3(np.concatenate([np.cos(theta.T), np.sin(theta.T)], axis=0))
    return forward, inverse


def remote(source, target, sems, place):
    return pltpu.make_async_remote_copy(
        src_ref=source, dst_ref=target, send_sem=sems[0], recv_sem=sems[1],
        device_id=place, device_id_type=MESH,
    )


def exchange(blocks_z, blocks_y, rows, source, target, sems, halves=False):
    size = blocks_z * blocks_y // GROUPS
    devices = size * GROUPS
    me = lax.axis_index("gz") * blocks_y + lax.axis_index("gy")
    group, inner = me // size, lax.rem(me, size)
    high, low = group // 2, lax.rem(group, 2)
    turn = lax.rem(high + low, 2)
    pitch_from, pitch_to = source.shape[0] // devices, target.shape[0] // devices

    order = [(flip + turn, low + other + turn, flip == other) for flip, other in ((1, 0), (1, 1), (0, 1), (0, 0))]
    if halves:
        order = [(1, 1 - high, False), (0, high, True), (1, high, False), (0, 1 - high, True)]
    for flip, other_low, own in order:
        across = lax.rem(high + flip, 2)
        far = across * 2 + lax.rem(other_low, 2)
        for step in range(size):
            other = far * size + lax.rem(inner + step, size)
            there = remote(
                source.at[pl.ds(pl.multiple_of(other * pitch_from, 8), rows)],
                target.at[pl.ds(pl.multiple_of(me * pitch_to, 8), rows)],
                (sems.at[0], sems.at[1 + flip if halves else 1]),
                (other // blocks_y, lax.rem(other, blocks_y)),
            )
            if step == 0 and own:
                pl.when(other != me)(there.start)
            else:
                there.start()
    span = min(pitch_from, pitch_to)
    mine_from = pl.ds(pl.multiple_of(me * pitch_from, 8), span)
    target[pl.ds(pl.multiple_of(me * pitch_to, 8), span), :] = source[mine_from, :]
    other = lax.rem(me + 1, devices)

    def counter(number, senders):
        span = pl.ds(0, senders * rows)
        place = (other // blocks_y, lax.rem(other, blocks_y))
        return remote(source.at[span], target.at[span], (sems.at[0], sems.at[number]), place)

    everything = counter(1, devices - 1)
    if halves:
        return everything, counter(1, devices // 2 - 1), counter(2, devices // 2)
    return everything, everything


def swap_parts(values):
    half = LANES // 2
    pieces = [
        pltpu.roll(values[:, p : p + LANES], half, 1) for p in range(0, values.shape[1], LANES)
    ]
    return jnp.concatenate(pieces, axis=1)


def stacked(values):
    high, low = split(values)
    return jnp.concatenate([low, high, high], axis=0)


def repeat(values, times):
    return jnp.concatenate([values] * times, axis=1)


def y_lines(ref, start, stride, blocks):
    return ref[pl.ds(start, blocks, stride=stride), :]


def middle_stage(sizes, held, table_y, table_b, forward, inverse, green, back):
    count, blocks_z, blocks_y, half = sizes
    planes = count // blocks_z
    pitch = held.shape[0] // (blocks_z * blocks_y)
    lane = lax.broadcasted_iota(jnp.int32, (1, LANES), 1)
    sign = jnp.where(lane < count, 1.0, -1.0)

    def gather(row):
        pieces = [y_lines(held, y * pitch + row, blocks_y * pitch, blocks_z) for y in range(blocks_y)]
        return jnp.concatenate(pieces, axis=1)

    lines = [
        jnp.concatenate([gather(column), gather(half + column)], axis=1) for column in range(half)
    ]
    if green is None:
        me = lax.axis_index("gz") * blocks_y + lax.axis_index("gy")
        keep = jnp.where(me == 0, 0.0, 1.0).astype(jnp.float32)
        first, second = gather(2 * half), gather(2 * half + 1)
        lines.append(jnp.concatenate([first, keep * second], axis=1))
        lines.append(
            jnp.concatenate([keep * first + (1.0 - keep) * second, -keep * second], axis=1)
        )
    width = len(lines)
    data = mul3_rows(split(jnp.concatenate(lines, axis=0)), table_y)
    data = jnp.concatenate(
        [
            jnp.concatenate(
                [
                    data[c * blocks_z : (c + 1) * blocks_z, p * LANES : (p + 1) * LANES]
                    for p in range(planes)
                ],
                axis=0,
            )
            for c in range(width)
        ],
        axis=1,
    )
    both = mul(forward, stacked(data))
    data = both[:count] + repeat(sign, width) * swap_parts(both[count:])
    spectra = None
    if green is None:
        scaled = data[:, half * LANES :] * (1.0 / count**3)
        green, spectra = scaled[:, :LANES], scaled
        data = data[:, : half * LANES]
    other = swap_parts(green)
    real = jnp.where(lane < count, green, other)
    imag = jnp.where(lane < count, -other, green)
    data = data * repeat(real, half) + swap_parts(data) * repeat(imag, half)
    both = mul(inverse, stacked(data))
    data = both[:count] - repeat(sign, half) * swap_parts(both[count:])
    data = jnp.concatenate(
        [
            jnp.concatenate(
                [
                    data[p * blocks_z : (p + 1) * blocks_z, c * LANES : (c + 1) * LANES]
                    for p in range(planes)
                ],
                axis=1,
            )
            for c in range(half)
        ],
        axis=0,
    )
    data = mul3_rows(split(data), table_b)
    out_pitch = 2 * half
    for column in range(half):
        for part in range(2):
            for y in range(blocks_y):
                at = (part * blocks_y + y) * LANES
                back[pl.ds(y * out_pitch + part * half + column, blocks_z, stride=blocks_y * out_pitch), :] = (
                    data[column * blocks_z : (column + 1) * blocks_z, at : at + LANES]
                )
    return spectra


def send_rims(blocks_z, blocks_y, planes, rows, own, sizes, stage, rims, sems):
    to_up, to_down, to_corner = stage
    low_z, high_z, low_y, high_y, corner = rims
    gz, gy = lax.axis_index("gz"), lax.axis_index("gy")
    next_z, last_z = lax.rem(gz + 1, blocks_z), lax.rem(gz + blocks_z - 1, blocks_z)
    next_y, last_y = lax.rem(gy + 1, blocks_y), lax.rem(gy + blocks_y - 1, blocks_y)
    end = (planes - 1) * rows
    def side(row):
        return jnp.concatenate([own[p * rows + row : p * rows + row + 1, :] for p in range(planes)], axis=0)

    to_up[...] = side(rows - 1)
    to_down[...] = jnp.concatenate([side(0), side(1)], axis=0)
    picks = (
        (end + rows - 1,), (end, end + 1), (rows - 1, 2 * rows - 1), (0, 1, rows, rows + 1),
    )
    for number, pick in enumerate(picks):
        pieces = [own[r : r + 1, :] for r in pick]
        pieces.append(jnp.zeros((8 - len(pick), own.shape[1]), jnp.float32))
        to_corner[number] = jnp.concatenate(pieces, axis=0)
    places = ((next_z, next_y), (next_z, last_y), (last_z, next_y), (last_z, last_y))
    copies = []
    for number, (pick, place) in enumerate(zip(picks, places)):
        span = pl.ds(0, len(pick))
        copies.append(
            remote(to_corner.at[number, span], corner.at[number, span], sems, place)
        )
    for copy in copies:
        copy.start()
    down = remote(own.at[pl.ds(0, 2 * rows)], high_z, sems, (last_z, gy))
    up = remote(own.at[pl.ds(end, rows)], low_z, sems, (next_z, gy))
    pl.when(gz == 0)(down.start)
    up.start()
    pl.when(gz != 0)(down.start)
    sides = [
        remote(to_up, low_y, sems, (gz, next_y)), remote(to_down, high_y, sems, (gz, last_y)),
    ]
    for copy in sides:
        copy.start()
    count = pl.ds(0, 3 * (planes + rows + 3) * own.shape[1] // LANES)
    return remote(sizes[0].at[count], sizes[1].at[count], sems, (next_z, gy))


def rim_lines(rims):
    low_z, high_z, low_y, high_y, corner = rims
    planes = low_y.shape[0]
    empty = jnp.zeros((5, low_z.shape[1]), jnp.float32)
    tiles = [low_z[...], high_z[...]]
    tiles += [low_y[...], corner[0, 0:1, :], corner[2, 0:2, :], empty]
    tiles += [high_y[:planes, :], corner[1, 0:1, :], corner[3, 0:1, :], corner[3, 2:3, :], empty]
    tiles += [high_y[planes:, :], corner[1, 1:2, :], corner[3, 1:2, :], corner[3, 3:4, :], empty]
    return jnp.concatenate(tiles, axis=0)


def main_kernel(sizes, *refs):
    count, blocks_z, blocks_y, half, n_tables = sizes
    devices = blocks_z * blocks_y
    planes = count // blocks_z
    sources = refs[: 2 + n_tables]
    packed = refs[2 + n_tables]
    loaded = refs[3 + n_tables : 5 + 2 * n_tables]
    (q_ref, k_ref), tables = loaded[:2], loaded[2:]
    rest = list(refs[5 + 2 * n_tables :])
    load_sem, sent_sem, back_sem, rim_sem, total, edge = rest[:6]
    sent, held, back, home = (rest[6 + 2 * i : 8 + 2 * i] for i in range(4))
    own = rest[14:17]
    stages = [rest[17 + 3 * i : 20 + 3 * i] for i in range(3)]
    rims = [rest[26 + 5 * i : 31 + 5 * i] for i in range(2)]
    table_k, table_x, table_y, table_b, table_z, table_f = (
        tables[0:2], tables[2:4], tables[4:6], tables[6:8], tables[8:10], tables[10:14]
    )
    me = lax.axis_index("gz") * blocks_y + lax.axis_index("gy")
    barrier = pltpu.get_barrier_semaphore()
    for step in range(1, devices):
        other = lax.rem(me + step, devices)
        pl.semaphore_signal(
            barrier, inc=1, device_id=(other // blocks_y, lax.rem(other, blocks_y)), device_id_type=MESH
        )
    loads = [
        pltpu.make_async_copy(s, t, load_sem.at[i]) for i, (s, t) in enumerate(zip(sources, loaded))
    ]
    for load in loads[:5]:
        load.start()
    rows = q_ref.shape[0] // planes
    size = 2 * half
    pitch = sent[0].shape[0] // devices

    def x_lines(chunk, charges):
        per = LANES // size
        for group in range(devices // per):
            both = mul(table_x[chunk][group * 2 * LANES : (group + 1) * 2 * LANES, :], charges, ((1,), (1,)))
            made = both[:LANES, :LANES] + both[:LANES, LANES:] + both[LANES:, :LANES]
            step = sent[chunk].shape[0] // devices
            for inner in range(per):
                at = (group * per + inner) * step
                sent[chunk][at : at + size, :] = made[inner * size : (inner + 1) * size, :]

    scope = jax.named_scope
    with scope("kernel_lines"):
        for load in loads[1:4]:
            load.wait()
        lines = mul3((table_k[0][...], table_k[1][...]), split(k_ref[...]), ((1,), (1,)))
        for device in range(devices):
            at = device * pitch + size
            sent[0][at : at + 8, :] = lines[device * 8 : (device + 1) * 8, :]
    with scope("x_load"):
        loads[0].wait()
        loads[4].wait()
        for load in loads[5:]:
            load.start()
    with scope("x_lines0"):
        charges = jnp.concatenate(split(q_ref[...]), axis=0)
        x_lines(0, charges)
    with scope("barrier"):
        pl.semaphore_wait(barrier, devices - 1)
    with scope("send0"):
        there = [exchange(blocks_z, blocks_y, size + 2, sent[0], held[0], sent_sem.at[0])]
    with scope("x_lines1"):
        loads[5].wait()
        x_lines(1, charges)
    with scope("send1"):
        there.append(exchange(blocks_z, blocks_y, size, sent[1], held[1], sent_sem.at[1]))
    with scope("wait_there0"):
        for load in loads[6:12]:
            load.wait()
        there[0][1].wait_recv()
    y_pairs = ((table_y[0][...], table_y[1][...]), (table_b[0][...], table_b[1][...]))
    z_pair = (table_z[0][...], table_z[1][...])
    shape = (count, blocks_z, blocks_y, half)
    with scope("middle0"):
        green = middle_stage(shape, held[0], *y_pairs, *z_pair, None, back[0])
    with scope("return0"):
        returns = [exchange(blocks_z, blocks_y, size, back[0], home[0], back_sem.at[0])]
    with scope("wait_there1"):
        there[1][1].wait_recv()
    with scope("middle1"):
        middle_stage(shape, held[1], *y_pairs, *z_pair, green[:, LANES:], back[1])
    with scope("return1"):
        returns.append(exchange(blocks_z, blocks_y, size, back[1], home[1], back_sem.at[1], True))
    for load in loads[12:]:
        load.wait()
    deep = home[0].shape[0]
    near = pl.multiple_of(me // (devices // 2) * (deep // 2), LANES)
    far = pl.multiple_of(deep // 2 - near, LANES)
    pieces = (
        (0, pl.ds(0, deep), returns[0][1]), (1, pl.ds(near, deep // 2), returns[1][1]),
        (1, pl.ds(far, deep // 2), returns[1][2]),
    )
    borders = []

    def fine_of(number):
        chunk, span, _ = pieces[number]
        return table_f[2 * chunk][span, :], table_f[2 * chunk + 1][span, :]

    half_of = me // (devices // 2)
    slots = (rims[0], *([r.at[s] for r in rims[1]] for s in (half_of, 1 - half_of)))
    rim_sems = [
        (rim_sem.at[0, 0], rim_sem.at[1, 0]),
        (rim_sem.at[0, 1], rim_sem.at[1, 1 + half_of]),
        (rim_sem.at[0, 2], rim_sem.at[1, 2 - half_of]),
    ]
    for number, (chunk, span, coming) in enumerate(pieces):
        with scope(f"wait_back{number}"):
            coming.wait_recv()
        with scope(f"turn{number}"):
            turned = jnp.transpose(home[chunk][span, :])
            own[number][...] = turned
        with scope(f"send_rim{number}"):
            borders.append(send_rims(
                blocks_z, blocks_y, planes, rows, own[number], home, stages[number], slots[number],
                rim_sems[number],
            ))
        with scope(f"own{number}"):
            made = mul3_rows(split(turned), fine_of(number))
            total[...] = total[...] + made if number else made
    flat = 3 * rows

    def pack(place, values):
        high, low = split(values)
        packed[place, :] = high
        packed[pl.ds(place.start + place.size, place.size), :] = low

    for p in range(planes):
        pack(pl.ds(2 * (p + 1) * rows, rows), total[p * rows : (p + 1) * rows, :])
    turn = lax.rem(lax.rem(me // blocks_y, blocks_z // 2), blocks_z // 2 - 1)
    border = jnp.where(turn == 0, 1, 0)
    late = lax.rem(half_of + 1 + border, 2)
    rim_order = [(0, pl.ds(0, deep), rims[0], rim_sem.at[1, 0])]
    for slot in (1 - late, late):
        span = pl.ds(pl.multiple_of(slot * (deep // 2), LANES), deep // 2)
        rim_order.append((1, span, [r.at[slot] for r in rims[1]], rim_sem.at[1, 1 + slot]))
    for number, (chunk, span, slot, sem) in enumerate(rim_order):
        with scope(f"wait_rim{number}"):
            count = pl.ds(0, 3 * (planes + rows + 3) * own[number].shape[1] // LANES)
            other = lax.rem(me + 1, devices)
            remote(
                home[0].at[count], home[1].at[count], (rim_sem.at[0, number], sem),
                (other // blocks_y, lax.rem(other, blocks_y)),
            ).wait_recv()
        with scope(f"rim{number}"):
            fine = (table_f[2 * chunk][span, :], table_f[2 * chunk + 1][span, :])
            made = mul3_rows(split(rim_lines(slot)), fine)
            if number:
                made = edge[...] + made
            if number < len(pieces) - 1:
                edge[...] = made
                continue
            for i, p in enumerate((0, planes + 1, planes + 2)):
                pack(pl.ds(2 * p * rows, rows), made[i * rows : (i + 1) * rows, :])
            pack(pl.ds(2 * (planes + 3) * rows, flat), made[flat:, :])
    with scope("wait_sends"):
        for copy in [there[0][0], there[1][0], returns[0][0], returns[1][0], *borders]:
            copy.wait_send()


STEP = 2


def refine_kernel(rows, x_ref, r_ref, o_ref, made, out_sem):
    planes = made.shape[0] // 2
    stores = []
    for p in range(0, planes, STEP):
        with jax.named_scope(f"refine{p}"):
            near = x_ref[2 * p * rows : 2 * (p + STEP + 3) * rows, :]
            near = jnp.concatenate([near, x_ref[2 * (planes + 3) * rows :, :]], axis=0)
            span = pl.ds(2 * p, 2 * STEP)
            made[span] = mul(r_ref[p // STEP], near).reshape(2 * STEP, -1, made.shape[2])
            stores.append(pltpu.make_async_copy(made.at[span], o_ref.at[span], out_sem.at[p // STEP]))
            stores[-1].start()
    with jax.named_scope("refine_store"):
        for store in stores:
            store.wait()


def rim_table(count):
    made = np.zeros((2 * count, count + 3))
    for i in range(count):
        made[2 * i, i + 1] = 1.0
        made[2 * i + 1, i : i + 4] = np.array([-1.0, 9.0, 9.0, -1.0]) / 16.0
    return made


def refine_tables(planes, rows):
    along_y = rim_table(rows)
    along_z = rim_table(planes)
    middle, sides = along_y[:, 1 : rows + 1], np.delete(along_y, np.arange(1, rows + 1), axis=1)
    order = [*range(1, planes + 1), 0, planes + 1, planes + 2]
    made = []
    for p in range(0, planes, STEP):
        lines = along_z[2 * p : 2 * (p + STEP)]
        own = np.kron(lines[:, p : p + STEP + 3], np.concatenate([middle, middle], axis=1))
        beside = np.einsum("ze,ys->zyse", lines[:, order], sides)
        beside = np.pad(beside, ((0, 0), (0, 0), (0, 0), (0, rows - len(order))))
        beside = beside.reshape(own.shape[0], 3 * rows)
        made.append(np.concatenate([own, beside, beside], axis=1))
    return np.stack(made)


def refine(haloed, planes, rows, width):
    tables = jnp.asarray(refine_tables(planes, rows), jnp.bfloat16)
    shape = (2 * planes, 2 * rows, width)
    return pl.pallas_call(
        functools.partial(refine_kernel, rows),
        out_shape=jax.ShapeDtypeStruct(shape, jnp.float32),
        in_specs=[
            pl.BlockSpec(memory_space=pltpu.VMEM),
            pl.BlockSpec(memory_space=pltpu.VMEM),
        ],
        out_specs=pl.BlockSpec(memory_space=pl.ANY),
        scratch_shapes=[
            pltpu.VMEM(shape, jnp.float32), pltpu.SemaphoreType.DMA((planes // STEP,)),
        ],
        compiler_params=pltpu.CompilerParams(vmem_limit_bytes=16 * 1024 * 1024),
    )(haloed, tables)


def per_device(charges, kernel):
    planes, rows, count = kernel.shape
    width = charges.shape[2]
    replicas = width // count
    half = replicas // 2
    blocks_z, blocks_y = lax.axis_size("gz"), lax.axis_size("gy")
    devices = blocks_z * blocks_y
    place = planes * rows
    fits = place == LANES and 2 * count == LANES and half == 8 and blocks_z == 8
    if not fits or count != CHUNKS * devices or replicas % 2 or rows != 16 or planes != 8 or devices % 8:
        return plain(charges, kernel)
    size = 2 * half
    per = LANES // size
    lines_x = pair_table(count, replicas, devices)
    table_x, table_f = [], []
    for chunk in range(CHUNKS):
        high, low = table(lines_x[chunk].reshape(devices // per, LANES, width))
        table_x.append(jnp.concatenate([high, low], axis=1).reshape(-1, width))
        table_f += table(refined(lines_x[chunk], 1).reshape(-1, 2 * width))
    lines_y = y_table(count, planes, rows)
    tables = [
        *table(line_table(count, devices)), *table_x, *table(lines_y), *table(lines_y.T),
        *z_tables(count, blocks_z), *table_f,
    ]
    arrays = [charges.reshape(place, width), kernel.reshape(place, count), *tables]
    deep = devices * size
    block = lambda *shape: pltpu.VMEM(shape, jnp.float32)
    dma = pltpu.SemaphoreType.DMA
    widths = (deep, deep // 2, deep // 2)
    stages = [block(*shape) for w in widths for shape in ((planes, w), (2 * planes, w), (4, 8, w))]
    rims = [
        block(*lead, *shape, w)
        for lead, w in (((), deep), ((2,), deep // 2))
        for shape in ((rows,), (2 * rows,), (planes,), (2 * planes,), (4, 8))
    ]
    haloed = pl.pallas_call(
        functools.partial(main_kernel, (count, blocks_z, blocks_y, half, len(tables))),
        out_shape=pltpu.VMEM((2 * (planes + 6) * rows, 2 * width), jnp.bfloat16),
        in_specs=[pl.BlockSpec(memory_space=pl.ANY)] * len(arrays),
        out_specs=pl.BlockSpec(memory_space=pltpu.VMEM),
        scratch_shapes=[
            *(pltpu.VMEM(a.shape, a.dtype) for a in arrays),
            dma((len(arrays),)), dma((CHUNKS, 2)), dma((CHUNKS, 3)), dma((2, 3)),
            block(place, 2 * width), block(6 * rows, 2 * width),
            block(devices * (size + 8), LANES), block(deep, LANES),
            block(devices * (size + 8), LANES), block(deep, LANES),
            block(deep, LANES), block(deep, LANES),
            block(deep, LANES), block(deep, LANES),
            *(block(place, w) for w in widths), *stages, *rims,
        ],
        compiler_params=pltpu.CompilerParams(
            collective_id=0, has_side_effects=True, vmem_limit_bytes=60 * 1024 * 1024
        ),
    )(*arrays)
    return refine(haloed, planes, rows, 2 * width)


def solution(mesh):
    placed = (P("gz", "gy", None), P("gz", "gy", None))
    return jax.shard_map(
        per_device, mesh=mesh, in_specs=placed, out_specs=P("gz", "gy", None), check_vma=False
    )
```

```python
import functools

import jax
import jax.numpy as jnp
import numpy as np
from jax import lax
from jax.experimental import pallas as pl
from jax.experimental.pallas import tpu as pltpu
from jax.sharding import PartitionSpec as P

AXES = ("gz", "gy")


def angle(first, second, count):
    return 2.0 * np.pi / count * ((first * second) % count)


def x_table(count, replicas, devices):
    half = replicas // 2
    columns = count * half // devices
    device, part, column, x, side, pair = np.ix_(
        *(np.arange(s) for s in (devices, 2, columns, count, 2, half))
    )
    flat = device * columns + column
    theta = angle(flat // half, x, count)
    value = np.where(part == side, np.cos(theta), np.where(part == 0, np.sin(theta), -np.sin(theta)))
    value = value * (flat % half == pair)
    return value.reshape(devices * 2 * columns, count, replicas)


def x_kernel_table(count, replicas, devices):
    half = replicas // 2
    columns = count * half // devices
    lines = max(1, columns // half)
    device, part, line, x = np.ix_(*(np.arange(s) for s in (devices, 2, lines, count)))
    theta = angle(device * columns // half + line, x, count)
    value = np.where(part == 0, np.cos(theta), -np.sin(theta))
    return value.reshape(devices * 2 * lines, count)


def y_table(count, planes, rows):
    part, block, plane, row, new_plane, new_part, freq = np.ix_(
        *(np.arange(s) for s in (2, count // rows, planes, rows, planes, 2, count))
    )
    theta = angle(block * rows + row, freq, count)
    value = np.where(
        part == new_part, np.cos(theta), np.where(new_part == 0, np.sin(theta), -np.sin(theta))
    )
    value = value * (plane == new_plane)
    return value.reshape(2 * count * planes, planes * 2 * count)


def z_table(count, planes, columns, lines, group, wave):
    blocks = count // planes
    low, high, column, z_low, z_high, line = np.ix_(
        *(np.arange(s) for s in (planes, blocks, columns, planes, blocks, lines))
    )
    theta = angle(high * planes + low, z_high * planes + z_low, count)
    value = wave(theta) * (column // group == line)
    return value.reshape(count * columns, count * lines)


def refined(values, axis):
    before = np.roll(values, 1, axis)
    after = np.roll(values, -1, axis)
    after_two = np.roll(values, -2, axis)
    middle = (9.0 * (values + after) - (before + after_two)) / 16.0
    stacked = np.stack([values, middle], axis=axis + 1)
    shape = list(values.shape)
    shape[axis] = 2 * shape[axis]
    return stacked.reshape(shape)


def const(values):
    return jnp.asarray(np.asarray(values, np.float32))


def dot(left, right, dims=((1,), (0,))):
    return lax.dot_general(
        left, right, (dims, ((), ())), precision=lax.Precision.HIGH,
        preferred_element_type=jnp.float32,
    )


def extended(block, axis, dim):
    size = lax.axis_size(axis)
    forward = [(i, (i + 1) % size) for i in range(size)]
    backward = [(target, source) for source, target in forward]
    low = lax.ppermute(lax.slice_in_dim(block, block.shape[dim] - 1, None, axis=dim), axis, forward)
    high = lax.ppermute(lax.slice_in_dim(block, 0, 2, axis=dim), axis, backward)
    return jnp.concatenate([low, block, high], axis=dim)


def refine_rim(haloed, axis, count):
    centre = lax.slice_in_dim(haloed, 1, 1 + count, axis=axis)
    before = lax.slice_in_dim(haloed, 0, count, axis=axis)
    after = lax.slice_in_dim(haloed, 2, 2 + count, axis=axis)
    after_two = lax.slice_in_dim(haloed, 3, 3 + count, axis=axis)
    middle = (9.0 * (centre + after) - (before + after_two)) / 16.0
    stacked = jnp.stack([centre, middle], axis=axis + 1)
    shape = list(centre.shape)
    shape[axis] = 2 * count
    return stacked.reshape(shape)


def plain(charges, kernel):
    planes, rows, count = kernel.shape
    replicas = charges.shape[2] // count
    half = replicas // 2
    blocks_z, blocks_y = lax.axis_size("gz"), lax.axis_size("gy")
    devices = blocks_z * blocks_y
    place = planes * rows
    columns = count * half // devices
    lines = max(1, columns // half)
    table_x = x_table(count, replicas, devices)
    table_y = const(y_table(count, planes, rows))
    cos_z = const(z_table(count, planes, columns, columns, 1, np.cos))
    sin_z = const(z_table(count, planes, columns, columns, 1, np.sin))
    cos_k = const(z_table(count, planes, columns, lines, half, np.cos) / count**3)
    sin_k = const(z_table(count, planes, columns, lines, half, np.sin) / count**3)

    sent = dot(const(table_x.reshape(-1, count * replicas)), charges.reshape(place, -1), ((1,), (1,)))
    sent_k = dot(const(x_kernel_table(count, replicas, devices)), kernel.reshape(place, count), ((1,), (1,)))
    both = jnp.concatenate(
        [sent.reshape(devices, 2 * columns, place), sent_k.reshape(devices, 2 * lines, place)], axis=1
    )
    both = lax.all_to_all(both, AXES, split_axis=0, concat_axis=0, tiled=True)

    def by_y(block, width):
        block = block.reshape(blocks_z, blocks_y, 2, width, place).transpose(0, 3, 2, 1, 4)
        block = dot(block.reshape(blocks_z * width, 2 * blocks_y * place), table_y)
        block = block.reshape(blocks_z * width, planes, 2 * count).transpose(1, 0, 2)
        return block.reshape(count * width, 2 * count)

    def swap(values):
        return jnp.concatenate([values[:, count:], values[:, :count]], axis=1)

    sign = jnp.where(lax.broadcasted_iota(jnp.int32, (1, 2 * count), 1) < count, 1.0, -1.0)
    data = by_y(both[:, : 2 * columns], columns)
    green = by_y(both[:, 2 * columns :], lines)
    data = dot(cos_z, data) + sign * swap(dot(sin_z, data))
    green = dot(cos_k, green) + sign * swap(dot(sin_k, green))
    real, imag = green[:, :count], green[:, count:]
    data = data * jnp.concatenate([real, real], axis=1) + swap(data) * jnp.concatenate([-imag, imag], axis=1)
    data = dot(cos_z, data) - sign * swap(dot(sin_z, data))
    data = data.reshape(planes, blocks_z * columns, 2 * count).transpose(1, 0, 2)
    data = dot(data.reshape(blocks_z * columns, planes * 2 * count), table_y, ((1,), (1,)))
    data = data.reshape(blocks_z, columns, 2, blocks_y, place).transpose(0, 3, 2, 1, 4)
    data = lax.all_to_all(
        data.reshape(devices, 2 * columns, place), AXES, split_axis=0, concat_axis=0, tiled=True
    )
    fine_x = const(refined(table_x, 1).reshape(-1, 2 * count * replicas))
    result = dot(data.reshape(devices * 2 * columns, place), fine_x, ((0,), (0,)))
    result = result.reshape(planes, rows, 2 * count * replicas)
    result = extended(extended(result, "gz", 0), "gy", 1)
    result = refine_rim(result, 0, planes)
    return refine_rim(result, 1, rows)


LANES = 128
MESH = pl.DeviceIdType.MESH


def table(values):
    high = np.asarray(values, np.float32).astype(jnp.bfloat16)
    low = (np.asarray(values, np.float64) - high.astype(np.float64)).astype(jnp.bfloat16)
    return [jnp.asarray(high), jnp.asarray(low)]


def split(values):
    high = values.astype(jnp.bfloat16)
    return high, (values - high.astype(jnp.float32)).astype(jnp.bfloat16)


def mul(left, right, dims=((1,), (0,))):
    return lax.dot_general(left, right, (dims, ((), ())), preferred_element_type=jnp.float32)


def mul3(left, right, dims=((1,), (0,))):
    (a, b), (c, d) = left, right
    return mul(a, d, dims) + mul(b, c, dims) + mul(a, c, dims)


GROUPS = 4
CHUNKS = 2


def mul3_rows(left, right):
    (a, b), (c, d) = left, right
    rows = a.shape[0]
    both = mul(jnp.concatenate([b, a], axis=0), c)
    return mul(a, d) + both[:rows] + both[rows:]


def line_of(device, chunk, count):
    flip = np.where(device == 0, count // 2, (count - device) % count)
    return np.where(chunk == 0, device, flip)


def pair_table(count, replicas, devices):
    half = replicas // 2
    chunk, device, part, row, x, side, pair = np.ix_(
        *(np.arange(s) for s in (CHUNKS, devices, 2, half, count, 2, half))
    )
    theta = angle(line_of(device, chunk, count), x, count)
    value = np.where(part == side, np.cos(theta), np.where(part == 0, np.sin(theta), -np.sin(theta)))
    value = value * (row == pair)
    return value.reshape(CHUNKS, devices * 2 * half, count, replicas)


def line_table(count, devices):
    device, row, x = np.ix_(*(np.arange(s) for s in (devices, 8, count)))
    theta = angle(device, x, count)
    other = np.where(device == 0, np.cos(angle(count // 2, x, count)), -np.sin(theta))
    value = np.where(row == 0, np.cos(theta), np.where(row == 1, other, 0.0))
    return value.reshape(devices * 8, count)


def stack3(values):
    high = np.asarray(values, np.float32).astype(jnp.bfloat16)
    low = (np.asarray(values, np.float64) - high.astype(np.float64)).astype(jnp.bfloat16)
    return jnp.asarray(np.concatenate([high, high, low], axis=1))


def z_tables(count, blocks):
    planes = count // blocks
    freq = np.arange(count)[:, None]
    place = np.arange(count)[None, :]
    theta = angle(freq, (place % blocks) * planes + place // blocks, count)
    forward = stack3(np.concatenate([np.cos(theta), np.sin(theta)], axis=0))
    inverse = stack3(np.concatenate([np.cos(theta.T), np.sin(theta.T)], axis=0))
    return forward, inverse


def remote(source, target, sems, place):
    return pltpu.make_async_remote_copy(
        src_ref=source, dst_ref=target, send_sem=sems[0], recv_sem=sems[1],
        device_id=place, device_id_type=MESH,
    )


def exchange(blocks_z, blocks_y, rows, source, target, sems, form, halves=False):
    size = blocks_z * blocks_y // GROUPS
    devices = size * GROUPS
    me = lax.axis_index("gz") * blocks_y + lax.axis_index("gy")
    group, inner = me // size, lax.rem(me, size)
    high, low = group // 2, lax.rem(group, 2)
    turn = lax.rem(high + low, 2)
    pitch_from, pitch_to = source.shape[0] // devices, target.shape[0] // devices

    order = [(flip + turn, low + other + turn, flip == other) for flip, other in ((1, 0), (1, 1), (0, 1), (0, 0))]
    ends_first = [(1, 1 - high, False), (0, high, True), (1, high, False), (0, 1 - high, True)]
    if form == 1:
        order = ends_first
    elif form == 2:
        order = ends_first[2:] + ends_first[:2]
    for flip, other_low, own in order:
        across = lax.rem(high + flip, 2)
        far = across * 2 + lax.rem(other_low, 2)
        for step in range(size):
            other = far * size + lax.rem(inner + step, size)
            there = remote(
                source.at[pl.ds(pl.multiple_of(other * pitch_from, 8), rows)],
                target.at[pl.ds(pl.multiple_of(me * pitch_to, 8), rows)],
                (sems.at[0], sems.at[1 + flip if halves else 1]),
                (other // blocks_y, lax.rem(other, blocks_y)),
            )
            if step == 0 and own:
                pl.when(other != me)(there.start)
            else:
                there.start()
    span = min(pitch_from, pitch_to)
    mine_from = pl.ds(pl.multiple_of(me * pitch_from, 8), span)
    target[pl.ds(pl.multiple_of(me * pitch_to, 8), span), :] = source[mine_from, :]
    other = lax.rem(me + 1, devices)

    def counter(number, senders):
        span = pl.ds(0, senders * rows)
        place = (other // blocks_y, lax.rem(other, blocks_y))
        return remote(source.at[span], target.at[span], (sems.at[0], sems.at[number]), place)

    everything = counter(1, devices - 1)
    if halves:
        return everything, counter(1, devices // 2 - 1), counter(2, devices // 2)
    return everything, everything


def swap_parts(values):
    half = LANES // 2
    pieces = [
        pltpu.roll(values[:, p : p + LANES], half, 1) for p in range(0, values.shape[1], LANES)
    ]
    return jnp.concatenate(pieces, axis=1)


def stacked(values):
    high, low = split(values)
    return jnp.concatenate([low, high, high], axis=0)


def repeat(values, times):
    return jnp.concatenate([values] * times, axis=1)


def y_lines(ref, start, stride, blocks):
    return ref[pl.ds(start, blocks, stride=stride), :]


def middle_stage(sizes, held, table_y, table_b, forward, inverse, green, back):
    count, blocks_z, blocks_y, half = sizes
    planes = count // blocks_z
    pitch = held.shape[0] // (blocks_z * blocks_y)
    lane = lax.broadcasted_iota(jnp.int32, (1, LANES), 1)
    sign = jnp.where(lane < count, 1.0, -1.0)

    def gather(row):
        pieces = [y_lines(held, y * pitch + row, blocks_y * pitch, blocks_z) for y in range(blocks_y)]
        return jnp.concatenate(pieces, axis=1)

    lines = [
        jnp.concatenate([gather(column), gather(half + column)], axis=1) for column in range(half)
    ]
    if green is None:
        me = lax.axis_index("gz") * blocks_y + lax.axis_index("gy")
        keep = jnp.where(me == 0, 0.0, 1.0).astype(jnp.float32)
        first, second = gather(2 * half), gather(2 * half + 1)
        lines.append(jnp.concatenate([first, keep * second], axis=1))
        lines.append(
            jnp.concatenate([keep * first + (1.0 - keep) * second, -keep * second], axis=1)
        )
    width = len(lines)
    data = mul3_rows(split(jnp.concatenate(lines, axis=0)), table_y)
    data = jnp.concatenate(
        [
            jnp.concatenate(
                [
                    data[c * blocks_z : (c + 1) * blocks_z, p * LANES : (p + 1) * LANES]
                    for p in range(planes)
                ],
                axis=0,
            )
            for c in range(width)
        ],
        axis=1,
    )
    both = mul(forward, stacked(data))
    data = both[:count] + repeat(sign, width) * swap_parts(both[count:])
    spectra = None
    if green is None:
        scaled = data[:, half * LANES :] * (1.0 / count**3)
        green, spectra = scaled[:, :LANES], scaled
        data = data[:, : half * LANES]
    other = swap_parts(green)
    real = jnp.where(lane < count, green, other)
    imag = jnp.where(lane < count, -other, green)
    data = data * repeat(real, half) + swap_parts(data) * repeat(imag, half)
    both = mul(inverse, stacked(data))
    data = both[:count] - repeat(sign, half) * swap_parts(both[count:])
    data = jnp.concatenate(
        [
            jnp.concatenate(
                [
                    data[p * blocks_z : (p + 1) * blocks_z, c * LANES : (c + 1) * LANES]
                    for p in range(planes)
                ],
                axis=1,
            )
            for c in range(half)
        ],
        axis=0,
    )
    data = mul3_rows(split(data), table_b)
    out_pitch = 2 * half
    for column in range(half):
        for part in range(2):
            for y in range(blocks_y):
                at = (part * blocks_y + y) * LANES
                back[pl.ds(y * out_pitch + part * half + column, blocks_z, stride=blocks_y * out_pitch), :] = (
                    data[column * blocks_z : (column + 1) * blocks_z, at : at + LANES]
                )
    return spectra


def send_rims(blocks_z, blocks_y, planes, rows, own, sizes, stage, rims, sems):
    to_up, to_down, to_corner = stage
    low_z, high_z, low_y, high_y, corner = rims
    gz, gy = lax.axis_index("gz"), lax.axis_index("gy")
    next_z, last_z = lax.rem(gz + 1, blocks_z), lax.rem(gz + blocks_z - 1, blocks_z)
    next_y, last_y = lax.rem(gy + 1, blocks_y), lax.rem(gy + blocks_y - 1, blocks_y)
    end = (planes - 1) * rows
    def side(row):
        return jnp.concatenate([own[p * rows + row : p * rows + row + 1, :] for p in range(planes)], axis=0)

    to_up[...] = side(rows - 1)
    to_down[...] = jnp.concatenate([side(0), side(1)], axis=0)
    picks = (
        (end + rows - 1,), (end, end + 1), (rows - 1, 2 * rows - 1), (0, 1, rows, rows + 1),
    )
    for number, pick in enumerate(picks):
        pieces = [own[r : r + 1, :] for r in pick]
        pieces.append(jnp.zeros((8 - len(pick), own.shape[1]), jnp.float32))
        to_corner[number] = jnp.concatenate(pieces, axis=0)
    places = ((next_z, next_y), (next_z, last_y), (last_z, next_y), (last_z, last_y))
    copies = []
    for number, (pick, place) in enumerate(zip(picks, places)):
        span = pl.ds(0, len(pick))
        copies.append(
            remote(to_corner.at[number, span], corner.at[number, span], sems, place)
        )
    for copy in copies:
        copy.start()
    down = remote(own.at[pl.ds(0, 2 * rows)], high_z, sems, (last_z, gy))
    up = remote(own.at[pl.ds(end, rows)], low_z, sems, (next_z, gy))
    pl.when(gz == 0)(down.start)
    up.start()
    pl.when(gz != 0)(down.start)
    sides = [
        remote(to_up, low_y, sems, (gz, next_y)), remote(to_down, high_y, sems, (gz, last_y)),
    ]
    for copy in sides:
        copy.start()
    count = pl.ds(0, 3 * (planes + rows + 3) * own.shape[1] // LANES)
    return remote(sizes[0].at[count], sizes[1].at[count], sems, (next_z, gy))


def rim_lines(rims):
    low_z, high_z, low_y, high_y, corner = rims
    planes = low_y.shape[0]
    empty = jnp.zeros((5, low_z.shape[1]), jnp.float32)
    tiles = [low_z[...], high_z[...]]
    tiles += [low_y[...], corner[0, 0:1, :], corner[2, 0:2, :], empty]
    tiles += [high_y[:planes, :], corner[1, 0:1, :], corner[3, 0:1, :], corner[3, 2:3, :], empty]
    tiles += [high_y[planes:, :], corner[1, 1:2, :], corner[3, 1:2, :], corner[3, 3:4, :], empty]
    return jnp.concatenate(tiles, axis=0)


def main_kernel(sizes, *refs):
    count, blocks_z, blocks_y, half, n_tables = sizes
    devices = blocks_z * blocks_y
    planes = count // blocks_z
    sources = refs[: 2 + n_tables]
    packed = refs[2 + n_tables]
    loaded = refs[3 + n_tables : 5 + 2 * n_tables]
    (q_ref, k_ref), tables = loaded[:2], loaded[2:]
    rest = list(refs[5 + 2 * n_tables :])
    load_sem, sent_sem, back_sem, rim_sem, total, edge = rest[:6]
    sent, held, back, home = (rest[6 + 2 * i : 8 + 2 * i] for i in range(4))
    own = rest[14:17]
    stages = [rest[17 + 3 * i : 20 + 3 * i] for i in range(3)]
    rims = [rest[26 + 5 * i : 31 + 5 * i] for i in range(2)]
    table_k, table_x, table_y, table_b, table_z, table_f = (
        tables[0:2], tables[2:4], tables[4:6], tables[6:8], tables[8:10], tables[10:14]
    )
    me = lax.axis_index("gz") * blocks_y + lax.axis_index("gy")
    barrier = pltpu.get_barrier_semaphore()
    for step in range(1, devices):
        other = lax.rem(me + step, devices)
        pl.semaphore_signal(
            barrier, inc=1, device_id=(other // blocks_y, lax.rem(other, blocks_y)), device_id_type=MESH
        )
    loads = [
        pltpu.make_async_copy(s, t, load_sem.at[i]) for i, (s, t) in enumerate(zip(sources, loaded))
    ]
    for load in loads[:5]:
        load.start()
    rows = q_ref.shape[0] // planes
    size = 2 * half
    pitch = sent[0].shape[0] // devices

    def x_lines(chunk, charges):
        per = LANES // size
        for group in range(devices // per):
            both = mul(table_x[chunk][group * 2 * LANES : (group + 1) * 2 * LANES, :], charges, ((1,), (1,)))
            made = both[:LANES, :LANES] + both[:LANES, LANES:] + both[LANES:, :LANES]
            step = sent[chunk].shape[0] // devices
            for inner in range(per):
                at = (group * per + inner) * step
                sent[chunk][at : at + size, :] = made[inner * size : (inner + 1) * size, :]

    scope = jax.named_scope
    with scope("kernel_lines"):
        for load in loads[1:4]:
            load.wait()
        lines = mul3((table_k[0][...], table_k[1][...]), split(k_ref[...]), ((1,), (1,)))
        for device in range(devices):
            at = device * pitch + size
            sent[0][at : at + 8, :] = lines[device * 8 : (device + 1) * 8, :]
    with scope("x_load"):
        loads[0].wait()
        loads[4].wait()
        for load in loads[5:]:
            load.start()
    with scope("x_lines0"):
        charges = jnp.concatenate(split(q_ref[...]), axis=0)
        x_lines(0, charges)
    with scope("barrier"):
        pl.semaphore_wait(barrier, devices - 1)
    with scope("send0"):
        there = [exchange(blocks_z, blocks_y, size + 2, sent[0], held[0], sent_sem.at[0], 2)]
    with scope("x_lines1"):
        loads[5].wait()
        x_lines(1, charges)
    with scope("send1"):
        there.append(exchange(blocks_z, blocks_y, size, sent[1], held[1], sent_sem.at[1], 2))
    with scope("wait_there0"):
        for load in loads[6:12]:
            load.wait()
        there[0][1].wait_recv()
    y_pairs = ((table_y[0][...], table_y[1][...]), (table_b[0][...], table_b[1][...]))
    z_pair = (table_z[0][...], table_z[1][...])
    shape = (count, blocks_z, blocks_y, half)
    with scope("middle0"):
        green = middle_stage(shape, held[0], *y_pairs, *z_pair, None, back[0])
    with scope("return0"):
        returns = [exchange(blocks_z, blocks_y, size, back[0], home[0], back_sem.at[0], 1)]
    with scope("wait_there1"):
        there[1][1].wait_recv()
    with scope("middle1"):
        middle_stage(shape, held[1], *y_pairs, *z_pair, green[:, LANES:], back[1])
    with scope("return1"):
        returns.append(exchange(blocks_z, blocks_y, size, back[1], home[1], back_sem.at[1], 1, True))
    for load in loads[12:]:
        load.wait()
    deep = home[0].shape[0]
    near = pl.multiple_of(me // (devices // 2) * (deep // 2), LANES)
    far = pl.multiple_of(deep // 2 - near, LANES)
    pieces = (
        (0, pl.ds(0, deep), returns[0][1]), (1, pl.ds(near, deep // 2), returns[1][1]),
        (1, pl.ds(far, deep // 2), returns[1][2]),
    )
    borders = []

    def fine_of(number):
        chunk, span, _ = pieces[number]
        return table_f[2 * chunk][span, :], table_f[2 * chunk + 1][span, :]

    half_of = me // (devices // 2)
    slots = (rims[0], *([r.at[s] for r in rims[1]] for s in (half_of, 1 - half_of)))
    rim_sems = [
        (rim_sem.at[0, 0], rim_sem.at[1, 0]),
        (rim_sem.at[0, 1], rim_sem.at[1, 1 + half_of]),
        (rim_sem.at[0, 2], rim_sem.at[1, 2 - half_of]),
    ]
    for number, (chunk, span, coming) in enumerate(pieces):
        with scope(f"wait_back{number}"):
            coming.wait_recv()
        with scope(f"turn{number}"):
            turned = jnp.transpose(home[chunk][span, :])
            own[number][...] = turned
        with scope(f"send_rim{number}"):
            borders.append(send_rims(
                blocks_z, blocks_y, planes, rows, own[number], home, stages[number], slots[number],
                rim_sems[number],
            ))
        with scope(f"own{number}"):
            made = mul3_rows(split(turned), fine_of(number))
            total[...] = total[...] + made if number else made
    flat = 3 * rows

    def pack(place, values):
        high, low = split(values)
        packed[place, :] = high
        packed[pl.ds(place.start + place.size, place.size), :] = low

    for p in range(planes):
        pack(pl.ds(2 * (p + 1) * rows, rows), total[p * rows : (p + 1) * rows, :])
    turn = lax.rem(lax.rem(me // blocks_y, blocks_z // 2), blocks_z // 2 - 1)
    border = jnp.where(turn == 0, 1, 0)
    late = lax.rem(half_of + 1 + border, 2)
    rim_order = [(0, pl.ds(0, deep), rims[0], rim_sem.at[1, 0])]
    for slot in (1 - late, late):
        span = pl.ds(pl.multiple_of(slot * (deep // 2), LANES), deep // 2)
        rim_order.append((1, span, [r.at[slot] for r in rims[1]], rim_sem.at[1, 1 + slot]))
    for number, (chunk, span, slot, sem) in enumerate(rim_order):
        with scope(f"wait_rim{number}"):
            count = pl.ds(0, 3 * (planes + rows + 3) * own[number].shape[1] // LANES)
            other = lax.rem(me + 1, devices)
            remote(
                home[0].at[count], home[1].at[count], (rim_sem.at[0, number], sem),
                (other // blocks_y, lax.rem(other, blocks_y)),
            ).wait_recv()
        with scope(f"rim{number}"):
            fine = (table_f[2 * chunk][span, :], table_f[2 * chunk + 1][span, :])
            made = mul3_rows(split(rim_lines(slot)), fine)
            if number:
                made = edge[...] + made
            if number < len(pieces) - 1:
                edge[...] = made
                continue
            for i, p in enumerate((0, planes + 1, planes + 2)):
                pack(pl.ds(2 * p * rows, rows), made[i * rows : (i + 1) * rows, :])
            pack(pl.ds(2 * (planes + 3) * rows, flat), made[flat:, :])
    with scope("wait_sends"):
        for copy in [there[0][0], there[1][0], returns[0][0], returns[1][0], *borders]:
            copy.wait_send()


STEP = 2


def refine_kernel(rows, x_ref, r_ref, o_ref, made, out_sem):
    planes = made.shape[0] // 2
    width = made.shape[2] // 2
    stores = []
    for p in range(0, planes, STEP):
        for half in range(2):
            with jax.named_scope(f"refine{p}"):
                lanes = pl.ds(half * width, width)
                near = x_ref[pl.ds(2 * p * rows, 2 * (STEP + 3) * rows), lanes]
                beside = x_ref[pl.ds(2 * (planes + 3) * rows, 6 * rows), lanes]
                fine = mul(r_ref[p // STEP], jnp.concatenate([near, beside], axis=0))
                place = (pl.ds(2 * p, 2 * STEP), slice(None), lanes)
                made[place] = fine.reshape(2 * STEP, -1, width)
                stores.append(
                    pltpu.make_async_copy(made.at[place], o_ref.at[place], out_sem.at[len(stores)])
                )
                stores[-1].start()
    with jax.named_scope("refine_store"):
        for store in stores:
            store.wait()


def rim_table(count):
    made = np.zeros((2 * count, count + 3))
    for i in range(count):
        made[2 * i, i + 1] = 1.0
        made[2 * i + 1, i : i + 4] = np.array([-1.0, 9.0, 9.0, -1.0]) / 16.0
    return made


def refine_tables(planes, rows):
    along_y = rim_table(rows)
    along_z = rim_table(planes)
    middle, sides = along_y[:, 1 : rows + 1], np.delete(along_y, np.arange(1, rows + 1), axis=1)
    order = [*range(1, planes + 1), 0, planes + 1, planes + 2]
    made = []
    for p in range(0, planes, STEP):
        lines = along_z[2 * p : 2 * (p + STEP)]
        own = np.kron(lines[:, p : p + STEP + 3], np.concatenate([middle, middle], axis=1))
        beside = np.einsum("ze,ys->zyse", lines[:, order], sides)
        beside = np.pad(beside, ((0, 0), (0, 0), (0, 0), (0, rows - len(order))))
        beside = beside.reshape(own.shape[0], 3 * rows)
        made.append(np.concatenate([own, beside, beside], axis=1))
    return np.stack(made)


def refine(haloed, planes, rows, width):
    tables = jnp.asarray(refine_tables(planes, rows), jnp.bfloat16)
    shape = (2 * planes, 2 * rows, width)
    return pl.pallas_call(
        functools.partial(refine_kernel, rows),
        out_shape=jax.ShapeDtypeStruct(shape, jnp.float32),
        in_specs=[
            pl.BlockSpec(memory_space=pltpu.VMEM),
            pl.BlockSpec(memory_space=pltpu.VMEM),
        ],
        out_specs=pl.BlockSpec(memory_space=pl.ANY),
        scratch_shapes=[
            pltpu.VMEM(shape, jnp.float32), pltpu.SemaphoreType.DMA((2 * planes // STEP,)),
        ],
        compiler_params=pltpu.CompilerParams(vmem_limit_bytes=16 * 1024 * 1024),
    )(haloed, tables)


def per_device(charges, kernel):
    planes, rows, count = kernel.shape
    width = charges.shape[2]
    replicas = width // count
    half = replicas // 2
    blocks_z, blocks_y = lax.axis_size("gz"), lax.axis_size("gy")
    devices = blocks_z * blocks_y
    place = planes * rows
    fits = place == LANES and 2 * count == LANES and half == 8 and blocks_z == 8
    if not fits or count != CHUNKS * devices or replicas % 2 or rows != 16 or planes != 8 or devices % 8:
        return plain(charges, kernel)
    size = 2 * half
    per = LANES // size
    lines_x = pair_table(count, replicas, devices)
    table_x, table_f = [], []
    for chunk in range(CHUNKS):
        high, low = table(lines_x[chunk].reshape(devices // per, LANES, width))
        table_x.append(jnp.concatenate([high, low], axis=1).reshape(-1, width))
        table_f += table(refined(lines_x[chunk], 1).reshape(-1, 2 * width))
    lines_y = y_table(count, planes, rows)
    tables = [
        *table(line_table(count, devices)), *table_x, *table(lines_y), *table(lines_y.T),
        *z_tables(count, blocks_z), *table_f,
    ]
    arrays = [charges.reshape(place, width), kernel.reshape(place, count), *tables]
    deep = devices * size
    block = lambda *shape: pltpu.VMEM(shape, jnp.float32)
    dma = pltpu.SemaphoreType.DMA
    widths = (deep, deep // 2, deep // 2)
    stages = [block(*shape) for w in widths for shape in ((planes, w), (2 * planes, w), (4, 8, w))]
    rims = [
        block(*lead, *shape, w)
        for lead, w in (((), deep), ((2,), deep // 2))
        for shape in ((rows,), (2 * rows,), (planes,), (2 * planes,), (4, 8))
    ]
    haloed = pl.pallas_call(
        functools.partial(main_kernel, (count, blocks_z, blocks_y, half, len(tables))),
        out_shape=pltpu.VMEM((2 * (planes + 6) * rows, 2 * width), jnp.bfloat16),
        in_specs=[pl.BlockSpec(memory_space=pl.ANY)] * len(arrays),
        out_specs=pl.BlockSpec(memory_space=pltpu.VMEM),
        scratch_shapes=[
            *(pltpu.VMEM(a.shape, a.dtype) for a in arrays),
            dma((len(arrays),)), dma((CHUNKS, 2)), dma((CHUNKS, 3)), dma((2, 3)),
            block(place, 2 * width), block(6 * rows, 2 * width),
            block(devices * (size + 8), LANES), block(deep, LANES),
            block(devices * (size + 8), LANES), block(deep, LANES),
            block(deep, LANES), block(deep, LANES),
            block(deep, LANES), block(deep, LANES),
            *(block(place, w) for w in widths), *stages, *rims,
        ],
        compiler_params=pltpu.CompilerParams(
            collective_id=0, has_side_effects=True, vmem_limit_bytes=60 * 1024 * 1024
        ),
    )(*arrays)
    return refine(haloed, planes, rows, 2 * width)


def solution(mesh):
    placed = (P("gz", "gy", None), P("gz", "gy", None))
    return jax.shard_map(
        per_device, mesh=mesh, in_specs=placed, out_specs=P("gz", "gy", None), check_vma=False
    )
```

```python
import functools

import jax
import jax.numpy as jnp
import numpy as np
from jax import lax
from jax.experimental import pallas as pl
from jax.experimental.pallas import tpu as pltpu
from jax.sharding import PartitionSpec as P

AXES = ("gz", "gy")


def angle(first, second, count):
    return 2.0 * np.pi / count * ((first * second) % count)


def x_table(count, replicas, devices):
    half = replicas // 2
    columns = count * half // devices
    device, part, column, x, side, pair = np.ix_(
        *(np.arange(s) for s in (devices, 2, columns, count, 2, half))
    )
    flat = device * columns + column
    theta = angle(flat // half, x, count)
    value = np.where(part == side, np.cos(theta), np.where(part == 0, np.sin(theta), -np.sin(theta)))
    value = value * (flat % half == pair)
    return value.reshape(devices * 2 * columns, count, replicas)


def x_kernel_table(count, replicas, devices):
    half = replicas // 2
    columns = count * half // devices
    lines = max(1, columns // half)
    device, part, line, x = np.ix_(*(np.arange(s) for s in (devices, 2, lines, count)))
    theta = angle(device * columns // half + line, x, count)
    value = np.where(part == 0, np.cos(theta), -np.sin(theta))
    return value.reshape(devices * 2 * lines, count)


def y_table(count, planes, rows):
    part, block, plane, row, new_plane, new_part, freq = np.ix_(
        *(np.arange(s) for s in (2, count // rows, planes, rows, planes, 2, count))
    )
    theta = angle(block * rows + row, freq, count)
    value = np.where(
        part == new_part, np.cos(theta), np.where(new_part == 0, np.sin(theta), -np.sin(theta))
    )
    value = value * (plane == new_plane)
    return value.reshape(2 * count * planes, planes * 2 * count)


def z_table(count, planes, columns, lines, group, wave):
    blocks = count // planes
    low, high, column, z_low, z_high, line = np.ix_(
        *(np.arange(s) for s in (planes, blocks, columns, planes, blocks, lines))
    )
    theta = angle(high * planes + low, z_high * planes + z_low, count)
    value = wave(theta) * (column // group == line)
    return value.reshape(count * columns, count * lines)


def refined(values, axis):
    before = np.roll(values, 1, axis)
    after = np.roll(values, -1, axis)
    after_two = np.roll(values, -2, axis)
    middle = (9.0 * (values + after) - (before + after_two)) / 16.0
    stacked = np.stack([values, middle], axis=axis + 1)
    shape = list(values.shape)
    shape[axis] = 2 * shape[axis]
    return stacked.reshape(shape)


def const(values):
    return jnp.asarray(np.asarray(values, np.float32))


def dot(left, right, dims=((1,), (0,))):
    return lax.dot_general(
        left, right, (dims, ((), ())), precision=lax.Precision.HIGH,
        preferred_element_type=jnp.float32,
    )


def extended(block, axis, dim):
    size = lax.axis_size(axis)
    forward = [(i, (i + 1) % size) for i in range(size)]
    backward = [(target, source) for source, target in forward]
    low = lax.ppermute(lax.slice_in_dim(block, block.shape[dim] - 1, None, axis=dim), axis, forward)
    high = lax.ppermute(lax.slice_in_dim(block, 0, 2, axis=dim), axis, backward)
    return jnp.concatenate([low, block, high], axis=dim)


def refine_rim(haloed, axis, count):
    centre = lax.slice_in_dim(haloed, 1, 1 + count, axis=axis)
    before = lax.slice_in_dim(haloed, 0, count, axis=axis)
    after = lax.slice_in_dim(haloed, 2, 2 + count, axis=axis)
    after_two = lax.slice_in_dim(haloed, 3, 3 + count, axis=axis)
    middle = (9.0 * (centre + after) - (before + after_two)) / 16.0
    stacked = jnp.stack([centre, middle], axis=axis + 1)
    shape = list(centre.shape)
    shape[axis] = 2 * count
    return stacked.reshape(shape)


def plain(charges, kernel):
    planes, rows, count = kernel.shape
    replicas = charges.shape[2] // count
    half = replicas // 2
    blocks_z, blocks_y = lax.axis_size("gz"), lax.axis_size("gy")
    devices = blocks_z * blocks_y
    place = planes * rows
    columns = count * half // devices
    lines = max(1, columns // half)
    table_x = x_table(count, replicas, devices)
    table_y = const(y_table(count, planes, rows))
    cos_z = const(z_table(count, planes, columns, columns, 1, np.cos))
    sin_z = const(z_table(count, planes, columns, columns, 1, np.sin))
    cos_k = const(z_table(count, planes, columns, lines, half, np.cos) / count**3)
    sin_k = const(z_table(count, planes, columns, lines, half, np.sin) / count**3)

    sent = dot(const(table_x.reshape(-1, count * replicas)), charges.reshape(place, -1), ((1,), (1,)))
    sent_k = dot(const(x_kernel_table(count, replicas, devices)), kernel.reshape(place, count), ((1,), (1,)))
    both = jnp.concatenate(
        [sent.reshape(devices, 2 * columns, place), sent_k.reshape(devices, 2 * lines, place)], axis=1
    )
    both = lax.all_to_all(both, AXES, split_axis=0, concat_axis=0, tiled=True)

    def by_y(block, width):
        block = block.reshape(blocks_z, blocks_y, 2, width, place).transpose(0, 3, 2, 1, 4)
        block = dot(block.reshape(blocks_z * width, 2 * blocks_y * place), table_y)
        block = block.reshape(blocks_z * width, planes, 2 * count).transpose(1, 0, 2)
        return block.reshape(count * width, 2 * count)

    def swap(values):
        return jnp.concatenate([values[:, count:], values[:, :count]], axis=1)

    sign = jnp.where(lax.broadcasted_iota(jnp.int32, (1, 2 * count), 1) < count, 1.0, -1.0)
    data = by_y(both[:, : 2 * columns], columns)
    green = by_y(both[:, 2 * columns :], lines)
    data = dot(cos_z, data) + sign * swap(dot(sin_z, data))
    green = dot(cos_k, green) + sign * swap(dot(sin_k, green))
    real, imag = green[:, :count], green[:, count:]
    data = data * jnp.concatenate([real, real], axis=1) + swap(data) * jnp.concatenate([-imag, imag], axis=1)
    data = dot(cos_z, data) - sign * swap(dot(sin_z, data))
    data = data.reshape(planes, blocks_z * columns, 2 * count).transpose(1, 0, 2)
    data = dot(data.reshape(blocks_z * columns, planes * 2 * count), table_y, ((1,), (1,)))
    data = data.reshape(blocks_z, columns, 2, blocks_y, place).transpose(0, 3, 2, 1, 4)
    data = lax.all_to_all(
        data.reshape(devices, 2 * columns, place), AXES, split_axis=0, concat_axis=0, tiled=True
    )
    fine_x = const(refined(table_x, 1).reshape(-1, 2 * count * replicas))
    result = dot(data.reshape(devices * 2 * columns, place), fine_x, ((0,), (0,)))
    result = result.reshape(planes, rows, 2 * count * replicas)
    result = extended(extended(result, "gz", 0), "gy", 1)
    result = refine_rim(result, 0, planes)
    return refine_rim(result, 1, rows)


LANES = 128
MESH = pl.DeviceIdType.MESH


def table(values):
    high = np.asarray(values, np.float32).astype(jnp.bfloat16)
    low = (np.asarray(values, np.float64) - high.astype(np.float64)).astype(jnp.bfloat16)
    return [jnp.asarray(high), jnp.asarray(low)]


def split(values):
    high = values.astype(jnp.bfloat16)
    return high, (values - high.astype(jnp.float32)).astype(jnp.bfloat16)


def mul(left, right, dims=((1,), (0,))):
    return lax.dot_general(left, right, (dims, ((), ())), preferred_element_type=jnp.float32)


def mul3(left, right, dims=((1,), (0,))):
    (a, b), (c, d) = left, right
    return mul(a, d, dims) + mul(b, c, dims) + mul(a, c, dims)


GROUPS = 4
CHUNKS = 2


def mul3_rows(left, right):
    (a, b), (c, d) = left, right
    rows = a.shape[0]
    both = mul(jnp.concatenate([b, a], axis=0), c)
    return mul(a, d) + both[:rows] + both[rows:]


def line_of(device, chunk, count):
    flip = np.where(device == 0, count // 2, (count - device) % count)
    return np.where(chunk == 0, device, flip)


def pair_table(count, replicas, devices):
    half = replicas // 2
    chunk, device, part, row, x, side, pair = np.ix_(
        *(np.arange(s) for s in (CHUNKS, devices, 2, half, count, 2, half))
    )
    theta = angle(line_of(device, chunk, count), x, count)
    value = np.where(part == side, np.cos(theta), np.where(part == 0, np.sin(theta), -np.sin(theta)))
    value = value * (row == pair)
    return value.reshape(CHUNKS, devices * 2 * half, count, replicas)


def line_table(count, devices):
    device, row, x = np.ix_(*(np.arange(s) for s in (devices, 8, count)))
    theta = angle(device, x, count)
    other = np.where(device == 0, np.cos(angle(count // 2, x, count)), -np.sin(theta))
    value = np.where(row == 0, np.cos(theta), np.where(row == 1, other, 0.0))
    return value.reshape(devices * 8, count)


def stack3(values):
    high = np.asarray(values, np.float32).astype(jnp.bfloat16)
    low = (np.asarray(values, np.float64) - high.astype(np.float64)).astype(jnp.bfloat16)
    return jnp.asarray(np.concatenate([high, high, low], axis=1))


def z_tables(count, blocks):
    planes = count // blocks
    freq = np.arange(count)[:, None]
    place = np.arange(count)[None, :]
    theta = angle(freq, (place % blocks) * planes + place // blocks, count)
    forward = stack3(np.concatenate([np.cos(theta), np.sin(theta)], axis=0))
    inverse = stack3(np.concatenate([np.cos(theta.T), np.sin(theta.T)], axis=0))
    return forward, inverse


def remote(source, target, sems, place):
    return pltpu.make_async_remote_copy(
        src_ref=source, dst_ref=target, send_sem=sems[0], recv_sem=sems[1],
        device_id=place, device_id_type=MESH,
    )


def exchange(blocks_z, blocks_y, rows, source, target, sems, form, halves=False):
    size = blocks_z * blocks_y // GROUPS
    devices = size * GROUPS
    me = lax.axis_index("gz") * blocks_y + lax.axis_index("gy")
    group, inner = me // size, lax.rem(me, size)
    high, low = group // 2, lax.rem(group, 2)
    turn = lax.rem(high + low, 2)
    pitch_from, pitch_to = source.shape[0] // devices, target.shape[0] // devices

    order = [(flip + turn, low + other + turn, flip == other) for flip, other in ((1, 0), (1, 1), (0, 1), (0, 0))]
    ends_first = [(1, 1 - high, False), (0, high, True), (1, high, False), (0, 1 - high, True)]
    if form == 1:
        order = ends_first
    elif form == 2:
        order = ends_first[2:] + ends_first[:2]
    for flip, other_low, own in order:
        across = lax.rem(high + flip, 2)
        far = across * 2 + lax.rem(other_low, 2)
        for step in range(size):
            other = far * size + lax.rem(inner + step, size)
            there = remote(
                source.at[pl.ds(pl.multiple_of(other * pitch_from, 8), rows)],
                target.at[pl.ds(pl.multiple_of(me * pitch_to, 8), rows)],
                (sems.at[0], sems.at[1 + flip if halves else 1]),
                (other // blocks_y, lax.rem(other, blocks_y)),
            )
            if step == 0 and own:
                pl.when(other != me)(there.start)
            else:
                there.start()
    span = min(pitch_from, pitch_to)
    mine_from = pl.ds(pl.multiple_of(me * pitch_from, 8), span)
    target[pl.ds(pl.multiple_of(me * pitch_to, 8), span), :] = source[mine_from, :]
    other = lax.rem(me + 1, devices)

    def counter(number, senders):
        span = pl.ds(0, senders * rows)
        place = (other // blocks_y, lax.rem(other, blocks_y))
        return remote(source.at[span], target.at[span], (sems.at[0], sems.at[number]), place)

    everything = counter(1, devices - 1)
    if halves:
        return everything, counter(1, devices // 2 - 1), counter(2, devices // 2)
    return everything, everything


def swap_parts(values):
    half = LANES // 2
    pieces = [
        pltpu.roll(values[:, p : p + LANES], half, 1) for p in range(0, values.shape[1], LANES)
    ]
    return jnp.concatenate(pieces, axis=1)


def stacked(values):
    high, low = split(values)
    return jnp.concatenate([low, high, high], axis=0)


def repeat(values, times):
    return jnp.concatenate([values] * times, axis=1)


def y_lines(ref, start, stride, blocks):
    return ref[pl.ds(start, blocks, stride=stride), :]


def middle_stage(sizes, held, table_y, table_b, forward, inverse, green, back):
    count, blocks_z, blocks_y, half = sizes
    planes = count // blocks_z
    pitch = held.shape[0] // (blocks_z * blocks_y)
    lane = lax.broadcasted_iota(jnp.int32, (1, LANES), 1)
    sign = jnp.where(lane < count, 1.0, -1.0)

    def gather(row):
        pieces = [y_lines(held, y * pitch + row, blocks_y * pitch, blocks_z) for y in range(blocks_y)]
        return jnp.concatenate(pieces, axis=1)

    lines = [
        jnp.concatenate([gather(column), gather(half + column)], axis=1) for column in range(half)
    ]
    if green is None:
        me = lax.axis_index("gz") * blocks_y + lax.axis_index("gy")
        keep = jnp.where(me == 0, 0.0, 1.0).astype(jnp.float32)
        first, second = gather(2 * half), gather(2 * half + 1)
        lines.append(jnp.concatenate([first, keep * second], axis=1))
        lines.append(
            jnp.concatenate([keep * first + (1.0 - keep) * second, -keep * second], axis=1)
        )
    width = len(lines)
    data = mul3_rows(split(jnp.concatenate(lines, axis=0)), table_y)
    data = jnp.concatenate(
        [
            jnp.concatenate(
                [
                    data[c * blocks_z : (c + 1) * blocks_z, p * LANES : (p + 1) * LANES]
                    for p in range(planes)
                ],
                axis=0,
            )
            for c in range(width)
        ],
        axis=1,
    )
    both = mul(forward, stacked(data))
    data = both[:count] + repeat(sign, width) * swap_parts(both[count:])
    spectra = None
    if green is None:
        scaled = data[:, half * LANES :] * (1.0 / count**3)
        green, spectra = scaled[:, :LANES], scaled
        data = data[:, : half * LANES]
    other = swap_parts(green)
    real = jnp.where(lane < count, green, other)
    imag = jnp.where(lane < count, -other, green)
    data = data * repeat(real, half) + swap_parts(data) * repeat(imag, half)
    both = mul(inverse, stacked(data))
    data = both[:count] - repeat(sign, half) * swap_parts(both[count:])
    data = jnp.concatenate(
        [
            jnp.concatenate(
                [
                    data[p * blocks_z : (p + 1) * blocks_z, c * LANES : (c + 1) * LANES]
                    for p in range(planes)
                ],
                axis=1,
            )
            for c in range(half)
        ],
        axis=0,
    )
    data = mul3_rows(split(data), table_b)
    out_pitch = 2 * half
    for column in range(half):
        for part in range(2):
            for y in range(blocks_y):
                at = (part * blocks_y + y) * LANES
                back[pl.ds(y * out_pitch + part * half + column, blocks_z, stride=blocks_y * out_pitch), :] = (
                    data[column * blocks_z : (column + 1) * blocks_z, at : at + LANES]
                )
    return spectra


def send_rims(blocks_z, blocks_y, planes, rows, own, sizes, stage, rims, sems):
    to_up, to_down, to_corner = stage
    low_z, high_z, low_y, high_y, corner = rims
    gz, gy = lax.axis_index("gz"), lax.axis_index("gy")
    next_z, last_z = lax.rem(gz + 1, blocks_z), lax.rem(gz + blocks_z - 1, blocks_z)
    next_y, last_y = lax.rem(gy + 1, blocks_y), lax.rem(gy + blocks_y - 1, blocks_y)
    end = (planes - 1) * rows
    def side(row):
        return jnp.concatenate([own[p * rows + row : p * rows + row + 1, :] for p in range(planes)], axis=0)

    to_up[...] = side(rows - 1)
    to_down[...] = jnp.concatenate([side(0), side(1)], axis=0)
    picks = (
        (end + rows - 1,), (end, end + 1), (rows - 1, 2 * rows - 1), (0, 1, rows, rows + 1),
    )
    for number, pick in enumerate(picks):
        pieces = [own[r : r + 1, :] for r in pick]
        pieces.append(jnp.zeros((8 - len(pick), own.shape[1]), jnp.float32))
        to_corner[number] = jnp.concatenate(pieces, axis=0)
    places = ((next_z, next_y), (next_z, last_y), (last_z, next_y), (last_z, last_y))
    copies = []
    for number, (pick, place) in enumerate(zip(picks, places)):
        span = pl.ds(0, len(pick))
        copies.append(
            remote(to_corner.at[number, span], corner.at[number, span], sems, place)
        )
    for copy in copies:
        copy.start()
    down = remote(own.at[pl.ds(0, 2 * rows)], high_z, sems, (last_z, gy))
    up = remote(own.at[pl.ds(end, rows)], low_z, sems, (next_z, gy))
    pl.when(gz == 0)(down.start)
    up.start()
    pl.when(gz != 0)(down.start)
    sides = [
        remote(to_up, low_y, sems, (gz, next_y)), remote(to_down, high_y, sems, (gz, last_y)),
    ]
    for copy in sides:
        copy.start()
    count = pl.ds(0, 3 * (planes + rows + 3) * own.shape[1] // LANES)
    return remote(sizes[0].at[count], sizes[1].at[count], sems, (next_z, gy))


def rim_lines(rims):
    low_z, high_z, low_y, high_y, corner = rims
    planes = low_y.shape[0]
    empty = jnp.zeros((5, low_z.shape[1]), jnp.float32)
    tiles = [low_z[...], high_z[...]]
    tiles += [low_y[...], corner[0, 0:1, :], corner[2, 0:2, :], empty]
    tiles += [high_y[:planes, :], corner[1, 0:1, :], corner[3, 0:1, :], corner[3, 2:3, :], empty]
    tiles += [high_y[planes:, :], corner[1, 1:2, :], corner[3, 1:2, :], corner[3, 3:4, :], empty]
    return jnp.concatenate(tiles, axis=0)


def main_kernel(sizes, *refs):
    count, blocks_z, blocks_y, half, n_tables = sizes
    devices = blocks_z * blocks_y
    planes = count // blocks_z
    sources = refs[: 2 + n_tables]
    packed = refs[2 + n_tables]
    loaded = refs[3 + n_tables : 5 + 2 * n_tables]
    (q_ref, k_ref), tables = loaded[:2], loaded[2:]
    rest = list(refs[5 + 2 * n_tables :])
    load_sem, sent_sem, back_sem, rim_sem, total, edge = rest[:6]
    sent, held, back, home = (rest[6 + 2 * i : 8 + 2 * i] for i in range(4))
    own = rest[14:17]
    stages = [rest[17 + 3 * i : 20 + 3 * i] for i in range(3)]
    rims = [rest[26 + 5 * i : 31 + 5 * i] for i in range(2)]
    table_k, table_x, table_y, table_b, table_z, table_f = (
        tables[0:2], tables[2:4], tables[4:6], tables[6:8], tables[8:10], tables[10:14]
    )
    me = lax.axis_index("gz") * blocks_y + lax.axis_index("gy")
    barrier = pltpu.get_barrier_semaphore()
    for step in range(1, devices):
        other = lax.rem(me + step, devices)
        pl.semaphore_signal(
            barrier, inc=1, device_id=(other // blocks_y, lax.rem(other, blocks_y)), device_id_type=MESH
        )
    loads = [
        pltpu.make_async_copy(s, t, load_sem.at[i]) for i, (s, t) in enumerate(zip(sources, loaded))
    ]
    deep = table_x[0].shape[0] // 2
    x_halves = [
        pltpu.make_async_copy(
            sources[4].at[pl.ds(i * deep, deep)], table_x[0].at[pl.ds(i * deep, deep)],
            load_sem.at[(4, len(loads))[i]],
        )
        for i in range(2)
    ]
    for load in loads[:4] + x_halves:
        load.start()
    rows = q_ref.shape[0] // planes
    size = 2 * half
    pitch = sent[0].shape[0] // devices

    def x_lines(chunk, charges, groups):
        per = LANES // size
        for group in groups:
            both = mul(table_x[chunk][group * 2 * LANES : (group + 1) * 2 * LANES, :], charges, ((1,), (1,)))
            made = both[:LANES, :LANES] + both[:LANES, LANES:] + both[LANES:, :LANES]
            step = sent[chunk].shape[0] // devices
            for inner in range(per):
                at = (group * per + inner) * step
                sent[chunk][at : at + size, :] = made[inner * size : (inner + 1) * size, :]

    scope = jax.named_scope
    with scope("kernel_lines"):
        for load in loads[1:4]:
            load.wait()
        lines = mul3((table_k[0][...], table_k[1][...]), split(k_ref[...]), ((1,), (1,)))
        for device in range(devices):
            at = device * pitch + size
            sent[0][at : at + 8, :] = lines[device * 8 : (device + 1) * 8, :]
    with scope("x_load"):
        loads[0].wait()
        x_halves[0].wait()
    with scope("x_lines0"):
        charges = jnp.concatenate(split(q_ref[...]), axis=0)
        groups = devices * size // LANES
        x_lines(0, charges, range(groups // 2))
        x_halves[1].wait()
        for load in loads[5:]:
            load.start()
        x_lines(0, charges, range(groups // 2, groups))
    with scope("barrier"):
        pl.semaphore_wait(barrier, devices - 1)
    with scope("send0"):
        there = [exchange(blocks_z, blocks_y, size + 2, sent[0], held[0], sent_sem.at[0], 2)]
    with scope("x_lines1"):
        loads[5].wait()
        x_lines(1, charges, range(groups))
    with scope("send1"):
        there.append(exchange(blocks_z, blocks_y, size, sent[1], held[1], sent_sem.at[1], 2))
    with scope("wait_there0"):
        for load in loads[6:12]:
            load.wait()
        there[0][1].wait_recv()
    y_pairs = ((table_y[0][...], table_y[1][...]), (table_b[0][...], table_b[1][...]))
    z_pair = (table_z[0][...], table_z[1][...])
    shape = (count, blocks_z, blocks_y, half)
    with scope("middle0"):
        green = middle_stage(shape, held[0], *y_pairs, *z_pair, None, back[0])
    with scope("return0"):
        returns = [exchange(blocks_z, blocks_y, size, back[0], home[0], back_sem.at[0], 1)]
    with scope("wait_there1"):
        there[1][1].wait_recv()
    with scope("middle1"):
        middle_stage(shape, held[1], *y_pairs, *z_pair, green[:, LANES:], back[1])
    with scope("return1"):
        returns.append(exchange(blocks_z, blocks_y, size, back[1], home[1], back_sem.at[1], 1, True))
    for load in loads[12:]:
        load.wait()
    deep = home[0].shape[0]
    near = pl.multiple_of(me // (devices // 2) * (deep // 2), LANES)
    far = pl.multiple_of(deep // 2 - near, LANES)
    pieces = (
        (0, pl.ds(0, deep), returns[0][1]), (1, pl.ds(near, deep // 2), returns[1][1]),
        (1, pl.ds(far, deep // 2), returns[1][2]),
    )
    borders = []

    def fine_of(number):
        chunk, span, _ = pieces[number]
        return table_f[2 * chunk][span, :], table_f[2 * chunk + 1][span, :]

    half_of = me // (devices // 2)
    slots = (rims[0], *([r.at[s] for r in rims[1]] for s in (half_of, 1 - half_of)))
    rim_sems = [
        (rim_sem.at[0, 0], rim_sem.at[1, 0]),
        (rim_sem.at[0, 1], rim_sem.at[1, 1 + half_of]),
        (rim_sem.at[0, 2], rim_sem.at[1, 2 - half_of]),
    ]
    for number, (chunk, span, coming) in enumerate(pieces):
        with scope(f"wait_back{number}"):
            coming.wait_recv()
        with scope(f"turn{number}"):
            turned = jnp.transpose(home[chunk][span, :])
            own[number][...] = turned
        with scope(f"send_rim{number}"):
            borders.append(send_rims(
                blocks_z, blocks_y, planes, rows, own[number], home, stages[number], slots[number],
                rim_sems[number],
            ))
        with scope(f"own{number}"):
            made = mul3_rows(split(turned), fine_of(number))
            total[...] = total[...] + made if number else made
    flat = 3 * rows

    def pack(place, values):
        high, low = split(values)
        packed[place, :] = high
        packed[pl.ds(place.start + place.size, place.size), :] = low

    for p in range(planes):
        pack(pl.ds(2 * (p + 1) * rows, rows), total[p * rows : (p + 1) * rows, :])
    turn = lax.rem(lax.rem(me // blocks_y, blocks_z // 2), blocks_z // 2 - 1)
    border = jnp.where(turn == 0, 1, 0)
    late = lax.rem(half_of + 1 + border, 2)
    rim_order = [(0, pl.ds(0, deep), rims[0], rim_sem.at[1, 0])]
    for slot in (1 - late, late):
        span = pl.ds(pl.multiple_of(slot * (deep // 2), LANES), deep // 2)
        rim_order.append((1, span, [r.at[slot] for r in rims[1]], rim_sem.at[1, 1 + slot]))
    for number, (chunk, span, slot, sem) in enumerate(rim_order):
        with scope(f"wait_rim{number}"):
            count = pl.ds(0, 3 * (planes + rows + 3) * own[number].shape[1] // LANES)
            other = lax.rem(me + 1, devices)
            remote(
                home[0].at[count], home[1].at[count], (rim_sem.at[0, number], sem),
                (other // blocks_y, lax.rem(other, blocks_y)),
            ).wait_recv()
        with scope(f"rim{number}"):
            fine = (table_f[2 * chunk][span, :], table_f[2 * chunk + 1][span, :])
            made = mul3_rows(split(rim_lines(slot)), fine)
            if number:
                made = edge[...] + made
            if number < len(pieces) - 1:
                edge[...] = made
                continue
            for i, p in enumerate((0, planes + 1, planes + 2)):
                pack(pl.ds(2 * p * rows, rows), made[i * rows : (i + 1) * rows, :])
            pack(pl.ds(2 * (planes + 3) * rows, flat), made[flat:, :])
    with scope("wait_sends"):
        for copy in [there[0][0], there[1][0], returns[0][0], returns[1][0], *borders]:
            copy.wait_send()


STEP = 2


def refine_kernel(rows, x_ref, r_ref, o_ref, made, out_sem):
    planes = made.shape[0] // 2
    width = made.shape[2] // 2
    stores = []
    for p in range(0, planes, STEP):
        for half in range(2):
            with jax.named_scope(f"refine{p}"):
                lanes = pl.ds(half * width, width)
                near = x_ref[pl.ds(2 * p * rows, 2 * (STEP + 3) * rows), lanes]
                beside = x_ref[pl.ds(2 * (planes + 3) * rows, 6 * rows), lanes]
                fine = mul(r_ref[p // STEP], jnp.concatenate([near, beside], axis=0))
                place = (pl.ds(2 * p, 2 * STEP), slice(None), lanes)
                made[place] = fine.reshape(2 * STEP, -1, width)
                stores.append(
                    pltpu.make_async_copy(made.at[place], o_ref.at[place], out_sem.at[len(stores)])
                )
                stores[-1].start()
    with jax.named_scope("refine_store"):
        for store in stores:
            store.wait()


def rim_table(count):
    made = np.zeros((2 * count, count + 3))
    for i in range(count):
        made[2 * i, i + 1] = 1.0
        made[2 * i + 1, i : i + 4] = np.array([-1.0, 9.0, 9.0, -1.0]) / 16.0
    return made


def refine_tables(planes, rows):
    along_y = rim_table(rows)
    along_z = rim_table(planes)
    middle, sides = along_y[:, 1 : rows + 1], np.delete(along_y, np.arange(1, rows + 1), axis=1)
    order = [*range(1, planes + 1), 0, planes + 1, planes + 2]
    made = []
    for p in range(0, planes, STEP):
        lines = along_z[2 * p : 2 * (p + STEP)]
        own = np.kron(lines[:, p : p + STEP + 3], np.concatenate([middle, middle], axis=1))
        beside = np.einsum("ze,ys->zyse", lines[:, order], sides)
        beside = np.pad(beside, ((0, 0), (0, 0), (0, 0), (0, rows - len(order))))
        beside = beside.reshape(own.shape[0], 3 * rows)
        made.append(np.concatenate([own, beside, beside], axis=1))
    return np.stack(made)


def refine(haloed, planes, rows, width):
    tables = jnp.asarray(refine_tables(planes, rows), jnp.bfloat16)
    shape = (2 * planes, 2 * rows, width)
    return pl.pallas_call(
        functools.partial(refine_kernel, rows),
        out_shape=jax.ShapeDtypeStruct(shape, jnp.float32),
        in_specs=[
            pl.BlockSpec(memory_space=pltpu.VMEM),
            pl.BlockSpec(memory_space=pltpu.VMEM),
        ],
        out_specs=pl.BlockSpec(memory_space=pl.ANY),
        scratch_shapes=[
            pltpu.VMEM(shape, jnp.float32), pltpu.SemaphoreType.DMA((2 * planes // STEP,)),
        ],
        compiler_params=pltpu.CompilerParams(vmem_limit_bytes=16 * 1024 * 1024),
    )(haloed, tables)


def per_device(charges, kernel):
    planes, rows, count = kernel.shape
    width = charges.shape[2]
    replicas = width // count
    half = replicas // 2
    blocks_z, blocks_y = lax.axis_size("gz"), lax.axis_size("gy")
    devices = blocks_z * blocks_y
    place = planes * rows
    fits = place == LANES and 2 * count == LANES and half == 8 and blocks_z == 8
    if not fits or count != CHUNKS * devices or replicas % 2 or rows != 16 or planes != 8 or devices % 8:
        return plain(charges, kernel)
    size = 2 * half
    per = LANES // size
    lines_x = pair_table(count, replicas, devices)
    table_x, table_f = [], []
    for chunk in range(CHUNKS):
        high, low = table(lines_x[chunk].reshape(devices // per, LANES, width))
        table_x.append(jnp.concatenate([high, low], axis=1).reshape(-1, width))
        table_f += table(refined(lines_x[chunk], 1).reshape(-1, 2 * width))
    lines_y = y_table(count, planes, rows)
    tables = [
        *table(line_table(count, devices)), *table_x, *table(lines_y), *table(lines_y.T),
        *z_tables(count, blocks_z), *table_f,
    ]
    arrays = [charges.reshape(place, width), kernel.reshape(place, count), *tables]
    deep = devices * size
    block = lambda *shape: pltpu.VMEM(shape, jnp.float32)
    dma = pltpu.SemaphoreType.DMA
    widths = (deep, deep // 2, deep // 2)
    stages = [block(*shape) for w in widths for shape in ((planes, w), (2 * planes, w), (4, 8, w))]
    rims = [
        block(*lead, *shape, w)
        for lead, w in (((), deep), ((2,), deep // 2))
        for shape in ((rows,), (2 * rows,), (planes,), (2 * planes,), (4, 8))
    ]
    haloed = pl.pallas_call(
        functools.partial(main_kernel, (count, blocks_z, blocks_y, half, len(tables))),
        out_shape=pltpu.VMEM((2 * (planes + 6) * rows, 2 * width), jnp.bfloat16),
        in_specs=[pl.BlockSpec(memory_space=pl.ANY)] * len(arrays),
        out_specs=pl.BlockSpec(memory_space=pltpu.VMEM),
        scratch_shapes=[
            *(pltpu.VMEM(a.shape, a.dtype) for a in arrays),
            dma((len(arrays) + 1,)), dma((CHUNKS, 2)), dma((CHUNKS, 3)), dma((2, 3)),
            block(place, 2 * width), block(6 * rows, 2 * width),
            block(devices * (size + 8), LANES), block(deep, LANES),
            block(devices * (size + 8), LANES), block(deep, LANES),
            block(deep, LANES), block(deep, LANES),
            block(deep, LANES), block(deep, LANES),
            *(block(place, w) for w in widths), *stages, *rims,
        ],
        compiler_params=pltpu.CompilerParams(
            collective_id=0, has_side_effects=True, vmem_limit_bytes=60 * 1024 * 1024
        ),
    )(*arrays)
    return refine(haloed, planes, rows, 2 * width)


def solution(mesh):
    placed = (P("gz", "gy", None), P("gz", "gy", None))
    return jax.shard_map(
        per_device, mesh=mesh, in_specs=placed, out_specs=P("gz", "gy", None), check_vma=False
    )
```
